8 devices in a mesh: dp: 1 (over z), col: 2 (over y), row: 4 (over x, core).
Axes of the slice: x: 2, y: 2, z: 1, core: 2. Of those that a mesh axis runs over, the one named last changes fastest.
Arguments:
- act_in: bfloat16 [8192, 8192], P(('dp', 'row'), 'col')
- w_down: bfloat16 [8192, 2048], P('row', 'col')
- grad_out: bfloat16 [8192, 2048], P(('dp', 'row'), 'col')
Outputs:
- output 1: bfloat16 [8192, 8192], P(('dp', 'row'), 'col')
- output 2: float32 [8192, 2048], P(('dp', 'row'), 'col')
All inputs are finite; a program needn't handle non-finite values.
Results may differ from the reference program's by a relative error of at most 0.001.
Values are sent between devices in bfloat16 or wider.
A program may use at most 1 GiB of HBM per device.

```python
import jax
import jax.numpy as jnp

TOKENS = 8192
FEAT_IN = 8192
FEAT_OUT = 2048


def setup_inputs(seed: int = 0, part: int = 0) -> dict:
    base_key = jax.random.key(seed)
    key_w, key_part = jax.random.split(base_key)
    part_key = jax.random.fold_in(key_part, part)
    key_x, key_dy = jax.random.split(part_key)
    act_vals = jax.random.normal(key_x, (TOKENS, FEAT_IN), jnp.float32) * (TOKENS ** -0.5)
    weight_vals = jax.random.normal(key_w, (FEAT_IN, FEAT_OUT), jnp.float32) * (FEAT_OUT ** -0.5)
    grad_vals = jax.random.normal(key_dy, (TOKENS, FEAT_OUT), jnp.float32)
    return {"act_in": act_vals.astype(jnp.bfloat16), "w_down": weight_vals.astype(jnp.bfloat16), "grad_out": grad_vals.astype(jnp.bfloat16)}


def reference(act_in, w_down, grad_out):
    grad_in = jnp.dot(grad_out, w_down.T, preferred_element_type=jnp.float32).astype(jnp.bfloat16)
    grad_w = jnp.dot(act_in.T, grad_out, preferred_element_type=jnp.float32)
    return (grad_in, grad_w)
```

```python
import functools

import jax
import jax.numpy as jnp
from jax import lax
from jax.experimental import pallas as pl
from jax.experimental.pallas import tpu as pltpu
from jax.sharding import PartitionSpec as P

MESH = pl.DeviceIdType.MESH
F32 = jnp.float32
BF16 = jnp.bfloat16


def _tdot(a, b):
    return lax.dot_general(a, b, (((0,), (0,)), ((), ())), preferred_element_type=F32)


def _dot_t(a, b):
    return lax.dot_general(a, b, (((1,), (1,)), ((), ())), preferred_element_type=F32)


def kernel(
    x_ref, w_ref, dy_ref,
    dx_ref, dw_ref, wbuf, bufx, bufy,
    dyv, xo, xs, pown, poth, wv, xv, lb,
    ld_sem, dys_r, dyy_r, xs_r, w_r, ws_r, px_r, py_r,
    s_dys, s_dyy, s_xs, s_w, s_ws, s_px, s_py, s_sum,
    wl_sem, xv_sem, lb_sem, out_sem,
):
    row = lax.axis_index("row")
    y = lax.axis_index("col")
    x = row // 2
    c = row % 2
    is_a = x == y
    is_b = x != y
    sib = {"row": row + 1 - 2 * c}
    xn = {"row": (row + 2) % 4}
    yn = {"col": 1 - y}

    def remote(src, dst, ssem, rsem, dev):
        return pltpu.make_async_remote_copy(
            src_ref=src, dst_ref=dst, send_sem=ssem, recv_sem=rsem, device_id=dev, device_id_type=MESH
        )

    def local(src, dst, sem):
        return pltpu.make_async_copy(src, dst, sem)

    def qs(q):
        return pl.ds(q * 256, 256)

    barrier = pltpu.get_barrier_semaphore()
    for dev in (sib, xn, yn):
        pl.semaphore_signal(barrier, inc=1, device_id=dev, device_id_type=MESH)
    pl.semaphore_wait(barrier, 3)

    def dy_to_sib(j, q):
        src = dy_ref.at[:, qs(q)] if j == 0 else dyv.at[0, 1, :, qs(q)]
        return remote(src, dyv.at[1, j, :, qs(q)], s_dys.at[0], dys_r.at[j, q], sib)

    def dy_to_y(q):
        return remote(dy_ref.at[:, qs(q)], dyv.at[0, 1, :, qs(q)], s_dyy.at[0], dyy_r.at[q], yn)

    def x_load(kt):
        return local(x_ref.at[:, pl.ds(c * 2048 + kt * 512, 512)], xo.at[kt], ld_sem.at[1 + kt])

    def x_to_sib(kt):
        return remote(
            x_ref.at[:, pl.ds((1 - c) * 2048 + kt * 512, 512)], xs.at[kt], s_xs.at[0], xs_r.at[kt], sib
        )

    def rows(i):
        return pl.ds(i * 256, 256)

    def w_own_to_x(i):
        return remote(w_ref.at[rows(i)], wbuf.at[0, 0, rows(i)], s_w.at[0], w_r.at[0, i], xn)

    def w_to_y(i):
        return remote(w_ref.at[rows(i)], wbuf.at[0, 1, rows(i)], s_w.at[0], w_r.at[1, i], yn)

    def w_fwd(i):
        return remote(wbuf.at[0, 1, rows(i)], wbuf.at[0, 1, rows(i)], s_w.at[0], w_r.at[1, i], xn)

    def w_to_sib(j, i, own):
        src = w_ref.at[rows(i)] if own else wbuf.at[0, j, rows(i)]
        return remote(src, wbuf.at[1, j, rows(i)], s_ws.at[0], ws_r.at[j, i], sib)

    def p_to_x(g, src, q, kt):
        return remote(src.at[q, kt], bufx.at[g, q % 2, kt], s_px.at[0], px_r.at[g * 8 + (q % 2) * 4 + kt], xn)

    def p_to_y_half(q, kt, h):
        part = pl.ds(h * 256, 256)
        return remote(
            poth.at[q, kt, part], bufy.at[q, kt, part], s_py.at[0], py_r.at[q * 8 + kt * 2 + h], yn
        )

    def p_fwd(i):
        q, kt, h = i // 8, (i // 2) % 4, i % 2
        part = pl.ds(h * 256, 256)
        return remote(bufy.at[q, kt, part], bufx.at[0, q, kt, part], s_px.at[0], px_r.at[i], xn)

    def p_term(q, kt):
        return remote(poth.at[q, kt], bufy.at[q, kt], s_py.at[0], py_r.at[q * 4 + kt], yn)

    def sum_to_y(q, kt):
        return remote(
            poth.at[q, kt], dw_ref.at[pl.ds(kt * 512, 512), qs(q)], s_sum.at[0],
            py_r.at[8 + (q - 2) * 4 + kt], yn,
        )

    dy_load = local(dy_ref, dyv.at[0, 0], ld_sem.at[0])
    dy_to_sib(0, 0).start()
    dy_to_y(0).start()
    dy_load.start()
    x_to_sib(0).start()
    x_load(0).start()

    @pl.when(is_a)
    def _():
        for i in range(8):
            w_own_to_x(i).start()
        for q in range(1, 4):
            dy_to_y(q).start()

    @pl.when(is_b)
    def _():
        dy_to_y(1).start()
        for i in range(6):
            w_to_y(i).start()
        dy_to_y(2).start()
        for i in range(6, 8):
            w_to_y(i).start()
        dy_to_y(3).start()

    for kt in range(1, 4):
        x_to_sib(kt).start()
        x_load(kt).start()
    for q in range(1, 4):
        dy_to_sib(0, q).start()

    @pl.when(is_a)
    def _():
        for i in range(8):
            w_to_sib(0, i, True).start()

    def p_tile(dst, j, q, kt):
        dst[q, kt] = _tdot(xo[kt], dyv[0, j, :, q * 256:(q + 1) * 256]) + _tdot(
            xs[kt], dyv[1, j, :, q * 256:(q + 1) * 256]
        )

    dy_load.wait()
    for q in range(4):
        dy_to_sib(0, q).wait_recv()

        def own_body(kt, carry, q=q):
            if q == 0:
                x_load(kt).wait()
                x_to_sib(kt).wait_recv()
            p_tile(pown, 0, q, kt)
            if q < 2:
                @pl.when(is_b)
                def _():
                    p_to_x(0, pown, q, kt).start()
            return carry

        lax.fori_loop(0, 4, own_body, 0)

    def other_pass(q):
        dy_to_y(q).wait_recv()
        dy_to_sib(1, q).start()
        dy_to_sib(1, q).wait_recv()

        def body(kt, carry):
            p_tile(poth, 1, q, kt)
            if q < 2:
                @pl.when(is_a)
                def _():
                    p_term(q, kt).start()

                @pl.when(is_b)
                def _():
                    p_to_y_half(q, kt, 0).start()
                    p_to_y_half(q, kt, 1).start()
            else:
                @pl.when(is_b)
                def _():
                    p_to_x(1, poth, q, kt).start()
            return carry

        lax.fori_loop(0, 4, body, 0)

    def a_final(g, t):
        q2, kt = t // 4, t % 4
        q = q2 + (0 if g == 0 else 2)
        p_to_x(g, pown, q, kt).wait_recv()
        ld = local(bufx.at[g, q2, kt], lb.at[0], lb_sem.at[0])
        ld.start()
        ld.wait()
        pown[q, kt] = pown[q, kt] + lb[0]
        local(pown.at[q, kt], dw_ref.at[pl.ds(kt * 512, 512), qs(q)], out_sem.at[0]).start()

    def a_sum(q, kt):
        p_to_x(1, poth, q, kt).wait_recv()
        ld = local(bufx.at[1, q % 2, kt], lb.at[1], lb_sem.at[1])
        ld.start()
        ld.wait()
        poth[q, kt] = poth[q, kt] + lb[1]
        sum_to_y(q, kt).start()

    def w_fwd_step(i):
        w_to_y(i).wait_recv()
        w_fwd(i).start()
        w_to_sib(1, i, False).start()

    def w_loads(e, own_from_arg):
        cc, d = e % 2, e // 2
        slot = e % 2
        if own_from_arg:
            first = local(w_ref.at[rows(d)], wv.at[slot, 0], wl_sem.at[slot, 0])
        else:
            first = local(wbuf.at[cc, 0, rows(d)], wv.at[slot, 0], wl_sem.at[slot, 0])
        return first, local(wbuf.at[cc, 1, rows(d)], wv.at[slot, 1], wl_sem.at[slot, 1])

    def xv_out(d, cc):
        k0 = (c + cc * (1 - 2 * c)) * 2048
        return local(xv.at[cc], dx_ref.at[:, pl.ds(k0 + d * 256, 256)], xv_sem.at[cc])

    def dx_stripe(d, cc):
        @pl.when(d > 0)
        def _():
            xv_out(d, cc).wait()

        def body(m, carry):
            part = pl.ds(m * 512, 512)
            xv[cc, part, :] = (
                _dot_t(dyv[0, 0, part, :], wv[cc, 0]) + _dot_t(dyv[0, 1, part, :], wv[cc, 1])
            ).astype(BF16)
            return carry

        lax.fori_loop(0, 4, body, 0)
        xv_out(d, cc).start()

    def start_loads(d, cc, own_from_arg):
        for cp in w_loads(2 * d + cc, own_from_arg):
            cp.start()

    def wait_loads(d, cc, own_from_arg):
        for cp in w_loads(2 * d + cc, own_from_arg):
            cp.wait()

    other_pass(0)
    other_pass(1)

    @pl.when(is_a)
    def _():
        def body(i, carry):
            w_fwd_step(i)
            a_final(0, i)
            return carry

        lax.fori_loop(0, 6, body, 0)

    other_pass(2)

    @pl.when(is_a)
    def _():
        def body(i, carry):
            w_fwd_step(i)
            a_final(0, i)
            a_sum(2, 2 * (i - 6))
            a_sum(2, 2 * (i - 6) + 1)
            return carry

        lax.fori_loop(6, 8, body, 0)

    other_pass(3)

    @pl.when(is_a)
    def _():
        def sib_wait(d):
            w_to_sib(0, d, True).wait_recv()
            w_to_sib(1, d, False).wait_recv()

        start_loads(0, 0, True)

        def body(d, carry):
            p_to_y_half(d // 4, d % 4, 0).wait_recv()
            p_fwd(2 * d).start()
            sib_wait(d)
            start_loads(d, 1, False)
            wait_loads(d, 0, True)
            dx_stripe(d, 0)

            @pl.when(d < 4)
            def _():
                a_sum(3, d)

            p_to_y_half(d // 4, d % 4, 1).wait_recv()
            p_fwd(2 * d + 1).start()

            @pl.when(d < 7)
            def _():
                start_loads(d + 1, 0, True)

            wait_loads(d, 1, False)
            dx_stripe(d, 1)

            @pl.when(d >= 2)
            def _():
                a_final(2, d - 2)
            return carry

        lax.fori_loop(0, 8, body, 0)
        a_final(2, 6)
        a_final(2, 7)
        for cc in range(2):
            xv_out(7, cc).wait()
        local(dw_ref, dw_ref, out_sem.at[0]).wait()
        remote(wbuf.at[0], wbuf.at[0], s_w.at[0], w_r.at[0, 0], xn).wait_send()
        remote(bufx.at[0], bufx.at[0], s_px.at[0], px_r.at[0], xn).wait_send()
        remote(bufy, bufy, s_py.at[0], py_r.at[0], yn).wait_send()
        remote(bufy, bufy, s_sum.at[0], py_r.at[0], yn).wait_send()

    @pl.when(is_b)
    def _():
        for q in range(2, 4):
            for kt in range(4):
                p_to_x(2, pown, q, kt).start()

        def own_w(i, carry):
            w_own_to_x(i).wait_recv()
            w_to_sib(0, i, False).start()
            return carry

        lax.fori_loop(0, 8, own_w, 0)

        def body(d, carry):
            w_to_y(d).wait_recv()
            w_to_sib(1, d, False).start()
            start_loads(d, 0, False)
            w_to_sib(0, d, False).wait_recv()
            w_to_sib(1, d, False).wait_recv()
            start_loads(d, 1, False)
            wait_loads(d, 0, False)
            dx_stripe(d, 0)
            wait_loads(d, 1, False)
            dx_stripe(d, 1)
            return carry

        lax.fori_loop(0, 8, body, 0)

        def out_half(q, kt, h, slot):
            return local(
                lb.at[2 + slot, pl.ds(0, 256)],
                dw_ref.at[pl.ds(kt * 512 + h * 256, 256), pl.ds(q * 256, 256)],
                out_sem.at[slot],
            )

        def fin(i, carry):
            q, kt = i // 4, i % 4
            p_term(q, kt).wait_recv()
            for h in range(2):
                part = pl.ds(h * 256, 256)
                first = local(bufy.at[q, kt, part], lb.at[h, pl.ds(0, 256)], lb_sem.at[h])
                first.start()
                p_fwd(i * 2 + h).wait_recv()
                second = local(bufx.at[0, q, kt, part], lb.at[h, pl.ds(256, 256)], lb_sem.at[2 + h])
                second.start()

                @pl.when(i > 0)
                def _():
                    out_half(q, kt, h, h).wait()

                first.wait()
                second.wait()
                lb[2 + h, 0:256] = lb[h, 0:256] + lb[h, 256:512]
                out_half(q, kt, h, h).start()
            return carry

        lax.fori_loop(0, 8, fin, 0)
        for q in range(2, 4):
            for kt in range(4):
                sum_to_y(q, kt).wait_recv()
        for h in range(2):
            out_half(1, 3, h, h).wait()
        for cc in range(2):
            xv_out(7, cc).wait()
        remote(wbuf.at[0, 0], wbuf.at[0, 0], s_w.at[0], w_r.at[0, 0], yn).wait_send()
        remote(bufx, bufx, s_px.at[0], px_r.at[0], xn).wait_send()
        remote(bufy, bufy, s_py.at[0], py_r.at[0], yn).wait_send()

    remote(dyv.at[0], dyv.at[0], s_dys.at[0], dys_r.at[0, 0], sib).wait_send()
    remote(dyv.at[0, 0], dyv.at[0, 0], s_dyy.at[0], dyy_r.at[0], yn).wait_send()
    remote(xs, xs, s_xs.at[0], xs_r.at[0], sib).wait_send()
    remote(wbuf.at[0], wbuf.at[0], s_ws.at[0], ws_r.at[0, 0], sib).wait_send()


def local_backward(act_blk, w_blk, grad_blk):
    any_spec = pl.BlockSpec(memory_space=pl.ANY)
    dma = pltpu.SemaphoreType.DMA
    outs = pl.pallas_call(
        kernel,
        out_shape=(
            jax.ShapeDtypeStruct((2048, 4096), BF16),
            jax.ShapeDtypeStruct((2048, 1024), F32),
            jax.ShapeDtypeStruct((2, 2, 2048, 1024), BF16),
            jax.ShapeDtypeStruct((3, 2, 4, 512, 256), F32),
            jax.ShapeDtypeStruct((2, 4, 512, 256), F32),
        ),
        in_specs=[any_spec] * 3,
        out_specs=(any_spec,) * 5,
        scratch_shapes=[
            pltpu.VMEM((2, 2, 2048, 1024), BF16),
            pltpu.VMEM((4, 2048, 512), BF16),
            pltpu.VMEM((4, 2048, 512), BF16),
            pltpu.VMEM((4, 4, 512, 256), F32),
            pltpu.VMEM((4, 4, 512, 256), F32),
            pltpu.VMEM((2, 2, 256, 1024), BF16),
            pltpu.VMEM((2, 2048, 256), BF16),
            pltpu.VMEM((4, 512, 256), F32),
            dma((5,)), dma((2, 4)), dma((4,)), dma((4,)), dma((2, 8)), dma((2, 8)), dma((24,)), dma((16,)),
            dma((1,)), dma((1,)), dma((1,)), dma((1,)), dma((1,)), dma((1,)), dma((1,)), dma((1,)),
            dma((2, 2)), dma((2,)), dma((4,)), dma((2,)),
        ],
        compiler_params=pltpu.CompilerParams(
            collective_id=0, has_side_effects=True, vmem_limit_bytes=66 * 1000 * 1000
        ),
        cost_estimate=pl.CostEstimate(flops=2 * 2048 * 2048 * 4096 * 2, bytes_accessed=100 << 20, transcendentals=0),
    )(act_blk, w_blk, grad_blk)
    return outs[0], outs[1]


def solution(mesh):
    io_spec = P(("dp", "row"), "col")
    w_spec = P("row", "col")
    return jax.shard_map(
        local_backward, mesh=mesh, in_specs=(io_spec, w_spec, io_spec), out_specs=(io_spec, io_spec), check_vma=False
    )
```

```python
import functools

import jax
import jax.numpy as jnp
from jax import lax
from jax.experimental import pallas as pl
from jax.experimental.pallas import tpu as pltpu
from jax.sharding import PartitionSpec as P

MESH = pl.DeviceIdType.MESH
F32 = jnp.float32
BF16 = jnp.bfloat16


def _tdot(a, b):
    return lax.dot_general(a, b, (((0,), (0,)), ((), ())), preferred_element_type=F32)


def _dot_t(a, b):
    return lax.dot_general(a, b, (((1,), (1,)), ((), ())), preferred_element_type=F32)


def kernel(
    x_ref, w_ref, dy_ref,
    dx_ref, dw_ref, wbuf, bufx, bufy,
    dyv, pown, poth, wv, lb,
    ld_sem, dys_r, dyy_r, xs_r, w_r, ws_r, px_r, py_r,
    s_dys, s_dyy, s_xs, s_w, s_ws, s_px, s_py, s_sum,
    wl_sem, lb_sem,
):
    row = lax.axis_index("row")
    y = lax.axis_index("col")
    x = row // 2
    c = row % 2
    is_a = x == y
    is_b = x != y
    sib = {"row": row + 1 - 2 * c}
    xn = {"row": (row + 2) % 4}
    yn = {"col": 1 - y}
    diag = {"row": (row + 2) % 4, "col": 1 - y}

    def remote(src, dst, ssem, rsem, dev):
        return pltpu.make_async_remote_copy(
            src_ref=src, dst_ref=dst, send_sem=ssem, recv_sem=rsem, device_id=dev, device_id_type=MESH
        )

    def local(src, dst, sem):
        return pltpu.make_async_copy(src, dst, sem)

    def qs(q):
        return pl.ds(q * 256, 256)

    barrier = pltpu.get_barrier_semaphore()
    for dev in (sib, xn, yn, diag):
        pl.semaphore_signal(barrier, inc=1, device_id=dev, device_id_type=MESH)
    pl.semaphore_wait(barrier, 4)

    def xo(kt):
        return dx_ref.at[:, pl.ds(pl.multiple_of(kt * 512, 512), 512)]

    def xs(kt):
        return dx_ref.at[:, pl.ds(pl.multiple_of(2048 + kt * 512, 512), 512)]

    def dw_tile(q, kt):
        return dw_ref.at[pl.ds(kt * 512, 512), pl.ds(pl.multiple_of(q * 256, 256), 256)]

    def dy_to_sib(j, q):
        src = dy_ref.at[:, qs(q)] if j == 0 else dyv.at[0, 1, :, qs(q)]
        return remote(src, dyv.at[1, j, :, qs(q)], s_dys.at[0], dys_r.at[j, q], sib)

    def dy_to_y(q):
        return remote(dy_ref.at[:, qs(q)], dyv.at[0, 1, :, qs(q)], s_dyy.at[0], dyy_r.at[q], yn)

    def x_load(kt):
        return local(x_ref.at[:, pl.ds(c * 2048 + kt * 512, 512)], xo(kt), ld_sem.at[1 + kt])

    def x_to_sib(kt):
        return remote(
            x_ref.at[:, pl.ds((1 - c) * 2048 + kt * 512, 512)], xs(kt), s_xs.at[0], xs_r.at[kt], sib
        )

    def rows(i):
        return pl.ds(i * 256, 256)

    def w_own_to_x(i):
        return remote(w_ref.at[rows(i)], wbuf.at[0, 0, rows(i)], s_w.at[0], w_r.at[0, i], xn)

    def w_to_y(i):
        return remote(w_ref.at[rows(i)], wbuf.at[0, 1, rows(i)], s_w.at[0], w_r.at[1, i], yn)

    def w_fwd(i):
        return remote(wbuf.at[0, 1, rows(i)], wbuf.at[0, 1, rows(i)], s_w.at[0], w_r.at[1, i], xn)

    def w_to_sib(j, i, own):
        src = w_ref.at[rows(i)] if own else wbuf.at[0, j, rows(i)]
        return remote(src, wbuf.at[1, j, rows(i)], s_ws.at[0], ws_r.at[j, i], sib)

    def p_to_x(g, src, q, kt):
        return remote(src.at[q, kt], bufx.at[g, q % 2, kt], s_px.at[0], px_r.at[g * 8 + (q % 2) * 4 + kt], xn)

    def p_diag(i):
        q, kt, h = i // 8, (i // 2) % 4, i % 2
        part = pl.ds(h * 256, 256)
        return remote(poth.at[q, kt, part], bufx.at[0, q, kt, part], s_py.at[0], px_r.at[i], diag)

    def p_term(q, kt):
        return remote(poth.at[q, kt], bufy.at[q, kt], s_py.at[0], py_r.at[q * 4 + kt], yn)

    def sum_to_y(q, kt):
        return remote(
            poth.at[q, kt], dw_tile(q, kt), s_sum.at[0], py_r.at[8 + (q - 2) * 4 + kt], yn
        )

    dy_load = local(dy_ref, dyv.at[0, 0], ld_sem.at[0])
    dy_to_sib(0, 0).start()
    dy_to_y(0).start()
    dy_load.start()
    x_to_sib(0).start()
    x_load(0).start()

    @pl.when(is_a)
    def _():
        for i in range(8):
            w_own_to_x(i).start()
        for q in range(1, 4):
            dy_to_y(q).start()

    @pl.when(is_b)
    def _():
        dy_to_y(1).start()
        for i in range(6):
            w_to_y(i).start()
        dy_to_y(2).start()
        for i in range(6, 8):
            w_to_y(i).start()
        dy_to_y(3).start()

    for kt in range(1, 4):
        x_to_sib(kt).start()
        x_load(kt).start()
    for q in range(1, 4):
        dy_to_sib(0, q).start()

    @pl.when(is_a)
    def _():
        for i in range(8):
            w_to_sib(0, i, True).start()

    def p_tile(dst, j, q, kt):
        dst[q, kt] = _tdot(xo(kt)[...], dyv[0, j, :, q * 256:(q + 1) * 256]) + _tdot(
            xs(kt)[...], dyv[1, j, :, q * 256:(q + 1) * 256]
        )

    dy_load.wait()
    for q in range(4):
        dy_to_sib(0, q).wait_recv()

        def own_body(kt, carry, q=q):
            if q == 0:
                x_load(kt).wait()
                x_to_sib(kt).wait_recv()
            p_tile(pown, 0, q, kt)
            if q < 2:
                @pl.when(is_b)
                def _():
                    p_to_x(0, pown, q, kt).start()
            return carry

        lax.fori_loop(0, 4, own_body, 0)

    def other_pass(q):
        dy_to_y(q).wait_recv()
        dy_to_sib(1, q).start()
        dy_to_sib(1, q).wait_recv()

        def body(kt, carry):
            p_tile(poth, 1, q, kt)
            if q < 2:
                @pl.when(is_a)
                def _():
                    p_term(q, kt).start()

                @pl.when(is_b)
                def _():
                    p_diag(8 * q + 2 * kt).start()
                    p_diag(8 * q + 2 * kt + 1).start()
            else:
                @pl.when(is_b)
                def _():
                    p_to_x(1, poth, q, kt).start()
            return carry

        lax.fori_loop(0, 4, body, 0)

    def a_final(g, t):
        q2, kt = t // 4, t % 4
        q = q2 + (0 if g == 0 else 2)
        p_to_x(g, pown, q, kt).wait_recv()
        ld = local(bufx.at[g, q2, kt], lb.at[0], lb_sem.at[0])
        ld.start()
        ld.wait()
        dw_tile(q, kt)[...] = pown[q, kt] + lb[0]

    def a_sum(q, kt):
        p_to_x(1, poth, q, kt).wait_recv()
        ld = local(bufx.at[1, q % 2, kt], lb.at[1], lb_sem.at[1])
        ld.start()
        ld.wait()
        poth[q, kt] = poth[q, kt] + lb[1]
        sum_to_y(q, kt).start()

    def w_fwd_step(i):
        w_to_y(i).wait_recv()
        w_fwd(i).start()
        w_to_sib(1, i, False).start()

    def w_loads(e, own_from_arg):
        cc, d = e % 2, e // 2
        slot = e % 2
        if own_from_arg:
            first = local(w_ref.at[rows(d)], wv.at[slot, 0], wl_sem.at[slot, 0])
        else:
            first = local(wbuf.at[cc, 0, rows(d)], wv.at[slot, 0], wl_sem.at[slot, 0])
        return first, local(wbuf.at[cc, 1, rows(d)], wv.at[slot, 1], wl_sem.at[slot, 1])

    def dx_stripe(d, cc):
        k0 = (c + cc * (1 - 2 * c)) * 2048
        cols = pl.ds(pl.multiple_of(k0 + d * 256, 256), 256)

        def body(m, carry):
            part = pl.ds(m * 512, 512)
            dx_ref[part, cols] = (
                _dot_t(dyv[0, 0, part, :], wv[cc, 0]) + _dot_t(dyv[0, 1, part, :], wv[cc, 1])
            ).astype(BF16)
            return carry

        lax.fori_loop(0, 4, body, 0)

    def start_loads(d, cc, own_from_arg):
        for cp in w_loads(2 * d + cc, own_from_arg):
            cp.start()

    def wait_loads(d, cc, own_from_arg):
        for cp in w_loads(2 * d + cc, own_from_arg):
            cp.wait()

    other_pass(0)
    other_pass(1)

    @pl.when(is_a)
    def _():
        def body(i, carry):
            w_fwd_step(i)
            a_final(0, i)
            return carry

        lax.fori_loop(0, 6, body, 0)

    other_pass(2)

    @pl.when(is_a)
    def _():
        def body(i, carry):
            w_fwd_step(i)
            a_final(0, i)
            a_sum(2, 2 * (i - 6))
            a_sum(2, 2 * (i - 6) + 1)
            return carry

        lax.fori_loop(6, 8, body, 0)

    other_pass(3)

    @pl.when(is_a)
    def _():
        def sib_wait(d):
            w_to_sib(0, d, True).wait_recv()
            w_to_sib(1, d, False).wait_recv()

        start_loads(0, 0, True)

        def body(d, carry):
            sib_wait(d)
            start_loads(d, 1, False)
            wait_loads(d, 0, True)
            dx_stripe(d, 0)

            @pl.when(d < 4)
            def _():
                a_sum(3, d)

            @pl.when(d < 7)
            def _():
                start_loads(d + 1, 0, True)

            wait_loads(d, 1, False)
            dx_stripe(d, 1)

            @pl.when(d >= 2)
            def _():
                a_final(2, d - 2)
            return carry

        lax.fori_loop(0, 8, body, 0)
        a_final(2, 6)
        a_final(2, 7)
        remote(wbuf.at[0], wbuf.at[0], s_w.at[0], w_r.at[0, 0], xn).wait_send()
        remote(bufy, bufy, s_py.at[0], py_r.at[0], yn).wait_send()
        remote(bufy, bufy, s_sum.at[0], py_r.at[0], yn).wait_send()

    @pl.when(is_b)
    def _():
        for q in range(2, 4):
            for kt in range(4):
                p_to_x(2, pown, q, kt).start()

        def own_w(i, carry):
            w_own_to_x(i).wait_recv()
            w_to_sib(0, i, False).start()
            return carry

        lax.fori_loop(0, 8, own_w, 0)

        def body(d, carry):
            w_to_y(d).wait_recv()
            w_to_sib(1, d, False).start()
            start_loads(d, 0, False)
            w_to_sib(0, d, False).wait_recv()
            w_to_sib(1, d, False).wait_recv()
            start_loads(d, 1, False)
            wait_loads(d, 0, False)
            dx_stripe(d, 0)
            wait_loads(d, 1, False)
            dx_stripe(d, 1)
            return carry

        lax.fori_loop(0, 8, body, 0)

        def fin(i, carry):
            q, kt = i // 4, i % 4
            p_term(q, kt).wait_recv()
            for h in range(2):
                part = pl.ds(h * 256, 256)
                first = local(bufy.at[q, kt, part], lb.at[h, pl.ds(0, 256)], lb_sem.at[h])
                first.start()
                p_diag(i * 2 + h).wait_recv()
                second = local(bufx.at[0, q, kt, part], lb.at[h, pl.ds(256, 256)], lb_sem.at[2 + h])
                second.start()
                first.wait()
                second.wait()
                dw_ref[pl.ds(kt * 512 + h * 256, 256), pl.ds(pl.multiple_of(q * 256, 256), 256)] = (
                    lb[h, 0:256] + lb[h, 256:512]
                )
            return carry

        lax.fori_loop(0, 8, fin, 0)
        for q in range(2, 4):
            for kt in range(4):
                sum_to_y(q, kt).wait_recv()
        remote(wbuf.at[0, 0], wbuf.at[0, 0], s_w.at[0], w_r.at[0, 0], yn).wait_send()
        remote(bufx, bufx, s_px.at[0], px_r.at[0], xn).wait_send()
        remote(bufy, bufy, s_py.at[0], py_r.at[0], yn).wait_send()

    remote(dyv.at[0], dyv.at[0], s_dys.at[0], dys_r.at[0, 0], sib).wait_send()
    remote(dyv.at[0, 0], dyv.at[0, 0], s_dyy.at[0], dyy_r.at[0], yn).wait_send()
    remote(wbuf.at[0], wbuf.at[0], s_xs.at[0], xs_r.at[0], sib).wait_send()
    remote(wbuf.at[0], wbuf.at[0], s_ws.at[0], ws_r.at[0, 0], sib).wait_send()


def store_kernel(dx_ref, dw_ref, dx_out, dw_out, sem):
    copies = []
    for i in range(4):
        part = pl.ds(i * 512, 512)
        copies.append(pltpu.make_async_copy(dx_ref.at[part], dx_out.at[part], sem.at[2 * i]))
        copies.append(pltpu.make_async_copy(dw_ref.at[part], dw_out.at[part], sem.at[2 * i + 1]))
    for cp in copies:
        cp.start()
    for cp in copies:
        cp.wait()


def local_backward(act_blk, w_blk, grad_blk):
    any_spec = pl.BlockSpec(memory_space=pl.ANY)
    vmem_spec = pl.BlockSpec(memory_space=pltpu.VMEM)
    dma = pltpu.SemaphoreType.DMA
    outs = pl.pallas_call(
        kernel,
        out_shape=(
            pltpu.VMEM((2048, 4096), BF16),
            pltpu.VMEM((2048, 1024), F32),
            jax.ShapeDtypeStruct((2, 2, 2048, 1024), BF16),
            jax.ShapeDtypeStruct((3, 2, 4, 512, 256), F32),
            jax.ShapeDtypeStruct((2, 4, 512, 256), F32),
        ),
        in_specs=[any_spec] * 3,
        out_specs=(vmem_spec, vmem_spec) + (any_spec,) * 3,
        scratch_shapes=[
            pltpu.VMEM((2, 2, 2048, 1024), BF16),
            pltpu.VMEM((4, 4, 512, 256), F32),
            pltpu.VMEM((4, 4, 512, 256), F32),
            pltpu.VMEM((2, 2, 256, 1024), BF16),
            pltpu.VMEM((2, 512, 256), F32),
            dma((5,)), dma((2, 4)), dma((4,)), dma((4,)), dma((2, 8)), dma((2, 8)), dma((24,)), dma((16,)),
            dma((1,)), dma((1,)), dma((1,)), dma((1,)), dma((1,)), dma((1,)), dma((1,)), dma((1,)),
            dma((2, 2)), dma((4,)),
        ],
        compiler_params=pltpu.CompilerParams(
            collective_id=0, has_side_effects=True, vmem_limit_bytes=39 << 20
        ),
        cost_estimate=pl.CostEstimate(flops=2 * 2048 * 2048 * 4096 * 2, bytes_accessed=100 << 20, transcendentals=0),
    )(act_blk, w_blk, grad_blk)
    return pl.pallas_call(
        store_kernel,
        out_shape=(jax.ShapeDtypeStruct((2048, 4096), BF16), jax.ShapeDtypeStruct((2048, 1024), F32)),
        in_specs=[vmem_spec, vmem_spec],
        out_specs=(any_spec, any_spec),
        scratch_shapes=[dma((8,))],
        compiler_params=pltpu.CompilerParams(vmem_limit_bytes=1 << 20),
        cost_estimate=pl.CostEstimate(flops=0, bytes_accessed=48 << 20, transcendentals=0),
    )(outs[0], outs[1])


def solution(mesh):
    io_spec = P(("dp", "row"), "col")
    w_spec = P("row", "col")
    return jax.shard_map(
        local_backward, mesh=mesh, in_specs=(io_spec, w_spec, io_spec), out_specs=(io_spec, io_spec), check_vma=False
    )
```

```python
import functools

import jax
import jax.numpy as jnp
from jax import lax
from jax.experimental import pallas as pl
from jax.experimental.pallas import tpu as pltpu
from jax.sharding import PartitionSpec as P

MESH = pl.DeviceIdType.MESH
F32 = jnp.float32
BF16 = jnp.bfloat16


def _tdot(a, b):
    return lax.dot_general(a, b, (((0,), (0,)), ((), ())), preferred_element_type=F32)


def _dot_t(a, b):
    return lax.dot_general(a, b, (((1,), (1,)), ((), ())), preferred_element_type=F32)


def kernel(
    x_ref, w_ref, dy_ref,
    dx_ref, dw_ref, wbuf, bufy,
    dyv, pown, poth, wv, land,
    ld_sem, dys_r, dyy_r, xs_r, w_r, ws_r, px_r, py_r, pf_r,
    s_dys, s_dyy, s_xs, s_w, s_ws, s_px, s_py, s_sum, wl_sem,
):
    row = lax.axis_index("row")
    y = lax.axis_index("col")
    x = row // 2
    c = row % 2
    is_a = x == y
    is_b = x != y
    sib = {"row": row + 1 - 2 * c}
    xn = {"row": (row + 2) % 4}
    yn = {"col": 1 - y}

    def remote(src, dst, ssem, rsem, dev):
        return pltpu.make_async_remote_copy(
            src_ref=src, dst_ref=dst, send_sem=ssem, recv_sem=rsem, device_id=dev, device_id_type=MESH
        )

    def local(src, dst, sem):
        return pltpu.make_async_copy(src, dst, sem)

    def qs(q):
        return pl.ds(q * 256, 256)

    def xo(k0, n):
        return dx_ref.at[:, pl.ds(pl.multiple_of(k0, 256), n)]

    def xs(k0, n):
        return dx_ref.at[:, pl.ds(pl.multiple_of(2048 + k0, 256), n)]

    def dw_tile(q, kt, r0=0, n=512):
        return dw_ref.at[pl.ds(kt * 512 + r0, n), pl.ds(pl.multiple_of(q * 256, 256), 256)]

    dy_load = local(dy_ref, dyv.at[0, 0], ld_sem.at[0])

    def x_load(kt):
        return local(x_ref.at[:, pl.ds(c * 2048 + kt * 512, 512)], xo(kt * 512, 512), ld_sem.at[1 + kt])

    def x_to_sib(kt):
        return remote(
            x_ref.at[:, pl.ds((1 - c) * 2048 + kt * 512, 512)], xs(kt * 512, 512), s_xs.at[0], xs_r.at[1 + kt], sib
        )

    def x_to_sib_half(h):
        return remote(
            x_ref.at[:, pl.ds((1 - c) * 2048 + h * 256, 256)], xs(h * 256, 256), s_xs.at[0], xs_r.at[h], sib
        )

    def dy_to_sib(j, q):
        src = dy_ref.at[:, qs(q)] if j == 0 else dyv.at[0, 1, :, qs(q)]
        return remote(src, dyv.at[1, j, :, qs(q)], s_dys.at[0], dys_r.at[j, q], sib)

    def dy_to_y(q):
        return remote(dy_ref.at[:, qs(q)], dyv.at[0, 1, :, qs(q)], s_dyy.at[0], dyy_r.at[q], yn)

    def rows(i):
        return pl.ds(i * 256, 256)

    def w_own_to_x(i):
        return remote(w_ref.at[rows(i)], wbuf.at[0, 0, rows(i)], s_w.at[0], w_r.at[0, i], xn)

    def w_to_y(i):
        return remote(w_ref.at[rows(i)], wbuf.at[0, 1, rows(i)], s_w.at[0], w_r.at[1, i], yn)

    def w_fwd(i):
        return remote(wbuf.at[0, 1, rows(i)], wbuf.at[0, 1, rows(i)], s_w.at[0], w_r.at[1, i], xn)

    def w_to_sib(j, i, own):
        src = w_ref.at[rows(i)] if own else wbuf.at[0, j, rows(i)]
        return remote(src, wbuf.at[1, j, rows(i)], s_ws.at[0], ws_r.at[j, i], sib)

    def p_own_half(q, kt, h):
        return remote(
            pown.at[q, kt, pl.ds(h * 256, 256)], dw_tile(q, kt, h * 256, 256), s_px.at[0],
            px_r.at[q * 8 + kt * 2 + h], xn,
        )

    def p_own(q, kt):
        return remote(pown.at[q, kt], dw_tile(q, kt), s_px.at[0], px_r.at[16 + (q - 2) * 4 + kt], xn)

    def p_other(q, kt):
        return remote(poth.at[q, kt], land.at[q - 2, kt], s_px.at[1], px_r.at[24 + (q - 2) * 4 + kt], xn)

    def p_trans(i):
        q, kt, r = i // 16, (i // 4) % 4, i % 4
        part = pl.ds(r * 128, 128)
        return remote(poth.at[q, kt, part], bufy.at[q, kt, part], s_py.at[0], pf_r.at[i], yn)

    def p_fwd(i):
        q, kt, r = i // 16, (i // 4) % 4, i % 4
        part = pl.ds(r * 128, 128)
        return remote(bufy.at[q, kt, part], land.at[q, kt, part], s_px.at[0], pf_r.at[i], xn)

    def p_term(q, kt):
        return remote(poth.at[q, kt], dw_tile(q, kt), s_py.at[0], py_r.at[q * 4 + kt], yn)

    def sum_to_y(q, kt):
        return remote(poth.at[q, kt], dw_tile(q, kt), s_sum.at[0], py_r.at[q * 4 + kt], yn)

    dy_load.start()
    for kt in range(4):
        x_load(kt).start()

    barrier = pltpu.get_barrier_semaphore()
    for dev in (sib, xn, yn):
        pl.semaphore_signal(barrier, inc=1, device_id=dev, device_id_type=MESH)
    pl.semaphore_wait(barrier, 3)

    dy_to_sib(0, 0).start()
    x_to_sib_half(0).start()
    dy_to_y(0).start()
    dy_to_y(1).start()

    @pl.when(is_a)
    def _():
        for i in range(8):
            w_own_to_x(i).start()
        for q in range(2, 4):
            dy_to_y(q).start()

    @pl.when(is_b)
    def _():
        for i in range(8):
            w_to_y(i).start()
        dy_to_y(2).start()

    x_to_sib_half(1).start()
    for kt in range(1, 4):
        x_to_sib(kt).start()
    for q in range(1, 4):
        dy_to_sib(0, q).start()

    @pl.when(is_a)
    def _():
        for i in range(8):
            w_to_sib(0, i, True).start()

    def p_part(j, q, k0, n):
        return _tdot(xo(k0, n)[...], dyv[0, j, :, q * 256:(q + 1) * 256]) + _tdot(
            xs(k0, n)[...], dyv[1, j, :, q * 256:(q + 1) * 256]
        )

    dy_load.wait()
    for q in range(4):
        dy_to_sib(0, q).wait_recv()
        if q == 0:
            x_load(0).wait()
            for h in range(2):
                x_to_sib_half(h).wait_recv()
                pown[0, 0, h * 256:(h + 1) * 256] = p_part(0, 0, h * 256, 256)

                @pl.when(is_b)
                def _(h=h):
                    p_own_half(0, 0, h).start()

        def own_body(kt, carry, q=q):
            if q == 0:
                x_load(kt).wait()
                x_to_sib(kt).wait_recv()
            for h in range(2):
                pown[q, kt, h * 256:(h + 1) * 256] = p_part(0, q, kt * 512 + h * 256, 256)
            if q < 2:
                @pl.when(is_b)
                def _():
                    p_own_half(q, kt, 0).start()
                    p_own_half(q, kt, 1).start()
            return carry

        lax.fori_loop(1 if q == 0 else 0, 4, own_body, 0)

    def other_tile(q, kt):
        for h in range(2):
            poth[q, kt, h * 256:(h + 1) * 256] = p_part(1, q, kt * 512 + h * 256, 256)

    def trans_tile(q, kt):
        for r in range(4):
            p_trans(16 * q + 4 * kt + r).start()

    def dy_in(q):
        dy_to_y(q).wait_recv()
        dy_to_sib(1, q).start()

    def other_pass(q):
        dy_in(q)
        dy_to_sib(1, q).wait_recv()

        def body(kt, carry):
            other_tile(q, kt)
            if q < 2:
                @pl.when(is_a)
                def _():
                    p_term(q, kt).start()

                @pl.when(is_b)
                def _():
                    trans_tile(q, kt)
                    if q == 0:
                        @pl.when(kt == 0)
                        def _():
                            dy_to_y(3).start()
            else:
                @pl.when(is_b)
                def _():
                    p_other(q, kt).start()
            return carry

        lax.fori_loop(0, 4, body, 0)

    def w_loads(d, cc, own_from_arg):
        if own_from_arg:
            first = local(w_ref.at[rows(d)], wv.at[cc, 0], wl_sem.at[cc, 0])
        else:
            first = local(wbuf.at[cc, 0, rows(d)], wv.at[cc, 0], wl_sem.at[cc, 0])
        return first, local(wbuf.at[cc, 1, rows(d)], wv.at[cc, 1], wl_sem.at[cc, 1])

    def start_loads(d, cc, own_from_arg):
        for cp in w_loads(d, cc, own_from_arg):
            cp.start()

    def wait_loads(d, cc, own_from_arg):
        for cp in w_loads(d, cc, own_from_arg):
            cp.wait()

    def dx_stripe(d, cc):
        k0 = (c + cc * (1 - 2 * c)) * 2048
        cols = pl.ds(pl.multiple_of(k0 + d * 256, 256), 256)

        def body(m, carry):
            part = pl.ds(m * 512, 512)
            dx_ref[part, cols] = (
                _dot_t(dyv[0, 0, part, :], wv[cc, 0]) + _dot_t(dyv[0, 1, part, :], wv[cc, 1])
            ).astype(BF16)
            return carry

        lax.fori_loop(0, 4, body, 0)

    def pair_wait(d, own_from_arg):
        w_to_sib(0, d, own_from_arg).wait_recv()
        w_to_sib(1, d, False).wait_recv()

    other_pass(0)
    other_pass(1)

    @pl.when(is_a)
    def _():
        def add(q, kt):
            tile = dw_tile(q, kt)
            tile[...] = tile[...] + pown[q, kt]

        def final_early(t):
            q, kt = t // 4, t % 4
            for h in range(2):
                p_own_half(q, kt, h).wait_recv()
            add(q, kt)

        def final_late(t):
            q, kt = 2 + t // 4, t % 4
            p_own(q, kt).wait_recv()
            add(q, kt)

        def a_sum(q, kt):
            p_other(q, kt).wait_recv()
            poth[q, kt] = poth[q, kt] + land[q - 2, kt]
            sum_to_y(q, kt).start()

        def fwd(i):
            p_trans(i).wait_recv()
            p_fwd(i).start()

        def early(i, carry):
            w_to_y(i).wait_recv()
            w_fwd(i).start()
            w_to_sib(1, i, False).start()
            final_early(i)
            return carry

        lax.fori_loop(0, 8, early, 0)

        dy_in(2)
        dy_to_sib(1, 2).wait_recv()

        def q2_body(kt, carry):
            other_tile(2, kt)
            a_sum(2, kt)
            fwd(kt)
            return carry

        lax.fori_loop(0, 4, q2_body, 0)

        pair_wait(0, True)
        start_loads(0, 0, True)
        dy_in(3)
        fwd(4)
        dy_to_sib(1, 3).wait_recv()

        def q3_body(kt, carry):
            other_tile(3, kt)

            @pl.when(kt < 3)
            def _():
                fwd(5 + kt)
            return carry

        lax.fori_loop(0, 4, q3_body, 0)

        def late(d, carry):
            @pl.when(d < 6)
            def _():
                fwd(4 * d + 8)
            start_loads(d, 1, False)
            wait_loads(d, 0, True)
            dx_stripe(d, 0)

            @pl.when(d < 6)
            def _():
                fwd(4 * d + 9)

            @pl.when(d < 7)
            def _():
                pair_wait(d + 1, True)
                start_loads(d + 1, 0, True)

            @pl.when(d < 4)
            def _():
                a_sum(3, d)

            @pl.when(d < 6)
            def _():
                fwd(4 * d + 10)
            wait_loads(d, 1, False)
            dx_stripe(d, 1)

            @pl.when(d < 6)
            def _():
                fwd(4 * d + 11)
                final_late(d)
            return carry

        lax.fori_loop(0, 8, late, 0)
        final_late(6)
        final_late(7)
        remote(wbuf.at[0], wbuf.at[0], s_w.at[0], w_r.at[0, 0], xn).wait_send()
        remote(land, land, s_px.at[0], px_r.at[0], xn).wait_send()
        remote(land, land, s_py.at[0], py_r.at[0], yn).wait_send()
        remote(land, land, s_sum.at[0], py_r.at[0], yn).wait_send()

    @pl.when(is_b)
    def _():
        other_pass(2)
        other_pass(3)
        for q in range(2, 4):
            for kt in range(4):
                p_own(q, kt).start()

        def own_w(i, carry):
            w_own_to_x(i).wait_recv()
            w_to_sib(0, i, False).start()
            return carry

        lax.fori_loop(0, 8, own_w, 0)

        def stripes(d, carry):
            w_to_y(d).wait_recv()
            w_to_sib(1, d, False).start()
            start_loads(d, 0, False)
            pair_wait(d, False)
            start_loads(d, 1, False)
            wait_loads(d, 0, False)
            dx_stripe(d, 0)
            wait_loads(d, 1, False)
            dx_stripe(d, 1)
            return carry

        lax.fori_loop(0, 8, stripes, 0)

        def fin(i, carry):
            q, kt, r = i // 16, (i // 4) % 4, i % 4

            @pl.when(r == 0)
            def _():
                p_term(q, kt).wait_recv()
            p_fwd(i).wait_recv()
            tile = dw_tile(q, kt, r * 128, 128)
            tile[...] = tile[...] + land[q, kt, pl.ds(r * 128, 128)]
            return carry

        lax.fori_loop(0, 32, fin, 0)
        for q in range(2, 4):
            for kt in range(4):
                sum_to_y(q, kt).wait_recv()
        remote(wbuf.at[0, 0], wbuf.at[0, 0], s_w.at[0], w_r.at[0, 0], yn).wait_send()
        remote(pown, pown, s_px.at[0], px_r.at[0], xn).wait_send()
        remote(land, land, s_px.at[1], px_r.at[0], xn).wait_send()
        remote(land, land, s_py.at[0], py_r.at[0], yn).wait_send()

    remote(dyv.at[0], dyv.at[0], s_dys.at[0], dys_r.at[0, 0], sib).wait_send()
    remote(dyv.at[0, 0], dyv.at[0, 0], s_dyy.at[0], dyy_r.at[0], yn).wait_send()
    remote(wbuf.at[0], wbuf.at[0], s_xs.at[0], xs_r.at[0], sib).wait_send()
    remote(wbuf.at[0], wbuf.at[0], s_ws.at[0], ws_r.at[0, 0], sib).wait_send()


def store_kernel(dx_ref, dw_ref, dx_out, dw_out, sem):
    copies = []
    for i in range(4):
        part = pl.ds(i * 512, 512)
        copies.append(pltpu.make_async_copy(dx_ref.at[part], dx_out.at[part], sem.at[2 * i]))
        copies.append(pltpu.make_async_copy(dw_ref.at[part], dw_out.at[part], sem.at[2 * i + 1]))
    for cp in copies:
        cp.start()
    for cp in copies:
        cp.wait()


def local_backward(act_blk, w_blk, grad_blk):
    any_spec = pl.BlockSpec(memory_space=pl.ANY)
    vmem_spec = pl.BlockSpec(memory_space=pltpu.VMEM)
    dma = pltpu.SemaphoreType.DMA
    outs = pl.pallas_call(
        kernel,
        out_shape=(
            pltpu.VMEM((2048, 4096), BF16),
            pltpu.VMEM((2048, 1024), F32),
            jax.ShapeDtypeStruct((2, 2, 2048, 1024), BF16),
            jax.ShapeDtypeStruct((2, 4, 512, 256), F32),
        ),
        in_specs=[any_spec] * 3,
        out_specs=(vmem_spec, vmem_spec) + (any_spec,) * 2,
        scratch_shapes=[
            pltpu.VMEM((2, 2, 2048, 1024), BF16),
            pltpu.VMEM((4, 4, 512, 256), F32),
            pltpu.VMEM((4, 4, 512, 256), F32),
            pltpu.VMEM((2, 2, 256, 1024), BF16),
            pltpu.VMEM((2, 4, 512, 256), F32),
            dma((5,)), dma((2, 4)), dma((4,)), dma((5,)), dma((2, 8)), dma((2, 8)), dma((32,)), dma((16,)), dma((32,)),
            dma((1,)), dma((1,)), dma((1,)), dma((1,)), dma((1,)), dma((2,)), dma((1,)), dma((1,)), dma((2, 2)),
        ],
        compiler_params=pltpu.CompilerParams(
            collective_id=0, has_side_effects=True, vmem_limit_bytes=41_800_000
        ),
        cost_estimate=pl.CostEstimate(flops=2 * 2048 * 2048 * 4096 * 2, bytes_accessed=100 << 20, transcendentals=0),
    )(act_blk, w_blk, grad_blk)
    return pl.pallas_call(
        store_kernel,
        out_shape=(jax.ShapeDtypeStruct((2048, 4096), BF16), jax.ShapeDtypeStruct((2048, 1024), F32)),
        in_specs=[vmem_spec, vmem_spec],
        out_specs=(any_spec, any_spec),
        scratch_shapes=[dma((8,))],
        compiler_params=pltpu.CompilerParams(vmem_limit_bytes=1 << 20),
        cost_estimate=pl.CostEstimate(flops=0, bytes_accessed=48 << 20, transcendentals=0),
    )(outs[0], outs[1])


def solution(mesh):
    io_spec = P(("dp", "row"), "col")
    w_spec = P("row", "col")
    return jax.shard_map(
        local_backward, mesh=mesh, in_specs=(io_spec, w_spec, io_spec), out_specs=(io_spec, io_spec), check_vma=False
    )
```

```python
import functools

import jax
import jax.numpy as jnp
from jax import lax
from jax.experimental import pallas as pl
from jax.experimental.pallas import tpu as pltpu
from jax.sharding import PartitionSpec as P

MESH = pl.DeviceIdType.MESH
F32 = jnp.float32
BF16 = jnp.bfloat16


def _tdot(a, b):
    return lax.dot_general(a, b, (((0,), (0,)), ((), ())), preferred_element_type=F32)


def _dot_t(a, b):
    return lax.dot_general(a, b, (((1,), (1,)), ((), ())), preferred_element_type=F32)


def kernel(
    x_ref, w_ref, dy_ref,
    dx_ref, dw_ref, wbuf, bufy,
    dyv, pown, poth, wv, land,
    ld_sem, dys_r, dyy_r, xs_r, w_r, wp_r, ws_r, px_r, py_r, pf_r,
    s_dys, s_dyy, s_xs, s_w, s_ws, s_px, s_py, s_sum, wl_sem,
):
    row = lax.axis_index("row")
    y = lax.axis_index("col")
    x = row // 2
    c = row % 2
    is_a = x == y
    is_b = x != y
    sib = {"row": row + 1 - 2 * c}
    xn = {"row": (row + 2) % 4}
    yn = {"col": 1 - y}

    def remote(src, dst, ssem, rsem, dev):
        return pltpu.make_async_remote_copy(
            src_ref=src, dst_ref=dst, send_sem=ssem, recv_sem=rsem, device_id=dev, device_id_type=MESH
        )

    def local(src, dst, sem):
        return pltpu.make_async_copy(src, dst, sem)

    def qs(q):
        return pl.ds(q * 256, 256)

    def xo(k0, n):
        return dx_ref.at[:, pl.ds(pl.multiple_of(k0, 128), n)]

    def xs(k0, n):
        return dx_ref.at[:, pl.ds(pl.multiple_of(2048 + k0, 128), n)]

    def dw_tile(q, kt, r0=0, n=512):
        return dw_ref.at[pl.ds(kt * 512 + r0, n), pl.ds(pl.multiple_of(q * 256, 256), 256)]

    dy_load = local(dy_ref, dyv.at[0, 0], ld_sem.at[0])

    def x_load(kt):
        return local(x_ref.at[:, pl.ds(c * 2048 + kt * 512, 512)], xo(kt * 512, 512), ld_sem.at[1 + kt])

    def x_to_sib(kt):
        return remote(
            x_ref.at[:, pl.ds((1 - c) * 2048 + kt * 512, 512)], xs(kt * 512, 512), s_xs.at[0], xs_r.at[kt], sib
        )

    FIRST = ((0, 128), (128, 128), (256, 256))

    def x_to_sib_part(i):
        k0, n = FIRST[i]
        return remote(
            x_ref.at[:, pl.ds((1 - c) * 2048 + k0, n)], xs(k0, n), s_xs.at[0], xs_r.at[4 + i], sib
        )

    def dy_to_sib(j, q):
        src = dy_ref.at[:, qs(q)] if j == 0 else dyv.at[0, 1, :, qs(q)]
        return remote(src, dyv.at[1, j, :, qs(q)], s_dys.at[0], dys_r.at[j, q], sib)

    def dy_to_y(q):
        return remote(dy_ref.at[:, qs(q)], dyv.at[0, 1, :, qs(q)], s_dyy.at[0], dyy_r.at[q], yn)

    def rows(i):
        return pl.ds(i * 256, 256)

    def w_own_to_x(i):
        return remote(w_ref.at[rows(i)], wbuf.at[0, 0, rows(i)], s_w.at[0], w_r.at[0, i], xn)

    def w_to_y(i):
        return remote(w_ref.at[rows(i)], wbuf.at[0, 1, rows(i)], s_w.at[0], w_r.at[1, i], yn)

    def w_part(p):
        return pl.ds(1024 + p * 64, 64)

    def w_to_y_part(p):
        return remote(w_ref.at[w_part(p)], wbuf.at[0, 1, w_part(p)], s_w.at[0], wp_r.at[p], yn)

    def w_fwd_part(p):
        return remote(wbuf.at[0, 1, w_part(p)], wbuf.at[0, 1, w_part(p)], s_w.at[0], wp_r.at[p], xn)

    def w_fwd(i):
        return remote(wbuf.at[0, 1, rows(i)], wbuf.at[0, 1, rows(i)], s_w.at[0], w_r.at[1, i], xn)

    def w_to_sib(j, i, own):
        src = w_ref.at[rows(i)] if own else wbuf.at[0, j, rows(i)]
        return remote(src, wbuf.at[1, j, rows(i)], s_ws.at[0], ws_r.at[j, i], sib)

    def p_own_half(q, kt, h):
        return remote(
            pown.at[q, kt, pl.ds(h * 256, 256)], dw_tile(q, kt, h * 256, 256), s_px.at[0],
            px_r.at[q * 8 + kt * 2 + h], xn,
        )

    def p_own_first(i):
        k0, n = FIRST[i]
        return remote(
            pown.at[0, 0, pl.ds(k0, n)], dw_tile(0, 0, k0, n), s_px.at[0], px_r.at[(0, 32, 1)[i]], xn
        )

    def p_own(q, kt):
        return remote(pown.at[q, kt], dw_tile(q, kt), s_px.at[0], px_r.at[16 + (q - 2) * 4 + kt], xn)

    def p_other(q, kt):
        return remote(poth.at[q, kt], land.at[q - 2, kt], s_px.at[1], px_r.at[24 + (q - 2) * 4 + kt], xn)

    def p_trans(i):
        q, kt, r = i // 16, (i // 4) % 4, i % 4
        part = pl.ds(r * 128, 128)
        return remote(poth.at[q, kt, part], bufy.at[q, kt, part], s_py.at[0], pf_r.at[i], yn)

    def p_fwd(i):
        q, kt, r = i // 16, (i // 4) % 4, i % 4
        part = pl.ds(r * 128, 128)
        return remote(bufy.at[q, kt, part], land.at[q, kt, part], s_px.at[0], pf_r.at[i], xn)

    def p_term(q, kt):
        return remote(poth.at[q, kt], dw_tile(q, kt), s_py.at[0], py_r.at[q * 4 + kt], yn)

    def sum_to_y(q, kt):
        return remote(poth.at[q, kt], dw_tile(q, kt), s_sum.at[0], py_r.at[q * 4 + kt], yn)

    dy_load.start()
    for kt in range(4):
        x_load(kt).start()

    barrier = pltpu.get_barrier_semaphore()
    for dev in (sib, xn, yn):
        pl.semaphore_signal(barrier, inc=1, device_id=dev, device_id_type=MESH)
    pl.semaphore_wait(barrier, 3)

    dy_to_sib(0, 0).start()
    x_to_sib_part(0).start()
    dy_to_y(0).start()
    dy_to_y(1).start()

    @pl.when(is_a)
    def _():
        for i in range(8):
            w_own_to_x(i).start()
        for q in range(2, 4):
            dy_to_y(q).start()

    @pl.when(is_b)
    def _():
        for i in range(4):
            w_to_y(i).start()
        for q in range(2, 4):
            dy_to_y(q).start()
        for p in range(16):
            w_to_y_part(p).start()

    x_to_sib_part(1).start()
    x_to_sib_part(2).start()
    for kt in range(1, 4):
        x_to_sib(kt).start()
    for q in range(1, 4):
        dy_to_sib(0, q).start()

    @pl.when(is_a)
    def _():
        for i in range(8):
            w_to_sib(0, i, True).start()

    def p_part(j, q, k0, n):
        def term(t, acc):
            part = pl.ds(t * 1024, 1024)
            cols = pl.ds(pl.multiple_of(k0, 128), n)
            both = pl.ds(pl.multiple_of(2048 + k0, 128), n)
            dy = pl.ds(q * 256, 256)
            return acc + _tdot(dx_ref[part, cols], dyv[0, j, part, dy]) + _tdot(
                dx_ref[part, both], dyv[1, j, part, dy]
            )

        return lax.fori_loop(0, 2, term, jnp.zeros((n, 256), F32), unroll=True)

    dy_load.wait()
    for q in range(4):
        dy_to_sib(0, q).wait_recv()
        if q == 0:
            x_load(0).wait()
            for i, (k0, n) in enumerate(FIRST):
                x_to_sib_part(i).wait_recv()
                pown[0, 0, k0:k0 + n] = p_part(0, 0, k0, n)

                @pl.when(is_b)
                def _(i=i):
                    p_own_first(i).start()

        def own_body(kt, carry, q=q):
            if q == 0:
                x_load(kt).wait()
                x_to_sib(kt).wait_recv()

            def half(h, carry):
                pown[q, kt, pl.ds(h * 256, 256)] = p_part(0, q, kt * 512 + h * 256, 256)
                return carry

            lax.fori_loop(0, 2, half, 0)
            if q < 2:
                @pl.when(is_b)
                def _():
                    p_own_half(q, kt, 0).start()
                    p_own_half(q, kt, 1).start()
            return carry

        lax.fori_loop(1 if q == 0 else 0, 4, own_body, 0)

    def other_tile(q, kt):
        def half(h, carry):
            poth[q, kt, pl.ds(h * 256, 256)] = p_part(1, q, kt * 512 + h * 256, 256)
            return carry

        lax.fori_loop(0, 2, half, 0)

    def trans_tile(q, kt):
        for r in range(4):
            p_trans(16 * q + 4 * kt + r).start()

    def dy_in(q):
        dy_to_y(q).wait_recv()
        dy_to_sib(1, q).start()

    def other_pass(q):
        dy_in(q)
        dy_to_sib(1, q).wait_recv()

        def body(kt, carry):
            other_tile(q, kt)
            if q < 2:
                @pl.when(is_a)
                def _():
                    p_term(q, kt).start()

                @pl.when(is_b)
                def _():
                    trans_tile(q, kt)
            else:
                @pl.when(is_b)
                def _():
                    p_other(q, kt).start()
            return carry

        lax.fori_loop(0, 4, body, 0)

    def w_loads(d, cc, own_from_arg):
        if own_from_arg:
            first = local(w_ref.at[rows(d)], wv.at[cc, 0], wl_sem.at[cc, 0])
        else:
            first = local(wbuf.at[cc, 0, rows(d)], wv.at[cc, 0], wl_sem.at[cc, 0])
        return first, local(wbuf.at[cc, 1, rows(d)], wv.at[cc, 1], wl_sem.at[cc, 1])

    def start_loads(d, cc, own_from_arg):
        for cp in w_loads(d, cc, own_from_arg):
            cp.start()

    def wait_loads(d, cc, own_from_arg):
        for cp in w_loads(d, cc, own_from_arg):
            cp.wait()

    def dx_stripe(d, cc, lo=0, hi=4):
        k0 = (c + cc * (1 - 2 * c)) * 2048
        cols = pl.ds(pl.multiple_of(k0 + d * 256, 256), 256)

        def body(m, carry):
            part = pl.ds(m * 512, 512)
            dx_ref[part, cols] = (
                _dot_t(dyv[0, 0, part, :], wv[cc, 0]) + _dot_t(dyv[0, 1, part, :], wv[cc, 1])
            ).astype(BF16)
            return carry

        lax.fori_loop(lo, hi, body, 0)

    def pair_wait(d, own_from_arg):
        w_to_sib(0, d, own_from_arg).wait_recv()
        w_to_sib(1, d, False).wait_recv()

    other_pass(0)
    other_pass(1)

    @pl.when(is_a)
    def _():
        def add(q, kt):
            tile = dw_tile(q, kt)
            tile[...] = tile[...] + pown[q, kt]

        def final_early(t):
            q, kt = t // 4, t % 4

            @pl.when(t == 0)
            def _():
                for i in range(3):
                    p_own_first(i).wait_recv()

            @pl.when(t > 0)
            def _():
                for h in range(2):
                    p_own_half(q, kt, h).wait_recv()
            add(q, kt)

        def final_late(t):
            q, kt = 2 + t // 4, t % 4
            p_own(q, kt).wait_recv()
            add(q, kt)

        def a_sum(q, kt):
            p_other(q, kt).wait_recv()
            poth[q, kt] = poth[q, kt] + land[q - 2, kt]
            sum_to_y(q, kt).start()

        def fwd(i):
            p_trans(i).wait_recv()
            p_fwd(i).start()

        def early(i, carry):
            w_to_y(i).wait_recv()
            w_fwd(i).start()
            w_to_sib(1, i, False).start()
            final_early(i)
            return carry

        lax.fori_loop(0, 4, early, 0)

        dy_in(2)
        dy_to_sib(1, 2).wait_recv()

        def q2_body(kt, carry):
            other_tile(2, kt)
            final_early(4 + kt)
            return carry

        lax.fori_loop(0, 4, q2_body, 0)
        start_loads(0, 0, True)
        dy_in(3)

        def step(i, carry):
            @pl.when(i < 16)
            def _():
                w_to_y_part(i).wait_recv()
                w_fwd_part(i).start()

                @pl.when(i % 4 == 3)
                def _():
                    w_to_sib(1, 4 + i // 4, False).start()

            @pl.when(i >= 16)
            def _():
                fwd(i - 16)

            @pl.when(i == 0)
            def _():
                dy_to_sib(1, 3).wait_recv()

            @pl.when(i < 4)
            def _():
                other_tile(3, i)

            @pl.when(jnp.logical_and(i >= 4, i < 36))
            def _():
                e = (i - 4) // 2
                d, cc = e // 2, e % 2
                odd = i % 2

                @pl.when(odd == 0)
                def _():
                    @pl.when(cc == 0)
                    def _():
                        pair_wait(d, True)
                        start_loads(d, 1, False)
                        wait_loads(d, 0, True)

                    @pl.when(cc == 1)
                    def _():
                        @pl.when(d < 7)
                        def _():
                            start_loads(d + 1, 0, True)
                        wait_loads(d, 1, False)

                dx_stripe(d, cc, 2 * odd, 2 * odd + 2)

            @pl.when(jnp.logical_and(i < 8, i % 2 == 1))
            def _():
                a_sum(2, i // 2)

            @pl.when(jnp.logical_and(jnp.logical_and(i >= 10, i < 26), i % 4 == 2))
            def _():
                a_sum(3, (i - 10) // 4)

            @pl.when(jnp.logical_and(i >= 26, i % 4 == 2))
            def _():
                final_late((i - 26) // 4)
            return carry

        lax.fori_loop(0, 48, step, 0)
        final_late(6)
        final_late(7)
        remote(wbuf.at[0], wbuf.at[0], s_w.at[0], w_r.at[0, 0], xn).wait_send()
        remote(land, land, s_px.at[0], px_r.at[0], xn).wait_send()
        remote(land, land, s_py.at[0], py_r.at[0], yn).wait_send()
        remote(land, land, s_sum.at[0], py_r.at[0], yn).wait_send()

    @pl.when(is_b)
    def _():
        other_pass(2)
        other_pass(3)
        for q in range(2, 4):
            for kt in range(4):
                p_own(q, kt).start()

        def own_w(i, carry):
            w_own_to_x(i).wait_recv()
            w_to_sib(0, i, False).start()
            return carry

        lax.fori_loop(0, 8, own_w, 0)

        def stripes(d, carry):
            @pl.when(d < 4)
            def _():
                w_to_y(d).wait_recv()

            @pl.when(d >= 4)
            def _():
                for p in range(4):
                    w_to_y_part(4 * (d - 4) + p).wait_recv()
            w_to_sib(1, d, False).start()
            start_loads(d, 0, False)
            pair_wait(d, False)
            start_loads(d, 1, False)
            wait_loads(d, 0, False)
            dx_stripe(d, 0)
            wait_loads(d, 1, False)
            dx_stripe(d, 1)
            return carry

        lax.fori_loop(0, 8, stripes, 0)

        def fin(i, carry):
            q, kt, r = i // 16, (i // 4) % 4, i % 4

            @pl.when(r == 0)
            def _():
                p_term(q, kt).wait_recv()
            p_fwd(i).wait_recv()
            tile = dw_tile(q, kt, r * 128, 128)
            tile[...] = tile[...] + land[q, kt, pl.ds(r * 128, 128)]
            return carry

        lax.fori_loop(0, 32, fin, 0)
        for q in range(2, 4):
            for kt in range(4):
                sum_to_y(q, kt).wait_recv()
        remote(wbuf.at[0, 0], wbuf.at[0, 0], s_w.at[0], w_r.at[0, 0], yn).wait_send()
        remote(pown, pown, s_px.at[0], px_r.at[0], xn).wait_send()
        remote(land, land, s_px.at[1], px_r.at[0], xn).wait_send()
        remote(land, land, s_py.at[0], py_r.at[0], yn).wait_send()

    remote(dyv.at[0], dyv.at[0], s_dys.at[0], dys_r.at[0, 0], sib).wait_send()
    remote(dyv.at[0, 0], dyv.at[0, 0], s_dyy.at[0], dyy_r.at[0], yn).wait_send()
    remote(wbuf.at[0], wbuf.at[0], s_xs.at[0], xs_r.at[0], sib).wait_send()
    remote(wbuf.at[0], wbuf.at[0], s_ws.at[0], ws_r.at[0, 0], sib).wait_send()


def store_kernel(dx_ref, dw_ref, dx_out, dw_out, sem):
    copies = []
    for i in range(4):
        part = pl.ds(i * 512, 512)
        copies.append(pltpu.make_async_copy(dx_ref.at[part], dx_out.at[part], sem.at[2 * i]))
        copies.append(pltpu.make_async_copy(dw_ref.at[part], dw_out.at[part], sem.at[2 * i + 1]))
    for cp in copies:
        cp.start()
    for cp in copies:
        cp.wait()


def local_backward(act_blk, w_blk, grad_blk):
    any_spec = pl.BlockSpec(memory_space=pl.ANY)
    vmem_spec = pl.BlockSpec(memory_space=pltpu.VMEM)
    dma = pltpu.SemaphoreType.DMA
    outs = pl.pallas_call(
        kernel,
        out_shape=(
            pltpu.VMEM((2048, 4096), BF16),
            pltpu.VMEM((2048, 1024), F32),
            jax.ShapeDtypeStruct((2, 2, 2048, 1024), BF16),
            jax.ShapeDtypeStruct((2, 4, 512, 256), F32),
        ),
        in_specs=[any_spec] * 3,
        out_specs=(vmem_spec, vmem_spec) + (any_spec,) * 2,
        scratch_shapes=[
            pltpu.VMEM((2, 2, 2048, 1024), BF16),
            pltpu.VMEM((4, 4, 512, 256), F32),
            pltpu.VMEM((4, 4, 512, 256), F32),
            pltpu.VMEM((2, 2, 256, 1024), BF16),
            pltpu.VMEM((2, 4, 512, 256), F32),
            dma((5,)), dma((2, 4)), dma((4,)), dma((7,)), dma((2, 8)), dma((16,)), dma((2, 8)), dma((33,)), dma((16,)),
            dma((32,)),
            dma((1,)), dma((1,)), dma((1,)), dma((1,)), dma((1,)), dma((2,)), dma((1,)), dma((1,)), dma((2, 2)),
        ],
        compiler_params=pltpu.CompilerParams(
            collective_id=0, has_side_effects=True, vmem_limit_bytes=41_800_000
        ),
        cost_estimate=pl.CostEstimate(flops=2 * 2048 * 2048 * 4096 * 2, bytes_accessed=100 << 20, transcendentals=0),
    )(act_blk, w_blk, grad_blk)
    return pl.pallas_call(
        store_kernel,
        out_shape=(jax.ShapeDtypeStruct((2048, 4096), BF16), jax.ShapeDtypeStruct((2048, 1024), F32)),
        in_specs=[vmem_spec, vmem_spec],
        out_specs=(any_spec, any_spec),
        scratch_shapes=[dma((8,))],
        compiler_params=pltpu.CompilerParams(vmem_limit_bytes=1 << 20),
        cost_estimate=pl.CostEstimate(flops=0, bytes_accessed=48 << 20, transcendentals=0),
    )(outs[0], outs[1])


def solution(mesh):
    io_spec = P(("dp", "row"), "col")
    w_spec = P("row", "col")
    return jax.shard_map(
        local_backward, mesh=mesh, in_specs=(io_spec, w_spec, io_spec), out_specs=(io_spec, io_spec), check_vma=False
    )
```

```python
import functools

import jax
import jax.numpy as jnp
from jax import lax
from jax.experimental import pallas as pl
from jax.experimental.pallas import tpu as pltpu
from jax.sharding import PartitionSpec as P

MESH = pl.DeviceIdType.MESH
F32 = jnp.float32
BF16 = jnp.bfloat16


def _tdot(a, b):
    return lax.dot_general(a, b, (((0,), (0,)), ((), ())), preferred_element_type=F32)


def _dot_t(a, b):
    return lax.dot_general(a, b, (((1,), (1,)), ((), ())), preferred_element_type=F32)


def kernel(
    x_ref, w_ref, dy_ref,
    dx_ref, dw_ref, wbuf, bufy, tail,
    dyv, pown, poth, wv, land,
    ld_sem, dys_r, dyy_r, xs_r, w_r, wp_r, ws_r, px_r, py_r, pf_r,
    s_dys, s_dyy, s_xs, s_w, s_ws, s_px, s_py, s_sum, wl_sem, tail_sem,
):
    row = lax.axis_index("row")
    y = lax.axis_index("col")
    x = row // 2
    c = row % 2
    is_a = x == y
    is_b = x != y
    sib = {"row": row + 1 - 2 * c}
    xn = {"row": (row + 2) % 4}
    yn = {"col": 1 - y}

    def remote(src, dst, ssem, rsem, dev):
        return pltpu.make_async_remote_copy(
            src_ref=src, dst_ref=dst, send_sem=ssem, recv_sem=rsem, device_id=dev, device_id_type=MESH
        )

    def local(src, dst, sem):
        return pltpu.make_async_copy(src, dst, sem)

    def qs(q):
        return pl.ds(q * 256, 256)

    def xo(k0, n):
        return dx_ref.at[:, pl.ds(pl.multiple_of(k0, 128), n)]

    def xs(k0, n):
        return dx_ref.at[:, pl.ds(pl.multiple_of(2048 + k0, 128), n)]

    def dw_tile(q, kt, r0=0, n=512):
        return dw_ref.at[pl.ds(kt * 512 + r0, n), pl.ds(pl.multiple_of(q * 256, 256), 256)]

    dy_load = local(dy_ref, dyv.at[0, 0], ld_sem.at[0])

    def x_load(kt):
        return local(x_ref.at[:, pl.ds(c * 2048 + kt * 512, 512)], xo(kt * 512, 512), ld_sem.at[1 + kt])

    def x_to_sib(kt):
        return remote(
            x_ref.at[:, pl.ds((1 - c) * 2048 + kt * 512, 512)], xs(kt * 512, 512), s_xs.at[0], xs_r.at[kt], sib
        )

    FIRST = ((0, 128), (128, 128), (256, 256))

    def x_to_sib_part(i):
        k0, n = FIRST[i]
        return remote(
            x_ref.at[:, pl.ds((1 - c) * 2048 + k0, n)], xs(k0, n), s_xs.at[0], xs_r.at[4 + i], sib
        )

    def dy_to_sib(j, q):
        src = dy_ref.at[:, qs(q)] if j == 0 else dyv.at[0, 1, :, qs(q)]
        return remote(src, dyv.at[1, j, :, qs(q)], s_dys.at[0], dys_r.at[j, q], sib)

    def dy_to_y(q):
        return remote(dy_ref.at[:, qs(q)], dyv.at[0, 1, :, qs(q)], s_dyy.at[0], dyy_r.at[q], yn)

    def rows(i):
        return pl.ds(i * 256, 256)

    def w_own_to_x(i):
        return remote(w_ref.at[rows(i)], wbuf.at[0, 0, rows(i)], s_w.at[0], w_r.at[0, i], xn)

    def w_to_y(i):
        return remote(w_ref.at[rows(i)], wbuf.at[0, 1, rows(i)], s_w.at[0], w_r.at[1, i], yn)

    def w_part(p):
        return pl.ds(1024 + p * 64, 64)

    def w_to_y_part(p):
        return remote(w_ref.at[w_part(p)], wbuf.at[0, 1, w_part(p)], s_w.at[0], wp_r.at[p], yn)

    def w_fwd_part(p):
        return remote(wbuf.at[0, 1, w_part(p)], wbuf.at[0, 1, w_part(p)], s_w.at[0], wp_r.at[p], xn)

    def w_fwd(i):
        return remote(wbuf.at[0, 1, rows(i)], wbuf.at[0, 1, rows(i)], s_w.at[0], w_r.at[1, i], xn)

    def w_to_sib(j, i, own):
        src = w_ref.at[rows(i)] if own else wbuf.at[0, j, rows(i)]
        return remote(src, wbuf.at[1, j, rows(i)], s_ws.at[0], ws_r.at[j, i], sib)

    def p_own_half(q, kt, h):
        return remote(
            pown.at[q, kt, pl.ds(h * 256, 256)], dw_tile(q, kt, h * 256, 256), s_px.at[0],
            px_r.at[q * 8 + kt * 2 + h], xn,
        )

    def p_own_first(i):
        k0, n = FIRST[i]
        return remote(
            pown.at[0, 0, pl.ds(k0, n)], dw_tile(0, 0, k0, n), s_px.at[0], px_r.at[(0, 32, 1)[i]], xn
        )

    def p_own(q, kt):
        return remote(pown.at[q, kt], dw_tile(q, kt), s_px.at[0], px_r.at[16 + (q - 2) * 4 + kt], xn)

    def p_own_last():
        return remote(
            pown.at[3, 3, pl.ds(0, 256)], dw_tile(3, 3, 0, 256), s_px.at[0], px_r.at[23], xn
        )

    def tail_store():
        return local(pown.at[3, 3, pl.ds(256, 256)], tail, tail_sem.at[0])

    def p_other(q, kt):
        return remote(poth.at[q, kt], land.at[q - 2, kt], s_px.at[1], px_r.at[24 + (q - 2) * 4 + kt], xn)

    def p_trans(i):
        q, kt, r = i // 16, (i // 4) % 4, i % 4
        part = pl.ds(r * 128, 128)
        return remote(poth.at[q, kt, part], bufy.at[q, kt, part], s_py.at[0], pf_r.at[i], yn)

    def p_trans_tail(i):
        return remote(
            poth.at[1, 3, pl.ds(i * 128 - 3584, 128)], tail.at[pl.ds((i - 30) * 128, 128)],
            s_py.at[0], pf_r.at[i], yn,
        )

    def p_fwd(i):
        q, kt, r = i // 16, (i // 4) % 4, i % 4
        part = pl.ds(r * 128, 128)
        return remote(bufy.at[q, kt, part], land.at[q, kt, part], s_px.at[0], pf_r.at[i], xn)

    def p_term(q, kt):
        return remote(poth.at[q, kt], dw_tile(q, kt), s_py.at[0], py_r.at[q * 4 + kt], yn)

    def sum_to_y(q, kt):
        return remote(poth.at[q, kt], dw_tile(q, kt), s_sum.at[0], py_r.at[q * 4 + kt], yn)

    dy_load.start()
    for kt in range(4):
        x_load(kt).start()

    barrier = pltpu.get_barrier_semaphore()
    for dev in (sib, xn, yn):
        pl.semaphore_signal(barrier, inc=1, device_id=dev, device_id_type=MESH)
    pl.semaphore_wait(barrier, 3)

    dy_to_sib(0, 0).start()
    x_to_sib_part(0).start()
    dy_to_y(0).start()
    dy_to_y(1).start()

    @pl.when(is_a)
    def _():
        for i in range(8):
            w_own_to_x(i).start()
        for q in range(2, 4):
            dy_to_y(q).start()

    @pl.when(is_b)
    def _():
        for i in range(4):
            w_to_y(i).start()
        for q in range(2, 4):
            dy_to_y(q).start()
        for p in range(16):
            w_to_y_part(p).start()

    x_to_sib_part(1).start()
    x_to_sib_part(2).start()
    for kt in range(1, 4):
        x_to_sib(kt).start()
    for q in range(1, 4):
        dy_to_sib(0, q).start()

    @pl.when(is_a)
    def _():
        for i in range(8):
            w_to_sib(0, i, True).start()

    def p_part(j, q, k0, n):
        def term(t, acc):
            part = pl.ds(t * 1024, 1024)
            cols = pl.ds(pl.multiple_of(k0, 128), n)
            both = pl.ds(pl.multiple_of(2048 + k0, 128), n)
            dy = pl.ds(q * 256, 256)
            return acc + _tdot(dx_ref[part, cols], dyv[0, j, part, dy]) + _tdot(
                dx_ref[part, both], dyv[1, j, part, dy]
            )

        return lax.fori_loop(0, 2, term, jnp.zeros((n, 256), F32), unroll=True)

    dy_load.wait()
    for q in range(4):
        dy_to_sib(0, q).wait_recv()
        if q == 0:
            x_load(0).wait()
            for i, (k0, n) in enumerate(FIRST):
                x_to_sib_part(i).wait_recv()
                pown[0, 0, k0:k0 + n] = p_part(0, 0, k0, n)

                @pl.when(is_b)
                def _(i=i):
                    p_own_first(i).start()

        def own_body(kt, carry, q=q):
            if q == 0:
                x_load(kt).wait()
                x_to_sib(kt).wait_recv()

            def half(h, carry):
                pown[q, kt, pl.ds(h * 256, 256)] = p_part(0, q, kt * 512 + h * 256, 256)
                return carry

            lax.fori_loop(0, 2, half, 0)
            if q < 2:
                @pl.when(is_b)
                def _():
                    p_own_half(q, kt, 0).start()
                    p_own_half(q, kt, 1).start()
            return carry

        lax.fori_loop(1 if q == 0 else 0, 4, own_body, 0)

    def other_tile(q, kt):
        def half(h, carry):
            poth[q, kt, pl.ds(h * 256, 256)] = p_part(1, q, kt * 512 + h * 256, 256)
            return carry

        lax.fori_loop(0, 2, half, 0)

    def trans_tile(q, kt):
        for r in range(4):
            if q == 1 and r >= 2:
                @pl.when(kt < 3)
                def _(r=r):
                    p_trans(16 * q + 4 * kt + r).start()

                @pl.when(kt == 3)
                def _(r=r):
                    p_trans_tail(28 + r).start()
            else:
                p_trans(16 * q + 4 * kt + r).start()

    def dy_in(q):
        dy_to_y(q).wait_recv()
        dy_to_sib(1, q).start()

    def other_pass(q):
        dy_in(q)
        dy_to_sib(1, q).wait_recv()

        def body(kt, carry):
            other_tile(q, kt)
            if q < 2:
                @pl.when(is_a)
                def _():
                    p_term(q, kt).start()

                @pl.when(is_b)
                def _():
                    trans_tile(q, kt)
            else:
                @pl.when(is_b)
                def _():
                    p_other(q, kt).start()
            return carry

        lax.fori_loop(0, 4, body, 0)

    def w_loads(d, cc, own_from_arg):
        if own_from_arg:
            first = local(w_ref.at[rows(d)], wv.at[cc, 0], wl_sem.at[cc, 0])
        else:
            first = local(wbuf.at[cc, 0, rows(d)], wv.at[cc, 0], wl_sem.at[cc, 0])
        return first, local(wbuf.at[cc, 1, rows(d)], wv.at[cc, 1], wl_sem.at[cc, 1])

    def start_loads(d, cc, own_from_arg):
        for cp in w_loads(d, cc, own_from_arg):
            cp.start()

    def wait_loads(d, cc, own_from_arg):
        for cp in w_loads(d, cc, own_from_arg):
            cp.wait()

    def dx_stripe(d, cc, lo=0, hi=4):
        k0 = (c + cc * (1 - 2 * c)) * 2048
        cols = pl.ds(pl.multiple_of(k0 + d * 256, 256), 256)

        def body(m, carry):
            part = pl.ds(m * 512, 512)
            dx_ref[part, cols] = (
                _dot_t(dyv[0, 0, part, :], wv[cc, 0]) + _dot_t(dyv[0, 1, part, :], wv[cc, 1])
            ).astype(BF16)
            return carry

        lax.fori_loop(lo, hi, body, 0)

    def pair_wait(d, own_from_arg):
        w_to_sib(0, d, own_from_arg).wait_recv()
        w_to_sib(1, d, False).wait_recv()

    other_pass(0)
    other_pass(1)

    @pl.when(is_a)
    def _():
        def add(q, kt):
            tile = dw_tile(q, kt)
            tile[...] = tile[...] + pown[q, kt]

        def final_early(t):
            q, kt = t // 4, t % 4

            @pl.when(t == 0)
            def _():
                for i in range(3):
                    p_own_first(i).wait_recv()

            @pl.when(t > 0)
            def _():
                for h in range(2):
                    p_own_half(q, kt, h).wait_recv()
            add(q, kt)

        def final_late(t):
            q, kt = 2 + t // 4, t % 4
            p_own(q, kt).wait_recv()
            add(q, kt)

        def a_sum(q, kt):
            p_other(q, kt).wait_recv()
            poth[q, kt] = poth[q, kt] + land[q - 2, kt]
            sum_to_y(q, kt).start()

        def fwd(i):
            p_trans(i).wait_recv()
            p_fwd(i).start()

        def early(i, carry):
            w_to_y(i).wait_recv()
            w_fwd(i).start()
            w_to_sib(1, i, False).start()
            final_early(i)
            return carry

        lax.fori_loop(0, 4, early, 0)

        dy_in(2)
        dy_to_sib(1, 2).wait_recv()

        def q2_body(kt, carry):
            other_tile(2, kt)
            final_early(4 + kt)
            return carry

        lax.fori_loop(0, 4, q2_body, 0)
        start_loads(0, 0, True)
        dy_in(3)

        def step(i, carry):
            @pl.when(i < 16)
            def _():
                w_to_y_part(i).wait_recv()
                w_fwd_part(i).start()

                @pl.when(i % 4 == 3)
                def _():
                    w_to_sib(1, 4 + i // 4, False).start()

            @pl.when(i >= 16)
            def _():
                fwd(i - 16)

            @pl.when(i == 0)
            def _():
                dy_to_sib(1, 3).wait_recv()

            @pl.when(i < 4)
            def _():
                other_tile(3, i)

            @pl.when(jnp.logical_and(i >= 4, i < 36))
            def _():
                e = (i - 4) // 2
                d, cc = e // 2, e % 2
                odd = i % 2

                @pl.when(odd == 0)
                def _():
                    @pl.when(cc == 0)
                    def _():
                        pair_wait(d, True)
                        start_loads(d, 1, False)
                        wait_loads(d, 0, True)

                    @pl.when(cc == 1)
                    def _():
                        @pl.when(d < 7)
                        def _():
                            start_loads(d + 1, 0, True)
                        wait_loads(d, 1, False)

                dx_stripe(d, cc, 2 * odd, 2 * odd + 2)

            @pl.when(jnp.logical_and(i < 8, i % 2 == 1))
            def _():
                a_sum(2, i // 2)

            @pl.when(jnp.logical_and(jnp.logical_and(i >= 10, i < 26), i % 4 == 2))
            def _():
                a_sum(3, (i - 10) // 4)

            @pl.when(jnp.logical_and(i >= 26, i % 4 == 2))
            def _():
                final_late((i - 26) // 4)
            return carry

        lax.fori_loop(0, 46, step, 0)
        final_late(5)
        final_late(6)
        low = dw_tile(3, 3, 256, 256)
        low[...] = pown[3, 3, 256:512]
        for i in (30, 31):
            p_trans_tail(i).wait_recv()
        p_own_last().wait_recv()
        top = dw_tile(3, 3, 0, 256)
        top[...] = top[...] + pown[3, 3, 0:256]
        remote(wbuf.at[0], wbuf.at[0], s_w.at[0], w_r.at[0, 0], xn).wait_send()
        sent = dyv.at[0, 0, pl.ds(0, 1920)]
        remote(sent, sent, s_px.at[0], px_r.at[0], xn).wait_send()
        remote(land, land, s_py.at[0], py_r.at[0], yn).wait_send()
        remote(land, land, s_sum.at[0], py_r.at[0], yn).wait_send()

    @pl.when(is_b)
    def _():
        other_pass(2)
        other_pass(3)
        for q in range(2, 4):
            for kt in range(4):
                if q == 3 and kt == 3:
                    p_own_last().start()
                    tail_store().start()
                else:
                    p_own(q, kt).start()

        def own_w(i, carry):
            w_own_to_x(i).wait_recv()
            w_to_sib(0, i, False).start()
            return carry

        lax.fori_loop(0, 8, own_w, 0)

        def stripes(d, carry):
            @pl.when(d < 4)
            def _():
                w_to_y(d).wait_recv()

            @pl.when(d >= 4)
            def _():
                for p in range(4):
                    w_to_y_part(4 * (d - 4) + p).wait_recv()
            w_to_sib(1, d, False).start()
            start_loads(d, 0, False)
            pair_wait(d, False)
            start_loads(d, 1, False)
            wait_loads(d, 0, False)
            dx_stripe(d, 0)
            wait_loads(d, 1, False)
            dx_stripe(d, 1)
            return carry

        lax.fori_loop(0, 8, stripes, 0)

        def fin(i, carry):
            q, kt, r = i // 16, (i // 4) % 4, i % 4

            @pl.when(r == 0)
            def _():
                p_term(q, kt).wait_recv()
            p_fwd(i).wait_recv()
            tile = dw_tile(q, kt, r * 128, 128)
            tile[...] = tile[...] + land[q, kt, pl.ds(r * 128, 128)]
            return carry

        lax.fori_loop(0, 30, fin, 0)
        for q in range(2, 4):
            for kt in range(4):
                sum_to_y(q, kt).wait_recv()
        remote(wbuf.at[0, 0], wbuf.at[0, 0], s_w.at[0], w_r.at[0, 0], yn).wait_send()
        tail_store().wait()
        sent = dw_ref.at[pl.ds(0, 1984)]
        remote(sent, sent, s_px.at[0], px_r.at[0], xn).wait_send()
        remote(land, land, s_px.at[1], px_r.at[0], xn).wait_send()
        remote(land, land, s_py.at[0], py_r.at[0], yn).wait_send()

    remote(dyv.at[0], dyv.at[0], s_dys.at[0], dys_r.at[0, 0], sib).wait_send()
    remote(dyv.at[0, 0], dyv.at[0, 0], s_dyy.at[0], dyy_r.at[0], yn).wait_send()
    remote(wbuf.at[0], wbuf.at[0], s_xs.at[0], xs_r.at[0], sib).wait_send()
    remote(wbuf.at[0], wbuf.at[0], s_ws.at[0], ws_r.at[0, 0], sib).wait_send()


def store_kernel(dx_ref, dw_ref, dx_out, dw_out, sem):
    copies = []
    for i in range(4):
        part = pl.ds(i * 512, 512)
        copies.append(pltpu.make_async_copy(dx_ref.at[part], dx_out.at[part], sem.at[2 * i]))
        copies.append(pltpu.make_async_copy(dw_ref.at[part], dw_out.at[part], sem.at[2 * i + 1]))
    for cp in copies:
        cp.start()
    for cp in copies:
        cp.wait()


def add_kernel(done_ref, dw_ref, tail_ref, dw_out, buf, sem):
    is_a = lax.axis_index("row") // 2 == lax.axis_index("col")
    col = jnp.where(is_a, 768, 256)
    cols = pl.ds(pl.multiple_of(col, 256), 256)
    buf[...] = dw_ref[1792:2048, cols] + tail_ref[...]
    cp = pltpu.make_async_copy(buf, dw_out.at[pl.ds(1792, 256), cols], sem.at[0])
    cp.start()
    cp.wait()


def local_backward(act_blk, w_blk, grad_blk):
    any_spec = pl.BlockSpec(memory_space=pl.ANY)
    vmem_spec = pl.BlockSpec(memory_space=pltpu.VMEM)
    dma = pltpu.SemaphoreType.DMA
    outs = pl.pallas_call(
        kernel,
        out_shape=(
            pltpu.VMEM((2048, 4096), BF16),
            pltpu.VMEM((2048, 1024), F32),
            jax.ShapeDtypeStruct((2, 2, 2048, 1024), BF16),
            jax.ShapeDtypeStruct((2, 4, 512, 256), F32),
            jax.ShapeDtypeStruct((256, 256), F32),
        ),
        in_specs=[any_spec] * 3,
        out_specs=(vmem_spec, vmem_spec) + (any_spec,) * 3,
        scratch_shapes=[
            pltpu.VMEM((2, 2, 2048, 1024), BF16),
            pltpu.VMEM((4, 4, 512, 256), F32),
            pltpu.VMEM((4, 4, 512, 256), F32),
            pltpu.VMEM((2, 2, 256, 1024), BF16),
            pltpu.VMEM((2, 4, 512, 256), F32),
            dma((5,)), dma((2, 4)), dma((4,)), dma((7,)), dma((2, 8)), dma((16,)), dma((2, 8)), dma((33,)), dma((16,)),
            dma((32,)),
            dma((1,)), dma((1,)), dma((1,)), dma((1,)), dma((1,)), dma((2,)), dma((1,)), dma((1,)), dma((2, 2)), dma((1,)),
        ],
        compiler_params=pltpu.CompilerParams(
            collective_id=0, has_side_effects=True, vmem_limit_bytes=41_800_000
        ),
        cost_estimate=pl.CostEstimate(flops=2 * 2048 * 2048 * 4096 * 2, bytes_accessed=100 << 20, transcendentals=0),
    )(act_blk, w_blk, grad_blk)
    tail = lax.ppermute(outs[4], "row", [(0, 2), (1, 3), (2, 0), (3, 1)])
    dx, dw = pl.pallas_call(
        store_kernel,
        out_shape=(jax.ShapeDtypeStruct((2048, 4096), BF16), jax.ShapeDtypeStruct((2048, 1024), F32)),
        in_specs=[vmem_spec, vmem_spec],
        out_specs=(any_spec, any_spec),
        scratch_shapes=[dma((8,))],
        compiler_params=pltpu.CompilerParams(vmem_limit_bytes=1 << 20),
        cost_estimate=pl.CostEstimate(flops=0, bytes_accessed=48 << 20, transcendentals=0),
    )(outs[0], outs[1])
    dw = pl.pallas_call(
        add_kernel,
        out_shape=jax.ShapeDtypeStruct((2048, 1024), F32),
        in_specs=[any_spec, vmem_spec, vmem_spec],
        out_specs=any_spec,
        scratch_shapes=[pltpu.VMEM((256, 256), F32), dma((1,))],
        input_output_aliases={0: 0},
        compiler_params=pltpu.CompilerParams(vmem_limit_bytes=2 << 20),
        cost_estimate=pl.CostEstimate(flops=0, bytes_accessed=1 << 20, transcendentals=0),
    )(dw, outs[1], tail)
    return dx, dw


def solution(mesh):
    io_spec = P(("dp", "row"), "col")
    w_spec = P("row", "col")
    return jax.shard_map(
        local_backward, mesh=mesh, in_specs=(io_spec, w_spec, io_spec), out_specs=(io_spec, io_spec), check_vma=False
    )
```

```python
import jax
import jax.numpy as jnp
from jax import lax
from jax.experimental import pallas as pl
from jax.experimental.pallas import tpu as pltpu
from jax.sharding import PartitionSpec as P

MESH = pl.DeviceIdType.MESH
F32 = jnp.float32
BF16 = jnp.bfloat16
H, N, D, T, Q, S = 2048, 1024, 512, 256, 128, 64
R = 320
ME, SIB = 0, 1
OWN, OTH = 0, 1
ARG, BUF = "arg", "buf"
FIRST = ((0, Q, 0, Q), (0, Q, Q, Q), (Q, Q, 0, T), (T, T, 0, T))


def _tdot(a, b):
    return lax.dot_general(a, b, (((0,), (0,)), ((), ())), preferred_element_type=F32)


def _dot_t(a, b):
    return lax.dot_general(a, b, (((1,), (1,)), ((), ())), preferred_element_type=F32)


def loop(n, f, start=0):
    def body(i, carry):
        f(i)
        return carry

    lax.fori_loop(start, n, body, start)


def cut(k0, n, unit=Q):
    return pl.ds(pl.multiple_of(k0, unit), n)


def kernel(
    x_ref, w_ref, dy_ref,
    dx_ref, dw_ref, wbuf, bufy, tail,
    dyv, pown, poth, wv, land,
    dy_sem, x_sem, dys_r, dyy_r, xs_r, xf_r, w_r, wp_r, ws_r, pa_r, ph_r, po_r, ps_r, py_r, pf_r,
    s_dys, s_dyy, s_xs, s_w, s_ws, s_px, s_po, s_py, s_sum, wl_sem, tail_sem,
):
    row = lax.axis_index("row")
    y = lax.axis_index("col")
    x = row // 2
    c = row % 2
    is_a = x == y
    is_b = x != y
    sib = {"row": row + 1 - 2 * c}
    xn = {"row": (row + 2) % 4}
    yn = {"col": 1 - y}

    def remote(src, dst, ssem, rsem, dev):
        return pltpu.make_async_remote_copy(
            src_ref=src, dst_ref=dst, send_sem=ssem, recv_sem=rsem, device_id=dev, device_id_type=MESH
        )

    def local(src, dst, sem):
        return pltpu.make_async_copy(src, dst, sem)

    def qs(q):
        return pl.ds(q * T, T)

    def xo(k0, n):
        return dx_ref.at[:, cut(k0, n)]

    def xs(k0, n):
        return dx_ref.at[:, cut(H + k0, n)]

    def dw_part(q, r0, n):
        return dw_ref.at[pl.ds(r0, n), cut(q * T, T)]

    def dw_tile(q, kt):
        return dw_part(q, kt * D, D)

    dy_load = local(dy_ref, dyv.at[ME, OWN], dy_sem)

    def x_load(kt):
        return local(x_ref.at[:, pl.ds(c * H + kt * D, D)], xo(kt * D, D), x_sem.at[kt])

    def x_cols_to_sib(k0, n, sem):
        return remote(x_ref.at[:, pl.ds((1 - c) * H + k0, n)], xs(k0, n), s_xs, sem, sib)

    def x_to_sib(kt):
        return x_cols_to_sib(kt * D, D, xs_r.at[kt])

    def x_first(i):
        k0, n = ((0, Q), (Q, Q), (T, T))[i]
        return x_cols_to_sib(k0, n, xf_r.at[i])

    def dy_first(i):
        cols = pl.ds(i * Q, Q)
        return remote(dy_ref.at[:, cols], dyv.at[SIB, OWN, :, cols], s_dys, xf_r.at[3 + i], sib)

    def dy_to_sib(j, q):
        src = dy_ref.at[:, qs(q)] if j == OWN else dyv.at[ME, OTH, :, qs(q)]
        return remote(src, dyv.at[SIB, j, :, qs(q)], s_dys, dys_r.at[j, q], sib)

    def dy_to_y(q):
        return remote(dy_ref.at[:, qs(q)], dyv.at[ME, OTH, :, qs(q)], s_dyy, dyy_r.at[q], yn)

    def w_own_to_x(i):
        return remote(w_ref.at[qs(i)], wbuf.at[ME, OWN, qs(i)], s_w, w_r.at[OWN, i], xn)

    def w_to_y(i):
        return remote(w_ref.at[qs(i)], wbuf.at[ME, OTH, qs(i)], s_w, w_r.at[OTH, i], yn)

    def w_fwd(i):
        return remote(wbuf.at[ME, OTH, qs(i)], wbuf.at[ME, OTH, qs(i)], s_w, w_r.at[OTH, i], xn)

    def w_piece(p):
        return pl.ds(N + p * S, S)

    def w_to_y_piece(p):
        return remote(w_ref.at[w_piece(p)], wbuf.at[ME, OTH, w_piece(p)], s_w, wp_r.at[p], yn)

    def w_fwd_piece(p):
        return remote(wbuf.at[ME, OTH, w_piece(p)], wbuf.at[ME, OTH, w_piece(p)], s_w, wp_r.at[p], xn)

    def w_to_sib(j, i, src):
        ref = w_ref.at[qs(i)] if src == ARG else wbuf.at[ME, j, qs(i)]
        return remote(ref, wbuf.at[SIB, j, qs(i)], s_ws, ws_r.at[j, i], sib)

    def p_first(i):
        r0, n, c0, m = FIRST[i]
        return remote(
            pown.at[0, 0, pl.ds(r0, n), pl.ds(c0, m)], dw_ref.at[pl.ds(r0, n), pl.ds(c0, m)],
            s_px, pa_r.at[i], xn,
        )

    def p_half(q, kt, h):
        return remote(
            pown.at[q, kt, pl.ds(h * T, T)], dw_part(q, kt * D + h * T, T), s_px, ph_r.at[q, 2 * kt + h], xn
        )

    def p_own(q, kt):
        return remote(pown.at[q, kt], dw_tile(q, kt), s_px, po_r.at[q - 2, kt], xn)

    def p_own_last():
        return remote(
            pown.at[3, 3, pl.ds(0, D - R)], dw_part(3, 3 * D, D - R), s_px, po_r.at[1, 3], xn
        )

    def tail_store():
        return local(pown.at[3, 3, pl.ds(D - R, R)], tail, tail_sem)

    def p_other(q, kt):
        return remote(poth.at[q, kt], land.at[q - 2, kt], s_po, ps_r.at[q - 2, kt], xn)

    def p_trans(q, kt, r):
        part = pl.ds(r * Q, Q)
        return remote(poth.at[q, kt, part], bufy.at[q, kt, part], s_py, pf_r.at[q, 4 * kt + r], yn)

    def p_fwd(q, kt, r):
        part = pl.ds(r * Q, Q)
        return remote(bufy.at[q, kt, part], land.at[q, kt, part], s_px, pf_r.at[q, 4 * kt + r], xn)

    def p_trans_short():
        part = pl.ds(Q, S)
        return remote(poth.at[1, 3, part], bufy.at[1, 3, part], s_py, pf_r.at[1, 13], yn)

    def p_fwd_short():
        part = pl.ds(Q, S)
        return remote(bufy.at[1, 3, part], land.at[1, 3, part], s_px, pf_r.at[1, 13], xn)

    def p_trans_tail():
        return remote(poth.at[1, 3, pl.ds(D - R, R)], tail, s_py, pf_r.at[1, 14], yn)

    def p_term(q, kt):
        return remote(poth.at[q, kt], dw_tile(q, kt), s_py, py_r.at[q, kt], yn)

    def sum_to_y(q, kt):
        return remote(poth.at[q, kt], dw_tile(q, kt), s_sum, py_r.at[q, kt], yn)

    def drain(ref, sem):
        remote(ref, ref, sem, dyy_r.at[0], yn).wait_send()

    dy_load.start()
    for kt in range(4):
        x_load(kt).start()

    barrier = pltpu.get_barrier_semaphore()
    for dev in (sib, xn, yn):
        pl.semaphore_signal(barrier, inc=1, device_id=dev, device_id_type=MESH)
    pl.semaphore_wait(barrier, 3)

    dy_first(0).start()
    x_first(0).start()
    dy_to_y(0).start()
    dy_first(1).start()
    x_first(1).start()
    x_first(2).start()
    dy_to_y(1).start()

    @pl.when(is_a)
    def _():
        for i in range(8):
            w_own_to_x(i).start()
        for q in (2, 3):
            dy_to_y(q).start()

    @pl.when(is_b)
    def _():
        for i in range(4):
            w_to_y(i).start()
        for q in (2, 3):
            dy_to_y(q).start()
        for p in range(16):
            w_to_y_piece(p).start()

    for kt in (1, 2, 3):
        x_to_sib(kt).start()
    for q in (1, 2, 3):
        dy_to_sib(OWN, q).start()

    @pl.when(is_a)
    def _():
        for i in range(8):
            w_to_sib(OWN, i, ARG).start()

    def p_part(j, c0, k0, n, m=T):
        dy = pl.ds(c0, m)
        acc = None
        for t in range(2):
            part = pl.ds(t * N, N)
            for who, base in ((ME, k0), (SIB, H + k0)):
                term = _tdot(dx_ref[part, cut(base, n)], dyv[who, j, part, dy])
                acc = term if acc is None else acc + term
        return acc

    def p_tile(dst, j, q, kt):
        loop(2, lambda h: put(dst.at[q, kt, pl.ds(h * T, T)], p_part(j, q * T, kt * D + h * T, T)))

    def put(ref, value):
        ref[...] = value

    dy_load.wait()
    x_load(0).wait()
    dy_first(0).wait_recv()
    for i, (r0, n, c0, m) in enumerate(FIRST):
        if i == 1:
            dy_first(1).wait_recv()
        else:
            x_first(max(i - 1, 0)).wait_recv()
        put(pown.at[0, 0, pl.ds(r0, n), pl.ds(c0, m)], p_part(OWN, c0, r0, n, m))

        @pl.when(is_b)
        def _(i=i):
            p_first(i).start()

    def own_tile(q, kt):
        if q == 0:
            x_load(kt).wait()
            x_to_sib(kt).wait_recv()
        p_tile(pown, OWN, q, kt)
        if q < 2:
            @pl.when(is_b)
            def _():
                p_half(q, kt, 0).start()
                p_half(q, kt, 1).start()

    for q in range(4):
        if q > 0:
            dy_to_sib(OWN, q).wait_recv()
        loop(4, lambda kt, q=q: own_tile(q, kt), int(q == 0))

    def trans_tile(q, kt):
        if q == 0:
            for r in range(4):
                p_trans(q, kt, r).start()
            return
        p_trans(q, kt, 0).start()

        @pl.when(kt < 3)
        def _():
            for r in (1, 2, 3):
                p_trans(q, kt, r).start()

        @pl.when(kt == 3)
        def _():
            p_trans_short().start()
            p_trans_tail().start()

    def dy_in(q):
        dy_to_y(q).wait_recv()
        dy_to_sib(OTH, q).start()

    def other_pass(q):
        dy_in(q)
        dy_to_sib(OTH, q).wait_recv()

        def tile(kt):
            p_tile(poth, OTH, q, kt)
            if q < 2:
                @pl.when(is_a)
                def _():
                    p_term(q, kt).start()

                @pl.when(is_b)
                def _():
                    trans_tile(q, kt)
            else:
                @pl.when(is_b)
                def _():
                    p_other(q, kt).start()

        loop(4, tile)

    def w_loads(d, cc, src):
        ref = w_ref.at[qs(d)] if src == ARG else wbuf.at[cc, OWN, qs(d)]
        return (
            local(ref, wv.at[cc, OWN], wl_sem.at[cc, OWN]),
            local(wbuf.at[cc, OTH, qs(d)], wv.at[cc, OTH], wl_sem.at[cc, OTH]),
        )

    def start_loads(d, cc, src):
        for cp in w_loads(d, cc, src):
            cp.start()

    def wait_loads(d, cc, src):
        for cp in w_loads(d, cc, src):
            cp.wait()

    def dx_stripe(d, cc, lo=0, hi=4):
        cols = cut((c + cc * (1 - 2 * c)) * H + d * T, T, T)

        def rows(m):
            part = pl.ds(m * D, D)
            dx_ref[part, cols] = (
                _dot_t(dyv[ME, OWN, part, :], wv[cc, OWN]) + _dot_t(dyv[ME, OTH, part, :], wv[cc, OTH])
            ).astype(BF16)

        loop(hi, rows, lo)

    def pair_wait(d, src):
        w_to_sib(OWN, d, src).wait_recv()
        w_to_sib(OTH, d, BUF).wait_recv()

    other_pass(0)
    other_pass(1)

    @pl.when(is_a)
    def _():
        def add(q, kt):
            tile = dw_tile(q, kt)
            tile[...] = tile[...] + pown[q, kt]

        def final_early(t):
            q, kt = t // 4, t % 4

            @pl.when(t == 0)
            def _():
                for i in range(len(FIRST)):
                    p_first(i).wait_recv()

            @pl.when(t > 0)
            def _():
                p_half(q, kt, 0).wait_recv()
                p_half(q, kt, 1).wait_recv()
            add(q, kt)

        def final_late(t):
            q, kt = 2 + t // 4, t % 4
            p_own(q, kt).wait_recv()
            add(q, kt)

        def a_sum(q, kt):
            p_other(q, kt).wait_recv()
            poth[q, kt] = poth[q, kt] + land[q - 2, kt]
            sum_to_y(q, kt).start()

        def early(i):
            w_to_y(i).wait_recv()
            w_fwd(i).start()
            w_to_sib(OTH, i, BUF).start()
            final_early(i)

        loop(4, early)
        dy_in(2)
        dy_to_sib(OTH, 2).wait_recv()

        def q2_tile(kt):
            p_tile(poth, OTH, 2, kt)
            final_early(4 + kt)

        loop(4, q2_tile)
        start_loads(0, ME, ARG)
        dy_in(3)

        def step(i):
            @pl.when(i < 16)
            def _():
                w_to_y_piece(i).wait_recv()
                w_fwd_piece(i).start()

                @pl.when(i % 4 == 3)
                def _():
                    w_to_sib(OTH, 4 + i // 4, BUF).start()

            @pl.when(i >= 16)
            def _():
                k = i - 16
                q, kt, r = k // 16, (k // 4) % 4, k % 4
                p_trans(q, kt, r).wait_recv()
                p_fwd(q, kt, r).start()

            @pl.when(i == 0)
            def _():
                dy_to_sib(OTH, 3).wait_recv()

            @pl.when(i < 4)
            def _():
                p_tile(poth, OTH, 3, i)

            @pl.when(jnp.logical_and(i >= 4, i < 36))
            def _():
                e = (i - 4) // 2
                d, cc = e // 2, e % 2
                odd = i % 2

                @pl.when(jnp.logical_and(odd == 0, cc == ME))
                def _():
                    pair_wait(d, ARG)
                    start_loads(d, SIB, BUF)
                    wait_loads(d, ME, ARG)

                @pl.when(jnp.logical_and(odd == 0, cc == SIB))
                def _():
                    @pl.when(d < 7)
                    def _():
                        start_loads(d + 1, ME, ARG)
                    wait_loads(d, SIB, BUF)

                dx_stripe(d, cc, 2 * odd, 2 * odd + 2)

            @pl.when(jnp.logical_and(i < 8, i % 2 == 1))
            def _():
                a_sum(2, i // 2)

            @pl.when(jnp.logical_and(jnp.logical_and(i >= 10, i < 26), i % 4 == 2))
            def _():
                a_sum(3, (i - 10) // 4)

            @pl.when(jnp.logical_and(i >= 26, i % 4 == 2))
            def _():
                final_late((i - 26) // 4)

        loop(45, step)
        p_trans_short().wait_recv()
        p_fwd_short().start()
        low = dw_part(3, 4 * D - R, R)
        low[...] = pown[3, 3, D - R:]
        final_late(5)
        final_late(6)
        p_trans_tail().wait_recv()
        p_own_last().wait_recv()
        top = dw_part(3, 3 * D, D - R)
        top[...] = top[...] + pown[3, 3, :D - R]
        drain(wbuf.at[ME], s_w)
        drain(dyv.at[ME, OWN, pl.ds(0, H - R // 2)], s_px)
        drain(land, s_py)
        drain(land, s_sum)

    @pl.when(is_b)
    def _():
        other_pass(2)
        other_pass(3)
        for t in range(7):
            p_own(2 + t // 4, t % 4).start()
        p_own_last().start()
        tail_store().start()

        def own_w(i):
            w_own_to_x(i).wait_recv()
            w_to_sib(OWN, i, BUF).start()

        loop(8, own_w)

        def stripes(d):
            @pl.when(d < 4)
            def _():
                w_to_y(d).wait_recv()

            @pl.when(d >= 4)
            def _():
                for p in range(4):
                    w_to_y_piece(4 * (d - 4) + p).wait_recv()
            w_to_sib(OTH, d, BUF).start()
            start_loads(d, ME, BUF)
            pair_wait(d, BUF)
            start_loads(d, SIB, BUF)
            for cc in (ME, SIB):
                wait_loads(d, cc, BUF)
                dx_stripe(d, cc)

        loop(8, stripes)

        def fin(i):
            q, kt, r = i // 16, (i // 4) % 4, i % 4

            @pl.when(r == 0)
            def _():
                p_term(q, kt).wait_recv()
            p_fwd(q, kt, r).wait_recv()
            tile = dw_part(q, kt * D + r * Q, Q)
            tile[...] = tile[...] + land[q, kt, pl.ds(r * Q, Q)]

        loop(29, fin)
        p_fwd_short().wait_recv()
        tile = dw_part(1, 3 * D + Q, S)
        tile[...] = tile[...] + land[1, 3, Q:Q + S]
        for q in (2, 3):
            for kt in range(4):
                sum_to_y(q, kt).wait_recv()
        tail_store().wait()
        drain(wbuf.at[ME, OWN], s_w)
        drain(dw_ref.at[pl.ds(0, H - R // 4)], s_px)
        drain(land, s_po)
        drain(land, s_py)

    drain(dyv.at[ME], s_dys)
    drain(dyv.at[ME, OWN], s_dyy)
    drain(wbuf.at[ME], s_xs)
    drain(wbuf.at[ME], s_ws)


def store_kernel(dx_ref, dw_ref, dx_out, dw_out, sem):
    copies = []
    for i in range(4):
        part = pl.ds(i * D, D)
        copies.append(pltpu.make_async_copy(dx_ref.at[part], dx_out.at[part], sem.at[0, i]))
        copies.append(pltpu.make_async_copy(dw_ref.at[part], dw_out.at[part], sem.at[1, i]))
    for cp in copies:
        cp.start()
    for cp in copies:
        cp.wait()


def add_kernel(done_ref, dw_ref, tail_ref, dw_out, buf, sem):
    is_a = lax.axis_index("row") // 2 == lax.axis_index("col")
    cols = cut(jnp.where(is_a, 3 * T, T), T)
    buf[...] = dw_ref[H - R:, cols] + tail_ref[...]
    cp = pltpu.make_async_copy(buf, dw_out.at[pl.ds(H - R, R), cols], sem)
    cp.start()
    cp.wait()


def local_backward(act_blk, w_blk, grad_blk):
    any_spec = pl.BlockSpec(memory_space=pl.ANY)
    vmem_spec = pl.BlockSpec(memory_space=pltpu.VMEM)
    dma = pltpu.SemaphoreType.DMA
    outs = pl.pallas_call(
        kernel,
        out_shape=(
            pltpu.VMEM((H, 2 * H), BF16),
            pltpu.VMEM((H, N), F32),
            jax.ShapeDtypeStruct((2, 2, H, N), BF16),
            jax.ShapeDtypeStruct((2, 4, D, T), F32),
            jax.ShapeDtypeStruct((R, T), F32),
        ),
        in_specs=[any_spec] * 3,
        out_specs=(vmem_spec,) * 2 + (any_spec,) * 3,
        scratch_shapes=[
            pltpu.VMEM((2, 2, H, N), BF16),
            pltpu.VMEM((4, 4, D, T), F32),
            pltpu.VMEM((4, 4, D, T), F32),
            pltpu.VMEM((2, 2, T, N), BF16),
            pltpu.VMEM((2, 4, D, T), F32),
            dma, dma((4,)), dma((2, 4)), dma((4,)), dma((4,)), dma((5,)), dma((2, 8)), dma((16,)), dma((2, 8)),
            dma((4,)), dma((2, 8)), dma((2, 4)), dma((2, 4)), dma((4, 4)), dma((2, 16)),
            dma, dma, dma, dma, dma, dma, dma, dma, dma, dma((2, 2)), dma,
        ],
        compiler_params=pltpu.CompilerParams(
            collective_id=0, has_side_effects=True, vmem_limit_bytes=41_800_000
        ),
        cost_estimate=pl.CostEstimate(flops=8 * H * H * H, bytes_accessed=100 << 20, transcendentals=0),
    )(act_blk, w_blk, grad_blk)
    tail = lax.ppermute(outs[4], "row", [(i, (i + 2) % 4) for i in range(4)])
    dx, dw = pl.pallas_call(
        store_kernel,
        out_shape=(jax.ShapeDtypeStruct((H, 2 * H), BF16), jax.ShapeDtypeStruct((H, N), F32)),
        in_specs=[vmem_spec] * 2,
        out_specs=(any_spec,) * 2,
        scratch_shapes=[dma((2, 4))],
        compiler_params=pltpu.CompilerParams(vmem_limit_bytes=1 << 20),
        cost_estimate=pl.CostEstimate(flops=0, bytes_accessed=48 << 20, transcendentals=0),
    )(outs[0], outs[1])
    dw = pl.pallas_call(
        add_kernel,
        out_shape=jax.ShapeDtypeStruct((H, N), F32),
        in_specs=[any_spec] + [vmem_spec] * 2,
        out_specs=any_spec,
        scratch_shapes=[pltpu.VMEM((R, T), F32), dma],
        input_output_aliases={0: 0},
        compiler_params=pltpu.CompilerParams(vmem_limit_bytes=2 << 20),
        cost_estimate=pl.CostEstimate(flops=0, bytes_accessed=1 << 20, transcendentals=0),
    )(dw, outs[1], tail)
    return dx, dw


def solution(mesh):
    io_spec = P(("dp", "row"), "col")
    w_spec = P("row", "col")
    return jax.shard_map(
        local_backward, mesh=mesh, in_specs=(io_spec, w_spec, io_spec), out_specs=(io_spec, io_spec), check_vma=False
    )
```

```python
import jax
import jax.numpy as jnp
from jax import lax
from jax.experimental import pallas as pl
from jax.experimental.pallas import tpu as pltpu
from jax.sharding import PartitionSpec as P

MESH = pl.DeviceIdType.MESH
F32 = jnp.float32
BF16 = jnp.bfloat16
H, N, D, T, Q, S = 2048, 1024, 512, 256, 128, 64
R = 352
E = 96
F = D - E - R
ME, SIB = 0, 1
OWN, OTH = 0, 1
ARG, BUF = "arg", "buf"
FIRST = ((0, Q, 0, Q), (0, Q, Q, Q), (Q, Q, 0, T), (T, T, 0, T))


def _tdot(a, b):
    return lax.dot_general(a, b, (((0,), (0,)), ((), ())), preferred_element_type=F32)


def _dot_t(a, b):
    return lax.dot_general(a, b, (((1,), (1,)), ((), ())), preferred_element_type=F32)


def loop(n, f, start=0):
    def body(i, carry):
        f(i)
        return carry

    lax.fori_loop(start, n, body, start)


def cut(k0, n, unit=Q):
    return pl.ds(pl.multiple_of(k0, unit), n)


def kernel(
    x_ref, w_ref, dy_ref,
    dx_ref, dw_ref, wbuf, bufy, tail, tail_y,
    dyv, pown, poth, wv, land, extra,
    dy_sem, x_sem, dys_r, dyy_r, xs_r, xf_r, w_r, wp_r, ws_r, pa_r, ph_r, po_r, ps_r, py_r, pf_r,
    s_dys, s_dyy, s_xs, s_w, s_ws, s_px, s_po, s_py, s_sum, wl_sem, tail_sem, tail_y_sem, s_ex, ex_r, py_ex,
):
    row = lax.axis_index("row")
    y = lax.axis_index("col")
    x = row // 2
    c = row % 2
    is_a = x == y
    is_b = x != y
    sib = {"row": row + 1 - 2 * c}
    xn = {"row": (row + 2) % 4}
    yn = {"col": 1 - y}

    def remote(src, dst, ssem, rsem, dev):
        return pltpu.make_async_remote_copy(
            src_ref=src, dst_ref=dst, send_sem=ssem, recv_sem=rsem, device_id=dev, device_id_type=MESH
        )

    def local(src, dst, sem):
        return pltpu.make_async_copy(src, dst, sem)

    def qs(q):
        return pl.ds(q * T, T)

    def xo(k0, n):
        return dx_ref.at[:, cut(k0, n)]

    def xs(k0, n):
        return dx_ref.at[:, cut(H + k0, n)]

    def dw_part(q, r0, n):
        return dw_ref.at[pl.ds(r0, n), cut(q * T, T)]

    def dw_tile(q, kt):
        return dw_part(q, kt * D, D)

    dy_load = local(dy_ref, dyv.at[ME, OWN], dy_sem)

    def x_load(kt):
        return local(x_ref.at[:, pl.ds(c * H + kt * D, D)], xo(kt * D, D), x_sem.at[kt])

    def x_cols_to_sib(k0, n, sem):
        return remote(x_ref.at[:, pl.ds((1 - c) * H + k0, n)], xs(k0, n), s_xs, sem, sib)

    def x_to_sib(kt):
        return x_cols_to_sib(kt * D, D, xs_r.at[kt])

    def x_first(i):
        k0, n = ((0, Q), (Q, Q), (T, T))[i]
        return x_cols_to_sib(k0, n, xf_r.at[i])

    def dy_first(i):
        cols = pl.ds(i * Q, Q)
        return remote(dy_ref.at[:, cols], dyv.at[SIB, OWN, :, cols], s_dys, xf_r.at[3 + i], sib)

    def dy_to_sib(j, q):
        src = dy_ref.at[:, qs(q)] if j == OWN else dyv.at[ME, OTH, :, qs(q)]
        return remote(src, dyv.at[SIB, j, :, qs(q)], s_dys, dys_r.at[j, q], sib)

    def dy_to_y(q):
        return remote(dy_ref.at[:, qs(q)], dyv.at[ME, OTH, :, qs(q)], s_dyy, dyy_r.at[q], yn)

    def w_own_to_x(i):
        return remote(w_ref.at[qs(i)], wbuf.at[ME, OWN, qs(i)], s_w, w_r.at[OWN, i], xn)

    def w_to_y(i):
        return remote(w_ref.at[qs(i)], wbuf.at[ME, OTH, qs(i)], s_w, w_r.at[OTH, i], yn)

    def w_fwd(i):
        return remote(wbuf.at[ME, OTH, qs(i)], wbuf.at[ME, OTH, qs(i)], s_w, w_r.at[OTH, i], xn)

    def w_piece(p):
        return pl.ds(N + p * S, S)

    def w_to_y_piece(p):
        return remote(w_ref.at[w_piece(p)], wbuf.at[ME, OTH, w_piece(p)], s_w, wp_r.at[p], yn)

    def w_fwd_piece(p):
        return remote(wbuf.at[ME, OTH, w_piece(p)], wbuf.at[ME, OTH, w_piece(p)], s_w, wp_r.at[p], xn)

    def w_to_sib(j, i, src):
        ref = w_ref.at[qs(i)] if src == ARG else wbuf.at[ME, j, qs(i)]
        return remote(ref, wbuf.at[SIB, j, qs(i)], s_ws, ws_r.at[j, i], sib)

    def p_first(i):
        r0, n, c0, m = FIRST[i]
        return remote(
            pown.at[0, 0, pl.ds(r0, n), pl.ds(c0, m)], dw_ref.at[pl.ds(r0, n), pl.ds(c0, m)],
            s_px, pa_r.at[i], xn,
        )

    def p_half(q, kt, h):
        return remote(
            pown.at[q, kt, pl.ds(h * T, T)], dw_part(q, kt * D + h * T, T), s_px, ph_r.at[q, 2 * kt + h], xn
        )

    def p_own(q, kt):
        return remote(pown.at[q, kt], dw_tile(q, kt), s_px, po_r.at[q - 2, kt], xn)

    def p_own_last():
        return remote(
            pown.at[3, 3, pl.ds(0, D - R)], dw_part(3, 3 * D, D - R), s_px, po_r.at[1, 3], xn
        )

    def tail_store():
        return local(pown.at[3, 3, pl.ds(D - R, R)], tail, tail_sem)

    def p_other(q, kt):
        return remote(poth.at[q, kt], land.at[q - 2, kt], s_po, ps_r.at[q - 2, kt], xn)

    def p_trans(q, kt, r):
        part = pl.ds(r * Q, Q)
        return remote(poth.at[q, kt, part], bufy.at[q, kt, part], s_py, pf_r.at[q, 4 * kt + r], yn)

    def p_fwd(q, kt, r):
        part = pl.ds(r * Q, Q)
        return remote(bufy.at[q, kt, part], land.at[q, kt, part], s_px, pf_r.at[q, 4 * kt + r], xn)

    def p_trans_short():
        part = pl.ds(0, F)
        return remote(poth.at[1, 3, part], bufy.at[1, 3, part], s_py, pf_r.at[1, 12], yn)

    def p_fwd_short():
        part = pl.ds(0, F)
        return remote(bufy.at[1, 3, part], land.at[1, 3, part], s_px, pf_r.at[1, 12], xn)

    def p_trans_tail():
        return remote(poth.at[1, 3, pl.ds(F, R)], tail, s_py, pf_r.at[1, 13], yn)

    def p_extra():
        return remote(poth.at[1, 3, pl.ds(D - E, E)], extra, s_ex, ex_r, xn)

    def extra_to_y():
        return remote(poth.at[1, 3, pl.ds(D - E, E)], dw_part(1, 4 * D - E, E), s_py, py_ex, yn)

    def p_term(q, kt):
        return remote(poth.at[q, kt], dw_tile(q, kt), s_py, py_r.at[q, kt], yn)

    def p_term_short():
        part = pl.ds(0, D - E)
        return remote(poth.at[1, 3, part], dw_part(1, 3 * D, D - E), s_py, py_r.at[1, 3], yn)

    def sum_short():
        part = pl.ds(0, D - E)
        return remote(poth.at[3, 3, part], dw_part(3, 3 * D, D - E), s_sum, py_r.at[3, 3], yn)

    def tail_y_store(src):
        return local(src.at[3, 3, pl.ds(D - E, E)], tail_y, tail_y_sem)

    def sum_to_y(q, kt):
        return remote(poth.at[q, kt], dw_tile(q, kt), s_sum, py_r.at[q, kt], yn)

    def drain(ref, sem):
        remote(ref, ref, sem, dyy_r.at[0], yn).wait_send()

    dy_load.start()
    for kt in range(4):
        x_load(kt).start()

    barrier = pltpu.get_barrier_semaphore()
    for dev in (sib, xn, yn):
        pl.semaphore_signal(barrier, inc=1, device_id=dev, device_id_type=MESH)
    pl.semaphore_wait(barrier, 3)

    dy_first(0).start()
    x_first(0).start()
    dy_to_y(0).start()
    dy_first(1).start()
    x_first(1).start()
    x_first(2).start()
    dy_to_y(1).start()

    @pl.when(is_a)
    def _():
        for i in range(8):
            w_own_to_x(i).start()
        for q in (2, 3):
            dy_to_y(q).start()

    @pl.when(is_b)
    def _():
        for i in range(4):
            w_to_y(i).start()
        for q in (2, 3):
            dy_to_y(q).start()
        for p in range(16):
            w_to_y_piece(p).start()

    for kt in (1, 2, 3):
        x_to_sib(kt).start()
    for q in (1, 2, 3):
        dy_to_sib(OWN, q).start()

    @pl.when(is_a)
    def _():
        for i in range(8):
            w_to_sib(OWN, i, ARG).start()

    def p_part(j, c0, k0, n, m=T):
        dy = pl.ds(c0, m)
        acc = None
        for t in range(2):
            part = pl.ds(t * N, N)
            for who, base in ((ME, k0), (SIB, H + k0)):
                term = _tdot(dx_ref[part, cut(base, n)], dyv[who, j, part, dy])
                acc = term if acc is None else acc + term
        return acc

    def p_tile(dst, j, q, kt):
        loop(2, lambda h: put(dst.at[q, kt, pl.ds(h * T, T)], p_part(j, q * T, kt * D + h * T, T)))

    def put(ref, value):
        ref[...] = value

    dy_load.wait()
    x_load(0).wait()
    dy_first(0).wait_recv()
    for i, (r0, n, c0, m) in enumerate(FIRST):
        if i == 1:
            dy_first(1).wait_recv()
        else:
            x_first(max(i - 1, 0)).wait_recv()
        put(pown.at[0, 0, pl.ds(r0, n), pl.ds(c0, m)], p_part(OWN, c0, r0, n, m))

        @pl.when(is_b)
        def _(i=i):
            p_first(i).start()

    def own_tile(q, kt):
        if q == 0:
            x_load(kt).wait()
            x_to_sib(kt).wait_recv()
        p_tile(pown, OWN, q, kt)
        if q < 2:
            @pl.when(is_b)
            def _():
                p_half(q, kt, 0).start()
                p_half(q, kt, 1).start()

    for q in range(4):
        if q > 0:
            dy_to_sib(OWN, q).wait_recv()
        loop(4, lambda kt, q=q: own_tile(q, kt), int(q == 0))

    def trans_tile(q, kt):
        if q == 0:
            for r in range(4):
                p_trans(q, kt, r).start()
            return

        @pl.when(kt < 3)
        def _():
            for r in range(4):
                p_trans(q, kt, r).start()

        @pl.when(kt == 3)
        def _():
            p_trans_short().start()
            p_trans_tail().start()
            p_extra().start()

    def dy_in(q):
        dy_to_y(q).wait_recv()
        dy_to_sib(OTH, q).start()

    def other_pass(q):
        dy_in(q)
        dy_to_sib(OTH, q).wait_recv()

        def tile(kt):
            p_tile(poth, OTH, q, kt)
            if q < 2:
                @pl.when(jnp.logical_and(is_a, 4 * q + kt < 7))
                def _():
                    p_term(q, kt).start()

                @pl.when(jnp.logical_and(is_a, 4 * q + kt == 7))
                def _():
                    p_term_short().start()

                @pl.when(is_b)
                def _():
                    trans_tile(q, kt)
            else:
                @pl.when(is_b)
                def _():
                    p_other(q, kt).start()

        loop(4, tile)

    def w_loads(d, cc, src):
        ref = w_ref.at[qs(d)] if src == ARG else wbuf.at[cc, OWN, qs(d)]
        return (
            local(ref, wv.at[cc, OWN], wl_sem.at[cc, OWN]),
            local(wbuf.at[cc, OTH, qs(d)], wv.at[cc, OTH], wl_sem.at[cc, OTH]),
        )

    def start_loads(d, cc, src):
        for cp in w_loads(d, cc, src):
            cp.start()

    def wait_loads(d, cc, src):
        for cp in w_loads(d, cc, src):
            cp.wait()

    def dx_stripe(d, cc, lo=0, hi=4):
        cols = cut((c + cc * (1 - 2 * c)) * H + d * T, T, T)

        def rows(m):
            part = pl.ds(m * D, D)
            dx_ref[part, cols] = (
                _dot_t(dyv[ME, OWN, part, :], wv[cc, OWN]) + _dot_t(dyv[ME, OTH, part, :], wv[cc, OTH])
            ).astype(BF16)

        loop(hi, rows, lo)

    def pair_wait(d, src):
        w_to_sib(OWN, d, src).wait_recv()
        w_to_sib(OTH, d, BUF).wait_recv()

    other_pass(0)
    other_pass(1)

    @pl.when(is_a)
    def _():
        def add(q, kt):
            tile = dw_tile(q, kt)
            tile[...] = tile[...] + pown[q, kt]

        def final_early(t):
            q, kt = t // 4, t % 4

            @pl.when(t == 0)
            def _():
                for i in range(len(FIRST)):
                    p_first(i).wait_recv()

            @pl.when(t > 0)
            def _():
                p_half(q, kt, 0).wait_recv()
                p_half(q, kt, 1).wait_recv()
            add(q, kt)

        def final_late(t):
            q, kt = 2 + t // 4, t % 4
            p_own(q, kt).wait_recv()
            add(q, kt)

        def a_sum(q, kt):
            p_other(q, kt).wait_recv()
            poth[q, kt] = poth[q, kt] + land[q - 2, kt]

            @pl.when(4 * q + kt < 15)
            def _():
                sum_to_y(q, kt).start()

            @pl.when(4 * q + kt == 15)
            def _():
                sum_short().start()
                tail_y_store(poth).start()

        def early(i):
            w_to_y(i).wait_recv()
            w_fwd(i).start()
            w_to_sib(OTH, i, BUF).start()
            final_early(i)

        loop(4, early)
        dy_in(2)
        dy_to_sib(OTH, 2).wait_recv()

        def q2_tile(kt):
            p_tile(poth, OTH, 2, kt)
            final_early(4 + kt)

        loop(4, q2_tile)
        p_extra().wait_recv()
        poth[1, 3, D - E:] = poth[1, 3, D - E:] + extra[...]
        extra_to_y().start()
        start_loads(0, ME, ARG)
        dy_in(3)

        def step(i):
            @pl.when(i < 16)
            def _():
                w_to_y_piece(i).wait_recv()
                w_fwd_piece(i).start()

                @pl.when(i % 4 == 3)
                def _():
                    w_to_sib(OTH, 4 + i // 4, BUF).start()

            @pl.when(i >= 16)
            def _():
                k = i - 16
                q, kt, r = k // 16, (k // 4) % 4, k % 4
                p_trans(q, kt, r).wait_recv()
                p_fwd(q, kt, r).start()

            @pl.when(i == 0)
            def _():
                dy_to_sib(OTH, 3).wait_recv()

            @pl.when(i < 4)
            def _():
                p_tile(poth, OTH, 3, i)

            @pl.when(jnp.logical_and(i >= 4, i < 36))
            def _():
                e = (i - 4) // 2
                d, cc = e // 2, e % 2
                odd = i % 2

                @pl.when(jnp.logical_and(odd == 0, cc == ME))
                def _():
                    pair_wait(d, ARG)
                    start_loads(d, SIB, BUF)
                    wait_loads(d, ME, ARG)

                @pl.when(jnp.logical_and(odd == 0, cc == SIB))
                def _():
                    @pl.when(d < 7)
                    def _():
                        start_loads(d + 1, ME, ARG)
                    wait_loads(d, SIB, BUF)

                dx_stripe(d, cc, 2 * odd, 2 * odd + 2)

            @pl.when(jnp.logical_and(i < 8, i % 2 == 1))
            def _():
                a_sum(2, i // 2)

            @pl.when(jnp.logical_and(jnp.logical_and(i >= 10, i < 26), i % 4 == 2))
            def _():
                a_sum(3, (i - 10) // 4)

            @pl.when(jnp.logical_and(i >= 26, i % 4 == 2))
            def _():
                final_late((i - 26) // 4)

        loop(44, step)
        p_trans_short().wait_recv()
        p_fwd_short().start()
        low = dw_part(3, 4 * D - R, R)
        low[...] = pown[3, 3, D - R:]
        final_late(5)
        final_late(6)
        p_trans_tail().wait_recv()
        p_own_last().wait_recv()
        top = dw_part(3, 3 * D, D - R)
        top[...] = top[...] + pown[3, 3, :D - R]
        drain(wbuf.at[ME], s_w)
        tail_y_store(poth).wait()
        drain(dyv.at[ME, OWN, pl.ds(0, H - (E + R) // 2)], s_px)
        drain(land, s_py)
        drain(dyv.at[ME, OWN, pl.ds(0, H - E // 2)], s_sum)

    @pl.when(is_b)
    def _():
        other_pass(2)
        other_pass(3)
        for t in range(7):
            p_own(2 + t // 4, t % 4).start()
        p_own_last().start()
        tail_store().start()
        tail_y_store(pown).start()

        def own_w(i):
            w_own_to_x(i).wait_recv()
            w_to_sib(OWN, i, BUF).start()

        loop(8, own_w)

        def stripes(d):
            @pl.when(d < 4)
            def _():
                w_to_y(d).wait_recv()

            @pl.when(d >= 4)
            def _():
                for p in range(4):
                    w_to_y_piece(4 * (d - 4) + p).wait_recv()
            w_to_sib(OTH, d, BUF).start()
            start_loads(d, ME, BUF)
            pair_wait(d, BUF)
            start_loads(d, SIB, BUF)
            for cc in (ME, SIB):
                wait_loads(d, cc, BUF)
                dx_stripe(d, cc)

        loop(8, stripes)

        def fin(i):
            q, kt, r = i // 16, (i // 4) % 4, i % 4

            @pl.when(r == 0)
            def _():
                p_term(q, kt).wait_recv()
            p_fwd(q, kt, r).wait_recv()
            tile = dw_part(q, kt * D + r * Q, Q)
            tile[...] = tile[...] + land[q, kt, pl.ds(r * Q, Q)]

        loop(28, fin)
        p_term_short().wait_recv()
        p_fwd_short().wait_recv()
        tile = dw_part(1, 3 * D, F)
        tile[...] = tile[...] + land[1, 3, :F]
        extra_to_y().wait_recv()
        for t in range(7):
            sum_to_y(2 + t // 4, t % 4).wait_recv()
        sum_short().wait_recv()
        tail_y_store(pown).wait()
        tail_store().wait()
        drain(wbuf.at[ME, OWN], s_w)
        drain(dw_ref.at[pl.ds(0, H - R // 4)], s_px)
        drain(land, s_po)
        drain(extra, s_ex)
        drain(dyv.at[ME, OWN, pl.ds(0, H - E // 2)], s_py)

    drain(dyv.at[ME], s_dys)
    drain(dyv.at[ME, OWN], s_dyy)
    drain(wbuf.at[ME], s_xs)
    drain(wbuf.at[ME], s_ws)


def store_kernel(dx_ref, dw_ref, dx_out, dw_out, sem):
    copies = []
    for i in range(4):
        part = pl.ds(i * D, D)
        copies.append(pltpu.make_async_copy(dx_ref.at[part], dx_out.at[part], sem.at[0, i]))
        copies.append(pltpu.make_async_copy(dw_ref.at[part], dw_out.at[part], sem.at[1, i]))
    for cp in copies:
        cp.start()
    for cp in copies:
        cp.wait()


def add_kernel(done_ref, dw_ref, tail_ref, tail_y_ref, dw_out, buf, buf_y, sem, sem_y):
    is_a = lax.axis_index("row") // 2 == lax.axis_index("col")
    rows = cut(jnp.where(is_a, H - R, 3 * D + F), R, 32)
    cols = cut(jnp.where(is_a, 3 * T, T), T)
    buf[...] = dw_ref[rows, cols] + tail_ref[...]
    first = pltpu.make_async_copy(buf, dw_out.at[rows, cols], sem)
    first.start()
    rows_y, cols_y = pl.ds(H - E, E), cut(jnp.where(is_a, 0, 3 * T), T)
    buf_y[...] = jnp.where(is_a, dw_ref[rows_y, cols_y], tail_y_ref[...])
    second = pltpu.make_async_copy(buf_y, dw_out.at[rows_y, cols_y], sem_y)
    second.start()
    first.wait()
    second.wait()


def local_backward(act_blk, w_blk, grad_blk):
    any_spec = pl.BlockSpec(memory_space=pl.ANY)
    vmem_spec = pl.BlockSpec(memory_space=pltpu.VMEM)
    dma = pltpu.SemaphoreType.DMA
    outs = pl.pallas_call(
        kernel,
        out_shape=(
            pltpu.VMEM((H, 2 * H), BF16),
            pltpu.VMEM((H, N), F32),
            jax.ShapeDtypeStruct((2, 2, H, N), BF16),
            jax.ShapeDtypeStruct((2, 4, D, T), F32),
            jax.ShapeDtypeStruct((R, T), F32),
            jax.ShapeDtypeStruct((E, T), F32),
        ),
        in_specs=[any_spec] * 3,
        out_specs=(vmem_spec,) * 2 + (any_spec,) * 4,
        scratch_shapes=[
            pltpu.VMEM((2, 2, H, N), BF16),
            pltpu.VMEM((4, 4, D, T), F32),
            pltpu.VMEM((4, 4, D, T), F32),
            pltpu.VMEM((2, 2, T, N), BF16),
            pltpu.VMEM((2, 4, D, T), F32),
            pltpu.VMEM((E, T), F32),
            dma, dma((4,)), dma((2, 4)), dma((4,)), dma((4,)), dma((5,)), dma((2, 8)), dma((16,)), dma((2, 8)),
            dma((4,)), dma((2, 8)), dma((2, 4)), dma((2, 4)), dma((4, 4)), dma((2, 16)),
            dma, dma, dma, dma, dma, dma, dma, dma, dma, dma((2, 2)), dma,
            dma, dma, dma, dma,
        ],
        compiler_params=pltpu.CompilerParams(
            collective_id=0, has_side_effects=True, vmem_limit_bytes=41_800_000
        ),
        cost_estimate=pl.CostEstimate(flops=8 * H * H * H, bytes_accessed=100 << 20, transcendentals=0),
    )(act_blk, w_blk, grad_blk)
    tail = lax.ppermute(outs[4], "row", [(i, (i + 2) % 4) for i in range(4)])
    tail_y = lax.ppermute(outs[5], "col", [(0, 1), (1, 0)])
    dx, dw = pl.pallas_call(
        store_kernel,
        out_shape=(jax.ShapeDtypeStruct((H, 2 * H), BF16), jax.ShapeDtypeStruct((H, N), F32)),
        in_specs=[vmem_spec] * 2,
        out_specs=(any_spec,) * 2,
        scratch_shapes=[dma((2, 4))],
        compiler_params=pltpu.CompilerParams(vmem_limit_bytes=1 << 20),
        cost_estimate=pl.CostEstimate(flops=0, bytes_accessed=48 << 20, transcendentals=0),
    )(outs[0], outs[1])
    dw = pl.pallas_call(
        add_kernel,
        out_shape=jax.ShapeDtypeStruct((H, N), F32),
        in_specs=[any_spec] + [vmem_spec] * 3,
        out_specs=any_spec,
        scratch_shapes=[pltpu.VMEM((R, T), F32), pltpu.VMEM((E, T), F32), dma, dma],
        input_output_aliases={0: 0},
        compiler_params=pltpu.CompilerParams(vmem_limit_bytes=2 << 20),
        cost_estimate=pl.CostEstimate(flops=0, bytes_accessed=1 << 20, transcendentals=0),
    )(dw, outs[1], tail, tail_y)
    return dx, dw


def solution(mesh):
    io_spec = P(("dp", "row"), "col")
    w_spec = P("row", "col")
    return jax.shard_map(
        local_backward, mesh=mesh, in_specs=(io_spec, w_spec, io_spec), out_specs=(io_spec, io_spec), check_vma=False
    )
```

```python
import jax
import jax.numpy as jnp
from jax import lax
from jax.experimental import pallas as pl
from jax.experimental.pallas import tpu as pltpu
from jax.sharding import PartitionSpec as P

MESH = pl.DeviceIdType.MESH
F32 = jnp.float32
BF16 = jnp.bfloat16
H, N, D, T, Q, S = 2048, 1024, 512, 256, 128, 64
R = 352
E = 128
F = D - E - R
ME, SIB = 0, 1
OWN, OTH = 0, 1
ARG, BUF = "arg", "buf"
FIRST = ((0, Q, 0, Q), (0, Q, Q, Q), (Q, Q, 0, T), (T, T, 0, T))


def _tdot(a, b):
    return lax.dot_general(a, b, (((0,), (0,)), ((), ())), preferred_element_type=F32)


def _dot_t(a, b):
    return lax.dot_general(a, b, (((1,), (1,)), ((), ())), preferred_element_type=F32)


def loop(n, f, start=0):
    def body(i, carry):
        f(i)
        return carry

    lax.fori_loop(start, n, body, start)


def cut(k0, n, unit=Q):
    return pl.ds(pl.multiple_of(k0, unit), n)


def kernel(
    x_ref, w_ref, dy_ref,
    dx_ref, dw_ref, wbuf, bufy, tail, tail_y,
    dyv, pown, poth, wv, land, extra,
    dy_sem, x_sem, dys_r, dyy_r, xs_r, xf_r, w_r, wp_r, ws_r, pa_r, ph_r, po_r, ps_r, py_r, pf_r,
    s_dys, s_dyy, s_xs, s_w, s_ws, s_px, s_po, s_py, s_sum, wl_sem, tail_sem, tail_y_sem, s_ex, ex_r, py_ex, dyq_sem, xt_sem, s_x0,
):
    row = lax.axis_index("row")
    y = lax.axis_index("col")
    x = row // 2
    c = row % 2
    is_a = x == y
    is_b = x != y
    sib = {"row": row + 1 - 2 * c}
    xn = {"row": (row + 2) % 4}
    yn = {"col": 1 - y}

    def remote(src, dst, ssem, rsem, dev):
        return pltpu.make_async_remote_copy(
            src_ref=src, dst_ref=dst, send_sem=ssem, recv_sem=rsem, device_id=dev, device_id_type=MESH
        )

    def local(src, dst, sem):
        return pltpu.make_async_copy(src, dst, sem)

    def qs(q):
        return pl.ds(q * T, T)

    def xo(k0, n):
        return dx_ref.at[:, cut(k0, n)]

    def xs(k0, n):
        return dx_ref.at[:, cut(H + k0, n)]

    def dw_part(q, r0, n):
        return dw_ref.at[pl.ds(r0, n), cut(q * T, T)]

    def dw_tile(q, kt):
        return dw_part(q, kt * D, D)

    dyq_load = local(dy_ref.at[:, pl.ds(0, T)], dyv.at[ME, OWN, :, pl.ds(0, T)], dyq_sem)
    dy_load = local(dy_ref.at[:, pl.ds(T, N - T)], dyv.at[ME, OWN, :, pl.ds(T, N - T)], dy_sem)
    xt_load = local(x_ref.at[:, pl.ds((1 - c) * H, Q)], xo(3 * D, Q), xt_sem)
    x_first_piece = remote(xo(3 * D, Q), xs(0, Q), s_x0, xf_r.at[0], sib)

    def x_load(kt):
        return local(x_ref.at[:, pl.ds(c * H + kt * D, D)], xo(kt * D, D), x_sem.at[kt])

    def x_cols_to_sib(k0, n, sem):
        return remote(x_ref.at[:, pl.ds((1 - c) * H + k0, n)], xs(k0, n), s_xs, sem, sib)

    def x_to_sib(kt):
        return x_cols_to_sib(kt * D, D, xs_r.at[kt])

    def x_first(i):
        if i == 0:
            return x_first_piece
        return x_cols_to_sib(i * Q, i * Q, xf_r.at[i])

    def dy_first(i):
        cols = pl.ds(i * Q, Q)
        return remote(dyv.at[ME, OWN, :, cols], dyv.at[SIB, OWN, :, cols], s_dys, xf_r.at[3 + i], sib)

    def dy_to_sib(j, q):
        src = dy_ref.at[:, qs(q)] if j == OWN else dyv.at[ME, OTH, :, qs(q)]
        return remote(src, dyv.at[SIB, j, :, qs(q)], s_dys, dys_r.at[j, q], sib)

    def dy_to_y(q):
        return remote(dy_ref.at[:, qs(q)], dyv.at[ME, OTH, :, qs(q)], s_dyy, dyy_r.at[q], yn)

    def w_own_to_x(i):
        return remote(w_ref.at[qs(i)], wbuf.at[ME, OWN, qs(i)], s_w, w_r.at[OWN, i], xn)

    def w_to_y(i):
        return remote(w_ref.at[qs(i)], wbuf.at[ME, OTH, qs(i)], s_w, w_r.at[OTH, i], yn)

    def w_fwd(i):
        return remote(wbuf.at[ME, OTH, qs(i)], wbuf.at[ME, OTH, qs(i)], s_w, w_r.at[OTH, i], xn)

    def w_piece(p):
        return pl.ds(N + p * S, S)

    def w_to_y_piece(p):
        return remote(w_ref.at[w_piece(p)], wbuf.at[ME, OTH, w_piece(p)], s_w, wp_r.at[p], yn)

    def w_fwd_piece(p):
        return remote(wbuf.at[ME, OTH, w_piece(p)], wbuf.at[ME, OTH, w_piece(p)], s_w, wp_r.at[p], xn)

    def w_to_sib(j, i, src):
        ref = w_ref.at[qs(i)] if src == ARG else wbuf.at[ME, j, qs(i)]
        return remote(ref, wbuf.at[SIB, j, qs(i)], s_ws, ws_r.at[j, i], sib)

    def p_first(i):
        r0, n, c0, m = FIRST[i]
        return remote(
            pown.at[0, 0, pl.ds(r0, n), pl.ds(c0, m)], dw_ref.at[pl.ds(r0, n), pl.ds(c0, m)],
            s_px, pa_r.at[i], xn,
        )

    def p_half(q, kt, h):
        return remote(
            pown.at[q, kt, pl.ds(h * T, T)], dw_part(q, kt * D + h * T, T), s_px, ph_r.at[q, 2 * kt + h], xn
        )

    def p_own(q, kt):
        return remote(pown.at[q, kt], dw_tile(q, kt), s_px, po_r.at[q - 2, kt], xn)

    def p_own_last():
        return remote(
            pown.at[3, 3, pl.ds(0, D - R)], dw_part(3, 3 * D, D - R), s_px, po_r.at[1, 3], xn
        )

    def tail_store():
        return local(pown.at[3, 3, pl.ds(D - R, R)], tail, tail_sem)

    def p_other(q, kt):
        return remote(poth.at[q, kt], land.at[q - 2, kt], s_po, ps_r.at[q - 2, kt], xn)

    def p_trans(q, kt, r):
        part = pl.ds(r * Q, Q)
        return remote(poth.at[q, kt, part], bufy.at[q, kt, part], s_py, pf_r.at[q, 4 * kt + r], yn)

    def p_fwd(q, kt, r):
        part = pl.ds(r * Q, Q)
        return remote(bufy.at[q, kt, part], land.at[q, kt, part], s_px, pf_r.at[q, 4 * kt + r], xn)

    def p_trans_short():
        part = pl.ds(0, F)
        return remote(poth.at[1, 3, part], bufy.at[1, 3, part], s_py, pf_r.at[1, 12], yn)

    def p_fwd_short():
        part = pl.ds(0, F)
        return remote(bufy.at[1, 3, part], land.at[1, 3, part], s_px, pf_r.at[1, 12], xn)

    def p_trans_tail():
        return remote(poth.at[1, 3, pl.ds(F, R)], tail, s_py, pf_r.at[1, 13], yn)

    def p_extra():
        return remote(poth.at[1, 3, pl.ds(D - E, E)], extra, s_ex, ex_r, xn)

    def extra_to_y():
        return remote(poth.at[1, 3, pl.ds(D - E, E)], dw_part(1, 4 * D - E, E), s_py, py_ex, yn)

    def p_term(q, kt):
        return remote(poth.at[q, kt], dw_tile(q, kt), s_py, py_r.at[q, kt], yn)

    def p_term_short():
        part = pl.ds(0, D - E)
        return remote(poth.at[1, 3, part], dw_part(1, 3 * D, D - E), s_py, py_r.at[1, 3], yn)

    def sum_short():
        part = pl.ds(0, D - E)
        return remote(poth.at[3, 3, part], dw_part(3, 3 * D, D - E), s_sum, py_r.at[3, 3], yn)

    def tail_y_store(src):
        return local(src.at[3, 3, pl.ds(D - E, E)], tail_y, tail_y_sem)

    def sum_to_y(q, kt):
        return remote(poth.at[q, kt], dw_tile(q, kt), s_sum, py_r.at[q, kt], yn)

    def drain(ref, sem):
        remote(ref, ref, sem, dyy_r.at[0], yn).wait_send()

    for cp in (dyq_load, xt_load, x_load(0), dy_load, x_load(1), x_load(2)):
        cp.start()

    barrier = pltpu.get_barrier_semaphore()
    for dev in (sib, xn, yn):
        pl.semaphore_signal(barrier, inc=1, device_id=dev, device_id_type=MESH)
    pl.semaphore_wait(barrier, 3)

    dy_to_y(0).start()

    @pl.when(is_a)
    def _():
        w_own_to_x(0).start()

    dyq_load.wait()
    dy_first(0).start()
    xt_load.wait()
    x_first(0).start()
    dy_first(1).start()
    x_first(1).start()
    x_first(2).start()
    dy_to_y(1).start()

    @pl.when(is_a)
    def _():
        for i in range(1, 8):
            w_own_to_x(i).start()
        for q in (2, 3):
            dy_to_y(q).start()

    @pl.when(is_b)
    def _():
        for i in range(4):
            w_to_y(i).start()
        for q in (2, 3):
            dy_to_y(q).start()
        for p in range(16):
            w_to_y_piece(p).start()

    for kt in (1, 2, 3):
        x_to_sib(kt).start()
    for q in (1, 2, 3):
        dy_to_sib(OWN, q).start()

    @pl.when(is_a)
    def _():
        for i in range(8):
            w_to_sib(OWN, i, ARG).start()

    def p_part(j, c0, k0, n, m=T):
        dy = pl.ds(c0, m)
        acc = None
        for t in range(2):
            part = pl.ds(t * N, N)
            for who, base in ((ME, k0), (SIB, H + k0)):
                term = _tdot(dx_ref[part, cut(base, n)], dyv[who, j, part, dy])
                acc = term if acc is None else acc + term
        return acc

    def p_tile(dst, j, q, kt):
        loop(2, lambda h: put(dst.at[q, kt, pl.ds(h * T, T)], p_part(j, q * T, kt * D + h * T, T)))

    def put(ref, value):
        ref[...] = value

    x_load(0).wait()
    dy_first(0).wait_recv()
    for i, (r0, n, c0, m) in enumerate(FIRST):
        if i == 1:
            dy_first(1).wait_recv()
        else:
            x_first(max(i - 1, 0)).wait_recv()
        put(pown.at[0, 0, pl.ds(r0, n), pl.ds(c0, m)], p_part(OWN, c0, r0, n, m))

        @pl.when(is_b)
        def _(i=i):
            p_first(i).start()

    x_first(0).wait_send()
    x_load(3).start()
    dy_load.wait()

    def own_tile(q, kt):
        if q == 0:
            x_load(kt).wait()
            x_to_sib(kt).wait_recv()
        p_tile(pown, OWN, q, kt)
        if q < 2:
            @pl.when(is_b)
            def _():
                p_half(q, kt, 0).start()
                p_half(q, kt, 1).start()

    for q in range(4):
        if q > 0:
            dy_to_sib(OWN, q).wait_recv()
        loop(4, lambda kt, q=q: own_tile(q, kt), int(q == 0))

    def trans_tile(q, kt):
        if q == 0:
            for r in range(4):
                p_trans(q, kt, r).start()
            return

        @pl.when(kt < 3)
        def _():
            for r in range(4):
                p_trans(q, kt, r).start()

        @pl.when(kt == 3)
        def _():
            p_trans_short().start()
            p_trans_tail().start()
            p_extra().start()

    def dy_in(q):
        dy_to_y(q).wait_recv()
        dy_to_sib(OTH, q).start()

    def other_pass(q):
        dy_in(q)
        dy_to_sib(OTH, q).wait_recv()

        def tile(kt):
            p_tile(poth, OTH, q, kt)
            if q < 2:
                @pl.when(jnp.logical_and(is_a, 4 * q + kt < 7))
                def _():
                    p_term(q, kt).start()

                @pl.when(jnp.logical_and(is_a, 4 * q + kt == 7))
                def _():
                    p_term_short().start()

                @pl.when(is_b)
                def _():
                    trans_tile(q, kt)
            else:
                @pl.when(is_b)
                def _():
                    p_other(q, kt).start()

        loop(4, tile)

    def w_loads(d, cc, src):
        ref = w_ref.at[qs(d)] if src == ARG else wbuf.at[cc, OWN, qs(d)]
        return (
            local(ref, wv.at[cc, OWN], wl_sem.at[cc, OWN]),
            local(wbuf.at[cc, OTH, qs(d)], wv.at[cc, OTH], wl_sem.at[cc, OTH]),
        )

    def start_loads(d, cc, src):
        for cp in w_loads(d, cc, src):
            cp.start()

    def wait_loads(d, cc, src):
        for cp in w_loads(d, cc, src):
            cp.wait()

    def dx_stripe(d, cc, lo=0, hi=4):
        cols = cut((c + cc * (1 - 2 * c)) * H + d * T, T, T)

        def rows(m):
            part = pl.ds(m * D, D)
            dx_ref[part, cols] = (
                _dot_t(dyv[ME, OWN, part, :], wv[cc, OWN]) + _dot_t(dyv[ME, OTH, part, :], wv[cc, OTH])
            ).astype(BF16)

        loop(hi, rows, lo)

    def pair_wait(d, src):
        w_to_sib(OWN, d, src).wait_recv()
        w_to_sib(OTH, d, BUF).wait_recv()

    other_pass(0)
    other_pass(1)

    @pl.when(is_a)
    def _():
        def add(q, kt):
            tile = dw_tile(q, kt)
            tile[...] = tile[...] + pown[q, kt]

        def final_early(t):
            q, kt = t // 4, t % 4

            @pl.when(t == 0)
            def _():
                for i in range(len(FIRST)):
                    p_first(i).wait_recv()

            @pl.when(t > 0)
            def _():
                p_half(q, kt, 0).wait_recv()
                p_half(q, kt, 1).wait_recv()
            add(q, kt)

        def final_late(t):
            q, kt = 2 + t // 4, t % 4
            p_own(q, kt).wait_recv()
            add(q, kt)

        def a_sum(q, kt):
            p_other(q, kt).wait_recv()
            poth[q, kt] = poth[q, kt] + land[q - 2, kt]

            @pl.when(4 * q + kt < 15)
            def _():
                sum_to_y(q, kt).start()

            @pl.when(4 * q + kt == 15)
            def _():
                sum_short().start()
                tail_y_store(poth).start()

        def early(i):
            w_to_y(i).wait_recv()
            w_fwd(i).start()
            w_to_sib(OTH, i, BUF).start()
            final_early(i)

        loop(4, early)
        dy_in(2)
        dy_to_sib(OTH, 2).wait_recv()

        def q2_tile(kt):
            p_tile(poth, OTH, 2, kt)
            final_early(4 + kt)

        loop(4, q2_tile)
        p_extra().wait_recv()
        poth[1, 3, D - E:] = poth[1, 3, D - E:] + extra[...]
        extra_to_y().start()
        start_loads(0, ME, ARG)
        dy_in(3)

        def step(i):
            @pl.when(i < 16)
            def _():
                w_to_y_piece(i).wait_recv()
                w_fwd_piece(i).start()

                @pl.when(i % 4 == 3)
                def _():
                    w_to_sib(OTH, 4 + i // 4, BUF).start()

            @pl.when(i >= 16)
            def _():
                k = i - 16
                q, kt, r = k // 16, (k // 4) % 4, k % 4
                p_trans(q, kt, r).wait_recv()
                p_fwd(q, kt, r).start()

            @pl.when(i == 0)
            def _():
                dy_to_sib(OTH, 3).wait_recv()

            @pl.when(i < 4)
            def _():
                p_tile(poth, OTH, 3, i)

            @pl.when(jnp.logical_and(i >= 4, i < 36))
            def _():
                e = (i - 4) // 2
                d, cc = e // 2, e % 2
                odd = i % 2

                @pl.when(jnp.logical_and(odd == 0, cc == ME))
                def _():
                    pair_wait(d, ARG)
                    start_loads(d, SIB, BUF)
                    wait_loads(d, ME, ARG)

                @pl.when(jnp.logical_and(odd == 0, cc == SIB))
                def _():
                    @pl.when(d < 7)
                    def _():
                        start_loads(d + 1, ME, ARG)
                    wait_loads(d, SIB, BUF)

                dx_stripe(d, cc, 2 * odd, 2 * odd + 2)

            @pl.when(jnp.logical_and(i < 8, i % 2 == 1))
            def _():
                a_sum(2, i // 2)

            @pl.when(jnp.logical_and(jnp.logical_and(i >= 10, i < 26), i % 4 == 2))
            def _():
                a_sum(3, (i - 10) // 4)

            @pl.when(jnp.logical_and(i >= 26, i % 4 == 2))
            def _():
                final_late((i - 26) // 4)

        loop(44, step)
        p_trans_short().wait_recv()
        p_fwd_short().start()
        low = dw_part(3, 4 * D - R, R)
        low[...] = pown[3, 3, D - R:]
        final_late(5)
        final_late(6)
        p_trans_tail().wait_recv()
        p_own_last().wait_recv()
        top = dw_part(3, 3 * D, D - R)
        top[...] = top[...] + pown[3, 3, :D - R]
        drain(wbuf.at[ME], s_w)
        tail_y_store(poth).wait()
        drain(dyv.at[ME, OWN, pl.ds(0, H - (E + R) // 2)], s_px)
        drain(land, s_py)
        drain(dyv.at[ME, OWN, pl.ds(0, H - E // 2)], s_sum)

    @pl.when(is_b)
    def _():
        other_pass(2)
        other_pass(3)
        for t in range(7):
            p_own(2 + t // 4, t % 4).start()
        p_own_last().start()
        tail_store().start()
        tail_y_store(pown).start()

        def own_w(i):
            w_own_to_x(i).wait_recv()
            w_to_sib(OWN, i, BUF).start()

        loop(8, own_w)

        def stripes(d):
            @pl.when(d < 4)
            def _():
                w_to_y(d).wait_recv()

            @pl.when(d >= 4)
            def _():
                for p in range(4):
                    w_to_y_piece(4 * (d - 4) + p).wait_recv()
            w_to_sib(OTH, d, BUF).start()
            start_loads(d, ME, BUF)
            pair_wait(d, BUF)
            start_loads(d, SIB, BUF)
            for cc in (ME, SIB):
                wait_loads(d, cc, BUF)
                dx_stripe(d, cc)

        loop(8, stripes)

        def fin(i):
            q, kt, r = i // 16, (i // 4) % 4, i % 4

            @pl.when(r == 0)
            def _():
                p_term(q, kt).wait_recv()
            p_fwd(q, kt, r).wait_recv()
            tile = dw_part(q, kt * D + r * Q, Q)
            tile[...] = tile[...] + land[q, kt, pl.ds(r * Q, Q)]

        loop(28, fin)
        p_term_short().wait_recv()
        p_fwd_short().wait_recv()
        tile = dw_part(1, 3 * D, F)
        tile[...] = tile[...] + land[1, 3, :F]
        extra_to_y().wait_recv()
        for t in range(7):
            sum_to_y(2 + t // 4, t % 4).wait_recv()
        sum_short().wait_recv()
        tail_y_store(pown).wait()
        tail_store().wait()
        drain(wbuf.at[ME, OWN], s_w)
        drain(dw_ref.at[pl.ds(0, H - R // 4)], s_px)
        drain(land, s_po)
        drain(extra, s_ex)
        drain(dyv.at[ME, OWN, pl.ds(0, H - E // 2)], s_py)

    drain(dyv.at[ME], s_dys)
    drain(dyv.at[ME, OWN], s_dyy)
    drain(dx_ref.at[:, pl.ds(0, H - Q)], s_xs)
    drain(wbuf.at[ME], s_ws)


def store_kernel(dx_ref, dw_ref, dx_out, dw_out, sem):
    copies = []
    for i in range(4):
        part = pl.ds(i * D, D)
        copies.append(pltpu.make_async_copy(dx_ref.at[part], dx_out.at[part], sem.at[0, i]))
        copies.append(pltpu.make_async_copy(dw_ref.at[part], dw_out.at[part], sem.at[1, i]))
    for cp in copies:
        cp.start()
    for cp in copies:
        cp.wait()


def add_kernel(done_ref, dw_ref, tail_ref, tail_y_ref, dw_out, buf, buf_y, sem, sem_y):
    is_a = lax.axis_index("row") // 2 == lax.axis_index("col")
    rows = cut(jnp.where(is_a, H - R, 3 * D + F), R, 32)
    cols = cut(jnp.where(is_a, 3 * T, T), T)
    buf[...] = dw_ref[rows, cols] + tail_ref[...]
    first = pltpu.make_async_copy(buf, dw_out.at[rows, cols], sem)
    first.start()
    rows_y, cols_y = pl.ds(H - E, E), cut(jnp.where(is_a, 0, 3 * T), T)
    buf_y[...] = jnp.where(is_a, dw_ref[rows_y, cols_y], tail_y_ref[...])
    second = pltpu.make_async_copy(buf_y, dw_out.at[rows_y, cols_y], sem_y)
    second.start()
    first.wait()
    second.wait()


def local_backward(act_blk, w_blk, grad_blk):
    any_spec = pl.BlockSpec(memory_space=pl.ANY)
    vmem_spec = pl.BlockSpec(memory_space=pltpu.VMEM)
    dma = pltpu.SemaphoreType.DMA
    outs = pl.pallas_call(
        kernel,
        out_shape=(
            pltpu.VMEM((H, 2 * H), BF16),
            pltpu.VMEM((H, N), F32),
            jax.ShapeDtypeStruct((2, 2, H, N), BF16),
            jax.ShapeDtypeStruct((2, 4, D, T), F32),
            jax.ShapeDtypeStruct((R, T), F32),
            jax.ShapeDtypeStruct((E, T), F32),
        ),
        in_specs=[any_spec] * 3,
        out_specs=(vmem_spec,) * 2 + (any_spec,) * 4,
        scratch_shapes=[
            pltpu.VMEM((2, 2, H, N), BF16),
            pltpu.VMEM((4, 4, D, T), F32),
            pltpu.VMEM((4, 4, D, T), F32),
            pltpu.VMEM((2, 2, T, N), BF16),
            pltpu.VMEM((2, 4, D, T), F32),
            pltpu.VMEM((E, T), F32),
            dma, dma((4,)), dma((2, 4)), dma((4,)), dma((4,)), dma((5,)), dma((2, 8)), dma((16,)), dma((2, 8)),
            dma((4,)), dma((2, 8)), dma((2, 4)), dma((2, 4)), dma((4, 4)), dma((2, 16)),
            dma, dma, dma, dma, dma, dma, dma, dma, dma, dma((2, 2)), dma,
            dma, dma, dma, dma, dma, dma, dma,
        ],
        compiler_params=pltpu.CompilerParams(
            collective_id=0, has_side_effects=True, vmem_limit_bytes=41_800_000
        ),
        cost_estimate=pl.CostEstimate(flops=8 * H * H * H, bytes_accessed=100 << 20, transcendentals=0),
    )(act_blk, w_blk, grad_blk)
    tail = lax.ppermute(outs[4], "row", [(i, (i + 2) % 4) for i in range(4)])
    tail_y = lax.ppermute(outs[5], "col", [(0, 1), (1, 0)])
    dx, dw = pl.pallas_call(
        store_kernel,
        out_shape=(jax.ShapeDtypeStruct((H, 2 * H), BF16), jax.ShapeDtypeStruct((H, N), F32)),
        in_specs=[vmem_spec] * 2,
        out_specs=(any_spec,) * 2,
        scratch_shapes=[dma((2, 4))],
        compiler_params=pltpu.CompilerParams(vmem_limit_bytes=1 << 20),
        cost_estimate=pl.CostEstimate(flops=0, bytes_accessed=48 << 20, transcendentals=0),
    )(outs[0], outs[1])
    dw = pl.pallas_call(
        add_kernel,
        out_shape=jax.ShapeDtypeStruct((H, N), F32),
        in_specs=[any_spec] + [vmem_spec] * 3,
        out_specs=any_spec,
        scratch_shapes=[pltpu.VMEM((R, T), F32), pltpu.VMEM((E, T), F32), dma, dma],
        input_output_aliases={0: 0},
        compiler_params=pltpu.CompilerParams(vmem_limit_bytes=2 << 20),
        cost_estimate=pl.CostEstimate(flops=0, bytes_accessed=1 << 20, transcendentals=0),
    )(dw, outs[1], tail, tail_y)
    return dx, dw


def solution(mesh):
    io_spec = P(("dp", "row"), "col")
    w_spec = P("row", "col")
    return jax.shard_map(
        local_backward, mesh=mesh, in_specs=(io_spec, w_spec, io_spec), out_specs=(io_spec, io_spec), check_vma=False
    )
```

```python
import jax
import jax.numpy as jnp
from jax import lax
from jax.experimental import pallas as pl
from jax.experimental.pallas import tpu as pltpu
from jax.sharding import PartitionSpec as P

MESH = pl.DeviceIdType.MESH
F32 = jnp.float32
BF16 = jnp.bfloat16
H, N, D, T, Q, S = 2048, 1024, 512, 256, 128, 64
R = 352
E = 128
F = D - E - R
ME, SIB = 0, 1
OWN, OTH = 0, 1
ARG, BUF = "arg", "buf"
FIRST = ((0, T), (T, T))


def _tdot(a, b):
    return lax.dot_general(a, b, (((0,), (0,)), ((), ())), preferred_element_type=F32)


def _dot_t(a, b):
    return lax.dot_general(a, b, (((1,), (1,)), ((), ())), preferred_element_type=F32)


def loop(n, f, start=0):
    def body(i, carry):
        f(i)
        return carry

    lax.fori_loop(start, n, body, start)


def cut(k0, n, unit=Q):
    return pl.ds(pl.multiple_of(k0, unit), n)


def kernel(
    x_ref, w_ref, dy_ref,
    dx_ref, dw_ref, wbuf, bufy, tail, tail_y,
    dyv, pown, poth, wv, land, extra, swap,
    dy_sem, x_sem, dys_r, dyy_r, xs_r, xf_r, w_r, wp_r, ws_r, pa_r, ph_r, po_r, ps_r, py_r, pf_r,
    s_dys, s_dyy, s_xs, s_w, s_ws, s_px, s_po, s_py, s_sum, wl_sem, tail_sem, tail_y_sem, s_ex, ex_r, py_ex, dyq_sem, xt_sem, xq_sem, s_sw, sw_r,
):
    row = lax.axis_index("row")
    y = lax.axis_index("col")
    x = row // 2
    c = row % 2
    is_a = x == y
    is_b = x != y
    sib = {"row": row + 1 - 2 * c}
    xn = {"row": (row + 2) % 4}
    yn = {"col": 1 - y}

    def remote(src, dst, ssem, rsem, dev):
        return pltpu.make_async_remote_copy(
            src_ref=src, dst_ref=dst, send_sem=ssem, recv_sem=rsem, device_id=dev, device_id_type=MESH
        )

    def local(src, dst, sem):
        return pltpu.make_async_copy(src, dst, sem)

    def qs(q):
        return pl.ds(q * T, T)

    def xo(k0, n):
        return dx_ref.at[:, cut(k0, n)]

    def xs(k0, n):
        return dx_ref.at[:, cut(H + k0, n)]

    def dw_part(q, r0, n):
        return dw_ref.at[pl.ds(r0, n), cut(q * T, T)]

    def dw_tile(q, kt):
        return dw_part(q, kt * D, D)

    dyq_load = local(dy_ref.at[:, pl.ds(0, T)], dyv.at[ME, OWN, :, pl.ds(0, T)], dyq_sem)
    dy_load = local(dy_ref.at[:, pl.ds(T, N - T)], dyv.at[ME, OWN, :, pl.ds(T, N - T)], dy_sem)
    xt_load = local(x_ref.at[:, pl.ds((1 - c) * H, T)], xo(3 * D, T), xt_sem)
    xq_load = local(x_ref.at[:, pl.ds(c * H, T)], xo(0, T), xq_sem)
    x0_load = local(x_ref.at[:, pl.ds(c * H + T, D - T)], xo(T, D - T), x_sem.at[0])
    swap_part = remote(swap.at[0], swap.at[1], s_sw, sw_r, sib)

    def x_load(kt):
        return local(x_ref.at[:, pl.ds(c * H + kt * D, D)], xo(kt * D, D), x_sem.at[kt])

    def x_cols_to_sib(k0, n, sem):
        return remote(x_ref.at[:, pl.ds((1 - c) * H + k0, n)], xs(k0, n), s_xs, sem, sib)

    def x_to_sib(kt):
        return x_cols_to_sib(kt * D, D, xs_r.at[kt])

    def x_first(i):
        k0, n = FIRST[i]
        return x_cols_to_sib(k0, n, xf_r.at[i])

    def dy_to_sib(j, q):
        src = dy_ref.at[:, qs(q)] if j == OWN else dyv.at[ME, OTH, :, qs(q)]
        return remote(src, dyv.at[SIB, j, :, qs(q)], s_dys, dys_r.at[j, q], sib)

    def dy_to_y(q):
        return remote(dy_ref.at[:, qs(q)], dyv.at[ME, OTH, :, qs(q)], s_dyy, dyy_r.at[q], yn)

    def w_own_to_x(i):
        return remote(w_ref.at[qs(i)], wbuf.at[ME, OWN, qs(i)], s_w, w_r.at[OWN, i], xn)

    def w_to_y(i):
        return remote(w_ref.at[qs(i)], wbuf.at[ME, OTH, qs(i)], s_w, w_r.at[OTH, i], yn)

    def w_fwd(i):
        return remote(wbuf.at[ME, OTH, qs(i)], wbuf.at[ME, OTH, qs(i)], s_w, w_r.at[OTH, i], xn)

    def w_piece(p):
        return pl.ds(N + p * S, S)

    def w_to_y_piece(p):
        return remote(w_ref.at[w_piece(p)], wbuf.at[ME, OTH, w_piece(p)], s_w, wp_r.at[p], yn)

    def w_fwd_piece(p):
        return remote(wbuf.at[ME, OTH, w_piece(p)], wbuf.at[ME, OTH, w_piece(p)], s_w, wp_r.at[p], xn)

    def w_to_sib(j, i, src):
        ref = w_ref.at[qs(i)] if src == ARG else wbuf.at[ME, j, qs(i)]
        return remote(ref, wbuf.at[SIB, j, qs(i)], s_ws, ws_r.at[j, i], sib)

    def p_first(i):
        r0, n = FIRST[i]
        return remote(pown.at[0, 0, pl.ds(r0, n)], dw_part(0, r0, n), s_px, pa_r.at[i], xn)

    def p_half(q, kt, h):
        return remote(
            pown.at[q, kt, pl.ds(h * T, T)], dw_part(q, kt * D + h * T, T), s_px, ph_r.at[q, 2 * kt + h], xn
        )

    def p_own(q, kt):
        return remote(pown.at[q, kt], dw_tile(q, kt), s_px, po_r.at[q - 2, kt], xn)

    def p_own_last():
        return remote(
            pown.at[3, 3, pl.ds(0, D - R)], dw_part(3, 3 * D, D - R), s_px, po_r.at[1, 3], xn
        )

    def tail_store():
        return local(pown.at[3, 3, pl.ds(D - R, R)], tail, tail_sem)

    def p_other(q, kt):
        return remote(poth.at[q, kt], land.at[q - 2, kt], s_po, ps_r.at[q - 2, kt], xn)

    def p_trans(q, kt, r):
        part = pl.ds(r * Q, Q)
        return remote(poth.at[q, kt, part], bufy.at[q, kt, part], s_py, pf_r.at[q, 4 * kt + r], yn)

    def p_fwd(q, kt, r):
        part = pl.ds(r * Q, Q)
        return remote(bufy.at[q, kt, part], land.at[q, kt, part], s_px, pf_r.at[q, 4 * kt + r], xn)

    def p_trans_short():
        part = pl.ds(0, F)
        return remote(poth.at[1, 3, part], bufy.at[1, 3, part], s_py, pf_r.at[1, 12], yn)

    def p_fwd_short():
        part = pl.ds(0, F)
        return remote(bufy.at[1, 3, part], land.at[1, 3, part], s_px, pf_r.at[1, 12], xn)

    def p_trans_tail():
        return remote(poth.at[1, 3, pl.ds(F, R)], tail, s_py, pf_r.at[1, 13], yn)

    def p_extra():
        return remote(poth.at[1, 3, pl.ds(D - E, E)], extra, s_ex, ex_r, xn)

    def extra_to_y():
        return remote(poth.at[1, 3, pl.ds(D - E, E)], dw_part(1, 4 * D - E, E), s_py, py_ex, yn)

    def p_term(q, kt):
        return remote(poth.at[q, kt], dw_tile(q, kt), s_py, py_r.at[q, kt], yn)

    def p_term_short():
        part = pl.ds(0, D - E)
        return remote(poth.at[1, 3, part], dw_part(1, 3 * D, D - E), s_py, py_r.at[1, 3], yn)

    def sum_short():
        part = pl.ds(0, D - E)
        return remote(poth.at[3, 3, part], dw_part(3, 3 * D, D - E), s_sum, py_r.at[3, 3], yn)

    def tail_y_store(src):
        return local(src.at[3, 3, pl.ds(D - E, E)], tail_y, tail_y_sem)

    def sum_to_y(q, kt):
        return remote(poth.at[q, kt], dw_tile(q, kt), s_sum, py_r.at[q, kt], yn)

    def drain(ref, sem):
        remote(ref, ref, sem, dyy_r.at[0], yn).wait_send()

    for cp in (dyq_load, xt_load, xq_load):
        cp.start()

    barrier = pltpu.get_barrier_semaphore()
    for dev in (sib, xn, yn):
        pl.semaphore_signal(barrier, inc=1, device_id=dev, device_id_type=MESH)
    pl.semaphore_wait(barrier, 3)

    dy_to_y(0).start()
    dy_to_y(1).start()

    @pl.when(is_a)
    def _():
        for i in range(8):
            w_own_to_x(i).start()
        for q in (2, 3):
            dy_to_y(q).start()

    @pl.when(is_b)
    def _():
        for i in range(4):
            w_to_y(i).start()
        for q in (2, 3):
            dy_to_y(q).start()
        for p in range(16):
            w_to_y_piece(p).start()

    dyq_load.wait()
    xt_load.wait()
    xq_load.wait()
    swap[0] = _tdot(dx_ref[:, 3 * D:3 * D + T], dyv[ME, OWN, :, :T])
    swap_part.start()
    dy_to_sib(OWN, 0).start()
    x_first(1).start()
    pown[0, 0, :T] = _tdot(dx_ref[:, :T], dyv[ME, OWN, :, :T])
    for cp in (x0_load, dy_load, x_load(1), x_load(2), x_load(3)):
        cp.start()
    x_first(0).start()
    for kt in (1, 2, 3):
        x_to_sib(kt).start()
    for q in (1, 2, 3):
        dy_to_sib(OWN, q).start()

    @pl.when(is_a)
    def _():
        for i in range(8):
            w_to_sib(OWN, i, ARG).start()

    swap_part.wait_recv()
    pown[0, 0, :T] = pown[0, 0, :T] + swap[1]

    @pl.when(is_b)
    def _():
        p_first(0).start()

    def p_part(j, c0, k0, n):
        dy = pl.ds(c0, T)
        acc = None
        for t in range(2):
            part = pl.ds(t * N, N)
            for who, base in ((ME, k0), (SIB, H + k0)):
                term = _tdot(dx_ref[part, cut(base, n)], dyv[who, j, part, dy])
                acc = term if acc is None else acc + term
        return acc

    def p_tile(dst, j, q, kt):
        loop(2, lambda h: put(dst.at[q, kt, pl.ds(h * T, T)], p_part(j, q * T, kt * D + h * T, T)))

    def put(ref, value):
        ref[...] = value

    x0_load.wait()
    dy_to_sib(OWN, 0).wait_recv()
    x_first(1).wait_recv()
    pown[0, 0, T:] = p_part(OWN, 0, T, T)

    @pl.when(is_b)
    def _():
        p_first(1).start()

    x_first(0).wait_recv()
    dy_load.wait()

    def own_tile(q, kt):
        if q == 0:
            x_load(kt).wait()
            x_to_sib(kt).wait_recv()
        p_tile(pown, OWN, q, kt)
        if q < 2:
            @pl.when(is_b)
            def _():
                p_half(q, kt, 0).start()
                p_half(q, kt, 1).start()

    for q in range(4):
        if q > 0:
            dy_to_sib(OWN, q).wait_recv()
        loop(4, lambda kt, q=q: own_tile(q, kt), int(q == 0))

    def trans_tile(q, kt):
        if q == 0:
            for r in range(4):
                p_trans(q, kt, r).start()
            return

        @pl.when(kt < 3)
        def _():
            for r in range(4):
                p_trans(q, kt, r).start()

        @pl.when(kt == 3)
        def _():
            p_trans_short().start()
            p_trans_tail().start()
            p_extra().start()

    def dy_in(q):
        dy_to_y(q).wait_recv()
        dy_to_sib(OTH, q).start()

    def other_pass(q):
        dy_in(q)
        dy_to_sib(OTH, q).wait_recv()

        def tile(kt):
            p_tile(poth, OTH, q, kt)
            if q < 2:
                @pl.when(jnp.logical_and(is_a, 4 * q + kt < 7))
                def _():
                    p_term(q, kt).start()

                @pl.when(jnp.logical_and(is_a, 4 * q + kt == 7))
                def _():
                    p_term_short().start()

                @pl.when(is_b)
                def _():
                    trans_tile(q, kt)
            else:
                @pl.when(is_b)
                def _():
                    p_other(q, kt).start()

        loop(4, tile)

    def w_loads(d, cc, src):
        ref = w_ref.at[qs(d)] if src == ARG else wbuf.at[cc, OWN, qs(d)]
        return (
            local(ref, wv.at[cc, OWN], wl_sem.at[cc, OWN]),
            local(wbuf.at[cc, OTH, qs(d)], wv.at[cc, OTH], wl_sem.at[cc, OTH]),
        )

    def start_loads(d, cc, src):
        for cp in w_loads(d, cc, src):
            cp.start()

    def wait_loads(d, cc, src):
        for cp in w_loads(d, cc, src):
            cp.wait()

    def dx_stripe(d, cc, lo=0, hi=4):
        cols = cut((c + cc * (1 - 2 * c)) * H + d * T, T, T)

        def rows(m):
            part = pl.ds(m * D, D)
            dx_ref[part, cols] = (
                _dot_t(dyv[ME, OWN, part, :], wv[cc, OWN]) + _dot_t(dyv[ME, OTH, part, :], wv[cc, OTH])
            ).astype(BF16)

        loop(hi, rows, lo)

    def pair_wait(d, src):
        w_to_sib(OWN, d, src).wait_recv()
        w_to_sib(OTH, d, BUF).wait_recv()

    other_pass(0)
    other_pass(1)

    @pl.when(is_a)
    def _():
        def add(q, kt):
            tile = dw_tile(q, kt)
            tile[...] = tile[...] + pown[q, kt]

        def final_early(t):
            q, kt = t // 4, t % 4

            @pl.when(t == 0)
            def _():
                for i in range(len(FIRST)):
                    p_first(i).wait_recv()

            @pl.when(t > 0)
            def _():
                p_half(q, kt, 0).wait_recv()
                p_half(q, kt, 1).wait_recv()
            add(q, kt)

        def final_late(t):
            q, kt = 2 + t // 4, t % 4
            p_own(q, kt).wait_recv()
            add(q, kt)

        def a_sum(q, kt):
            p_other(q, kt).wait_recv()
            poth[q, kt] = poth[q, kt] + land[q - 2, kt]

            @pl.when(4 * q + kt < 15)
            def _():
                sum_to_y(q, kt).start()

            @pl.when(4 * q + kt == 15)
            def _():
                sum_short().start()
                tail_y_store(poth).start()

        def early(i):
            w_to_y(i).wait_recv()
            w_fwd(i).start()
            w_to_sib(OTH, i, BUF).start()
            final_early(i)

        loop(4, early)
        dy_in(2)
        dy_to_sib(OTH, 2).wait_recv()

        def q2_tile(kt):
            p_tile(poth, OTH, 2, kt)
            final_early(4 + kt)

        loop(4, q2_tile)
        p_extra().wait_recv()
        poth[1, 3, D - E:] = poth[1, 3, D - E:] + extra[...]
        extra_to_y().start()
        start_loads(0, ME, ARG)
        dy_in(3)

        def step(i):
            @pl.when(i < 16)
            def _():
                w_to_y_piece(i).wait_recv()
                w_fwd_piece(i).start()

                @pl.when(i % 4 == 3)
                def _():
                    w_to_sib(OTH, 4 + i // 4, BUF).start()

            @pl.when(i >= 16)
            def _():
                k = i - 16
                q, kt, r = k // 16, (k // 4) % 4, k % 4
                p_trans(q, kt, r).wait_recv()
                p_fwd(q, kt, r).start()

            @pl.when(i == 0)
            def _():
                dy_to_sib(OTH, 3).wait_recv()

            @pl.when(i < 4)
            def _():
                p_tile(poth, OTH, 3, i)

            @pl.when(jnp.logical_and(i >= 4, i < 36))
            def _():
                e = (i - 4) // 2
                d, cc = e // 2, e % 2
                odd = i % 2

                @pl.when(jnp.logical_and(odd == 0, cc == ME))
                def _():
                    pair_wait(d, ARG)
                    start_loads(d, SIB, BUF)
                    wait_loads(d, ME, ARG)

                @pl.when(jnp.logical_and(odd == 0, cc == SIB))
                def _():
                    @pl.when(d < 7)
                    def _():
                        start_loads(d + 1, ME, ARG)
                    wait_loads(d, SIB, BUF)

                dx_stripe(d, cc, 2 * odd, 2 * odd + 2)

            @pl.when(jnp.logical_and(i < 8, i % 2 == 1))
            def _():
                a_sum(2, i // 2)

            @pl.when(jnp.logical_and(jnp.logical_and(i >= 10, i < 26), i % 4 == 2))
            def _():
                a_sum(3, (i - 10) // 4)

            @pl.when(jnp.logical_and(i >= 26, i % 4 == 2))
            def _():
                final_late((i - 26) // 4)

        loop(44, step)
        p_trans_short().wait_recv()
        p_fwd_short().start()
        low = dw_part(3, 4 * D - R, R)
        low[...] = pown[3, 3, D - R:]
        final_late(5)
        final_late(6)
        p_trans_tail().wait_recv()
        p_own_last().wait_recv()
        top = dw_part(3, 3 * D, D - R)
        top[...] = top[...] + pown[3, 3, :D - R]
        drain(wbuf.at[ME], s_w)
        tail_y_store(poth).wait()
        drain(dyv.at[ME, OWN, pl.ds(0, H - (E + R) // 2)], s_px)
        drain(land, s_py)
        drain(dyv.at[ME, OWN, pl.ds(0, H - E // 2)], s_sum)

    @pl.when(is_b)
    def _():
        other_pass(2)
        other_pass(3)
        for t in range(7):
            p_own(2 + t // 4, t % 4).start()
        p_own_last().start()
        tail_store().start()
        tail_y_store(pown).start()

        def own_w(i):
            w_own_to_x(i).wait_recv()
            w_to_sib(OWN, i, BUF).start()

        loop(8, own_w)

        def stripes(d):
            @pl.when(d < 4)
            def _():
                w_to_y(d).wait_recv()

            @pl.when(d >= 4)
            def _():
                for p in range(4):
                    w_to_y_piece(4 * (d - 4) + p).wait_recv()
            w_to_sib(OTH, d, BUF).start()
            start_loads(d, ME, BUF)
            pair_wait(d, BUF)
            start_loads(d, SIB, BUF)
            for cc in (ME, SIB):
                wait_loads(d, cc, BUF)
                dx_stripe(d, cc)

        loop(8, stripes)

        def fin(i):
            q, kt, r = i // 16, (i // 4) % 4, i % 4

            @pl.when(r == 0)
            def _():
                p_term(q, kt).wait_recv()
            p_fwd(q, kt, r).wait_recv()
            tile = dw_part(q, kt * D + r * Q, Q)
            tile[...] = tile[...] + land[q, kt, pl.ds(r * Q, Q)]

        loop(28, fin)
        p_term_short().wait_recv()
        p_fwd_short().wait_recv()
        tile = dw_part(1, 3 * D, F)
        tile[...] = tile[...] + land[1, 3, :F]
        extra_to_y().wait_recv()
        for t in range(7):
            sum_to_y(2 + t // 4, t % 4).wait_recv()
        sum_short().wait_recv()
        tail_y_store(pown).wait()
        tail_store().wait()
        drain(wbuf.at[ME, OWN], s_w)
        drain(dw_ref.at[pl.ds(0, H - R // 4)], s_px)
        drain(land, s_po)
        drain(extra, s_ex)
        drain(dyv.at[ME, OWN, pl.ds(0, H - E // 2)], s_py)

    drain(dyv.at[ME], s_dys)
    drain(dyv.at[ME, OWN], s_dyy)
    drain(wbuf.at[ME], s_xs)
    drain(swap.at[0], s_sw)
    drain(wbuf.at[ME], s_ws)


def store_kernel(dx_ref, dw_ref, dx_out, dw_out, sem):
    copies = []
    for i in range(4):
        part = pl.ds(i * D, D)
        copies.append(pltpu.make_async_copy(dx_ref.at[part], dx_out.at[part], sem.at[0, i]))
        copies.append(pltpu.make_async_copy(dw_ref.at[part], dw_out.at[part], sem.at[1, i]))
    for cp in copies:
        cp.start()
    for cp in copies:
        cp.wait()


def add_kernel(done_ref, dw_ref, tail_ref, tail_y_ref, dw_out, buf, buf_y, sem, sem_y):
    is_a = lax.axis_index("row") // 2 == lax.axis_index("col")
    rows = cut(jnp.where(is_a, H - R, 3 * D + F), R, 32)
    cols = cut(jnp.where(is_a, 3 * T, T), T)
    buf[...] = dw_ref[rows, cols] + tail_ref[...]
    first = pltpu.make_async_copy(buf, dw_out.at[rows, cols], sem)
    first.start()
    rows_y, cols_y = pl.ds(H - E, E), cut(jnp.where(is_a, 0, 3 * T), T)
    buf_y[...] = jnp.where(is_a, dw_ref[rows_y, cols_y], tail_y_ref[...])
    second = pltpu.make_async_copy(buf_y, dw_out.at[rows_y, cols_y], sem_y)
    second.start()
    first.wait()
    second.wait()


def local_backward(act_blk, w_blk, grad_blk):
    any_spec = pl.BlockSpec(memory_space=pl.ANY)
    vmem_spec = pl.BlockSpec(memory_space=pltpu.VMEM)
    dma = pltpu.SemaphoreType.DMA
    outs = pl.pallas_call(
        kernel,
        out_shape=(
            pltpu.VMEM((H, 2 * H), BF16),
            pltpu.VMEM((H, N), F32),
            jax.ShapeDtypeStruct((2, 2, H, N), BF16),
            jax.ShapeDtypeStruct((2, 4, D, T), F32),
            jax.ShapeDtypeStruct((R, T), F32),
            jax.ShapeDtypeStruct((E, T), F32),
        ),
        in_specs=[any_spec] * 3,
        out_specs=(vmem_spec,) * 2 + (any_spec,) * 4,
        scratch_shapes=[
            pltpu.VMEM((2, 2, H, N), BF16),
            pltpu.VMEM((4, 4, D, T), F32),
            pltpu.VMEM((4, 4, D, T), F32),
            pltpu.VMEM((2, 2, T, N), BF16),
            pltpu.VMEM((2, 4, D, T), F32),
            pltpu.VMEM((E, T), F32),
            pltpu.VMEM((2, T, T), F32),
            dma, dma((4,)), dma((2, 4)), dma((4,)), dma((4,)), dma((5,)), dma((2, 8)), dma((16,)), dma((2, 8)),
            dma((4,)), dma((2, 8)), dma((2, 4)), dma((2, 4)), dma((4, 4)), dma((2, 16)),
            dma, dma, dma, dma, dma, dma, dma, dma, dma, dma((2, 2)), dma,
            dma, dma, dma, dma, dma, dma, dma, dma, dma,
        ],
        compiler_params=pltpu.CompilerParams(
            collective_id=0, has_side_effects=True, vmem_limit_bytes=41_800_000
        ),
        cost_estimate=pl.CostEstimate(flops=8 * H * H * H, bytes_accessed=100 << 20, transcendentals=0),
    )(act_blk, w_blk, grad_blk)
    tail = lax.ppermute(outs[4], "row", [(i, (i + 2) % 4) for i in range(4)])
    tail_y = lax.ppermute(outs[5], "col", [(0, 1), (1, 0)])
    dx, dw = pl.pallas_call(
        store_kernel,
        out_shape=(jax.ShapeDtypeStruct((H, 2 * H), BF16), jax.ShapeDtypeStruct((H, N), F32)),
        in_specs=[vmem_spec] * 2,
        out_specs=(any_spec,) * 2,
        scratch_shapes=[dma((2, 4))],
        compiler_params=pltpu.CompilerParams(vmem_limit_bytes=1 << 20),
        cost_estimate=pl.CostEstimate(flops=0, bytes_accessed=48 << 20, transcendentals=0),
    )(outs[0], outs[1])
    dw = pl.pallas_call(
        add_kernel,
        out_shape=jax.ShapeDtypeStruct((H, N), F32),
        in_specs=[any_spec] + [vmem_spec] * 3,
        out_specs=any_spec,
        scratch_shapes=[pltpu.VMEM((R, T), F32), pltpu.VMEM((E, T), F32), dma, dma],
        input_output_aliases={0: 0},
        compiler_params=pltpu.CompilerParams(vmem_limit_bytes=2 << 20),
        cost_estimate=pl.CostEstimate(flops=0, bytes_accessed=1 << 20, transcendentals=0),
    )(dw, outs[1], tail, tail_y)
    return dx, dw


def solution(mesh):
    io_spec = P(("dp", "row"), "col")
    w_spec = P("row", "col")
    return jax.shard_map(
        local_backward, mesh=mesh, in_specs=(io_spec, w_spec, io_spec), out_specs=(io_spec, io_spec), check_vma=False
    )
```

```python
import jax
import jax.numpy as jnp
from jax import lax
from jax.experimental import pallas as pl
from jax.experimental.pallas import tpu as pltpu
from jax.sharding import PartitionSpec as P

MESH = pl.DeviceIdType.MESH
F32 = jnp.float32
BF16 = jnp.bfloat16
H, N, D, T, Q, S = 2048, 1024, 512, 256, 128, 64
R = 384
E = 96
F = D - E - R
ME, SIB = 0, 1
OWN, OTH = 0, 1
ARG, BUF = "arg", "buf"
FIRST = ((0, T), (T, T))


def _tdot(a, b):
    return lax.dot_general(a, b, (((0,), (0,)), ((), ())), preferred_element_type=F32)


def _dot_t(a, b):
    return lax.dot_general(a, b, (((1,), (1,)), ((), ())), preferred_element_type=F32)


def loop(n, f, start=0):
    def body(i, carry):
        f(i)
        return carry

    lax.fori_loop(start, n, body, start)


def cut(k0, n, unit=Q):
    return pl.ds(pl.multiple_of(k0, unit), n)


def kernel(
    x_ref, w_ref, dy_ref,
    dx_ref, dw_ref, wbuf, bufy, tail, tail_y,
    dyv, pown, poth, wv, land, extra, swap,
    dy_sem, x_sem, dys_r, dyy_r, xs_r, xf_r, w_r, wp_r, ws_r, pa_r, ph_r, po_r, ps_r, py_r, pf_r,
    s_dys, s_dyy, s_xs, s_w, s_ws, s_px, s_po, s_py, s_sum, wl_sem, tail_sem, tail_y_sem, s_ex, ex_r, py_ex, dyq_sem, xt_sem, xq_sem, s_sw, sw_r,
):
    row = lax.axis_index("row")
    y = lax.axis_index("col")
    x = row // 2
    c = row % 2
    is_a = x == y
    is_b = x != y
    sib = {"row": row + 1 - 2 * c}
    xn = {"row": (row + 2) % 4}
    yn = {"col": 1 - y}

    def remote(src, dst, ssem, rsem, dev):
        return pltpu.make_async_remote_copy(
            src_ref=src, dst_ref=dst, send_sem=ssem, recv_sem=rsem, device_id=dev, device_id_type=MESH
        )

    def local(src, dst, sem):
        return pltpu.make_async_copy(src, dst, sem)

    def qs(q):
        return pl.ds(q * T, T)

    def xo(k0, n):
        return dx_ref.at[:, cut(k0, n)]

    def xs(k0, n):
        return dx_ref.at[:, cut(H + k0, n)]

    def dw_part(q, r0, n):
        return dw_ref.at[pl.ds(r0, n), cut(q * T, T)]

    def dw_tile(q, kt):
        return dw_part(q, kt * D, D)

    dyq_load = local(dy_ref.at[:, pl.ds(0, T)], dyv.at[ME, OWN, :, pl.ds(0, T)], dyq_sem)
    dy_load = local(dy_ref.at[:, pl.ds(T, N - T)], dyv.at[ME, OWN, :, pl.ds(T, N - T)], dy_sem)
    xt_load = local(x_ref.at[:, pl.ds((1 - c) * H, T)], xo(3 * D, T), xt_sem)
    xq_load = local(x_ref.at[:, pl.ds(c * H, T)], xo(0, T), xq_sem)
    x0_load = local(x_ref.at[:, pl.ds(c * H + T, D - T)], xo(T, D - T), x_sem.at[0])
    swap_part = remote(swap.at[0], swap.at[1], s_sw, sw_r, sib)

    def x_load(kt):
        return local(x_ref.at[:, pl.ds(c * H + kt * D, D)], xo(kt * D, D), x_sem.at[kt])

    def x_cols_to_sib(k0, n, sem):
        return remote(x_ref.at[:, pl.ds((1 - c) * H + k0, n)], xs(k0, n), s_xs, sem, sib)

    def x_to_sib(kt):
        return x_cols_to_sib(kt * D, D, xs_r.at[kt])

    def x_first(i):
        k0, n = FIRST[i]
        return x_cols_to_sib(k0, n, xf_r.at[i])

    def dy_to_sib(j, q):
        src = dy_ref.at[:, qs(q)] if j == OWN else dyv.at[ME, OTH, :, qs(q)]
        return remote(src, dyv.at[SIB, j, :, qs(q)], s_dys, dys_r.at[j, q], sib)

    def dy_to_y(q):
        return remote(dy_ref.at[:, qs(q)], dyv.at[ME, OTH, :, qs(q)], s_dyy, dyy_r.at[q], yn)

    def w_own_to_x(i):
        return remote(w_ref.at[qs(i)], wbuf.at[ME, OWN, qs(i)], s_w, w_r.at[OWN, i], xn)

    def w_to_y(i):
        return remote(w_ref.at[qs(i)], wbuf.at[ME, OTH, qs(i)], s_w, w_r.at[OTH, i], yn)

    def w_fwd(i):
        return remote(wbuf.at[ME, OTH, qs(i)], wbuf.at[ME, OTH, qs(i)], s_w, w_r.at[OTH, i], xn)

    def w_piece(p):
        return pl.ds(N + p * S, S)

    def w_to_y_piece(p):
        return remote(w_ref.at[w_piece(p)], wbuf.at[ME, OTH, w_piece(p)], s_w, wp_r.at[p], yn)

    def w_fwd_piece(p):
        return remote(wbuf.at[ME, OTH, w_piece(p)], wbuf.at[ME, OTH, w_piece(p)], s_w, wp_r.at[p], xn)

    def w_to_sib(j, i, src):
        ref = w_ref.at[qs(i)] if src == ARG else wbuf.at[ME, j, qs(i)]
        return remote(ref, wbuf.at[SIB, j, qs(i)], s_ws, ws_r.at[j, i], sib)

    def p_first(i):
        r0, n = FIRST[i]
        return remote(pown.at[0, 0, pl.ds(r0, n)], dw_part(0, r0, n), s_px, pa_r.at[i], xn)

    def p_half(q, kt, h):
        return remote(
            pown.at[q, kt, pl.ds(h * T, T)], dw_part(q, kt * D + h * T, T), s_px, ph_r.at[q, 2 * kt + h], xn
        )

    def p_own(q, kt):
        return remote(pown.at[q, kt], dw_tile(q, kt), s_px, po_r.at[q - 2, kt], xn)

    def p_own_last():
        return remote(
            pown.at[3, 3, pl.ds(0, D - R)], dw_part(3, 3 * D, D - R), s_px, po_r.at[1, 3], xn
        )

    def tail_store():
        return local(pown.at[3, 3, pl.ds(D - R, R)], tail, tail_sem)

    def p_other(q, kt):
        return remote(poth.at[q, kt], land.at[q - 2, kt], s_po, ps_r.at[q - 2, kt], xn)

    def p_trans(q, kt, r):
        part = pl.ds(r * Q, Q)
        return remote(poth.at[q, kt, part], bufy.at[q, kt, part], s_py, pf_r.at[q, 4 * kt + r], yn)

    def p_fwd(q, kt, r):
        part = pl.ds(r * Q, Q)
        return remote(bufy.at[q, kt, part], land.at[q, kt, part], s_px, pf_r.at[q, 4 * kt + r], xn)

    def p_trans_short():
        part = pl.ds(0, F)
        return remote(poth.at[1, 3, part], bufy.at[1, 3, part], s_py, pf_r.at[1, 12], yn)

    def p_fwd_short():
        part = pl.ds(0, F)
        return remote(bufy.at[1, 3, part], land.at[1, 3, part], s_px, pf_r.at[1, 12], xn)

    def p_trans_tail():
        return remote(poth.at[1, 3, pl.ds(F, R)], tail, s_py, pf_r.at[1, 13], yn)

    def p_extra():
        return remote(poth.at[1, 3, pl.ds(D - E, E)], extra, s_ex, ex_r, xn)

    def extra_to_y():
        return remote(poth.at[1, 3, pl.ds(D - E, E)], dw_part(1, 4 * D - E, E), s_py, py_ex, yn)

    def p_term(q, kt):
        return remote(poth.at[q, kt], dw_tile(q, kt), s_py, py_r.at[q, kt], yn)

    def p_term_short():
        part = pl.ds(0, D - E)
        return remote(poth.at[1, 3, part], dw_part(1, 3 * D, D - E), s_py, py_r.at[1, 3], yn)

    def sum_short():
        part = pl.ds(0, D - E)
        return remote(poth.at[3, 3, part], dw_part(3, 3 * D, D - E), s_sum, py_r.at[3, 3], yn)

    def tail_y_store(src):
        return local(src.at[3, 3, pl.ds(D - E, E)], tail_y, tail_y_sem)

    def sum_to_y(q, kt):
        return remote(poth.at[q, kt], dw_tile(q, kt), s_sum, py_r.at[q, kt], yn)

    def drain(ref, sem):
        remote(ref, ref, sem, dyy_r.at[0], yn).wait_send()

    for cp in (dyq_load, xt_load, xq_load):
        cp.start()

    barrier = pltpu.get_barrier_semaphore()
    for dev in (sib, xn, yn):
        pl.semaphore_signal(barrier, inc=1, device_id=dev, device_id_type=MESH)
    pl.semaphore_wait(barrier, 3)

    dy_to_y(0).start()
    dy_to_y(1).start()

    @pl.when(is_a)
    def _():
        for i in range(8):
            w_own_to_x(i).start()
        for q in (2, 3):
            dy_to_y(q).start()

    @pl.when(is_b)
    def _():
        for i in range(4):
            w_to_y(i).start()
        for q in (2, 3):
            dy_to_y(q).start()
        for p in range(16):
            w_to_y_piece(p).start()

    dyq_load.wait()
    xt_load.wait()
    xq_load.wait()
    swap[0] = _tdot(dx_ref[:, 3 * D:3 * D + T], dyv[ME, OWN, :, :T])
    swap_part.start()
    dy_to_sib(OWN, 0).start()
    x_first(1).start()
    pown[0, 0, :T] = _tdot(dx_ref[:, :T], dyv[ME, OWN, :, :T])
    for cp in (x0_load, dy_load, x_load(1), x_load(2), x_load(3)):
        cp.start()
    x_first(0).start()
    for kt in (1, 2, 3):
        x_to_sib(kt).start()
    for q in (1, 2, 3):
        dy_to_sib(OWN, q).start()

    @pl.when(is_a)
    def _():
        for i in range(8):
            w_to_sib(OWN, i, ARG).start()

    swap_part.wait_recv()
    pown[0, 0, :T] = pown[0, 0, :T] + swap[1]

    @pl.when(is_b)
    def _():
        p_first(0).start()

    def p_part(j, c0, k0, n):
        dy = pl.ds(c0, T)
        acc = None
        for t in range(2):
            part = pl.ds(t * N, N)
            for who, base in ((ME, k0), (SIB, H + k0)):
                term = _tdot(dx_ref[part, cut(base, n)], dyv[who, j, part, dy])
                acc = term if acc is None else acc + term
        return acc

    def p_tile(dst, j, q, kt):
        loop(2, lambda h: put(dst.at[q, kt, pl.ds(h * T, T)], p_part(j, q * T, kt * D + h * T, T)))

    def put(ref, value):
        ref[...] = value

    x0_load.wait()
    dy_to_sib(OWN, 0).wait_recv()
    x_first(1).wait_recv()
    pown[0, 0, T:] = p_part(OWN, 0, T, T)

    @pl.when(is_b)
    def _():
        p_first(1).start()

    x_first(0).wait_recv()
    dy_load.wait()

    def own_tile(q, kt):
        if q == 0:
            x_load(kt).wait()
            x_to_sib(kt).wait_recv()
        p_tile(pown, OWN, q, kt)
        if q < 2:
            @pl.when(is_b)
            def _():
                p_half(q, kt, 0).start()
                p_half(q, kt, 1).start()

    for q in range(4):
        if q > 0:
            dy_to_sib(OWN, q).wait_recv()
        loop(4, lambda kt, q=q: own_tile(q, kt), int(q == 0))

    def trans_tile(q, kt):
        if q == 0:
            for r in range(4):
                p_trans(q, kt, r).start()
            return

        @pl.when(kt < 3)
        def _():
            for r in range(4):
                p_trans(q, kt, r).start()

        @pl.when(kt == 3)
        def _():
            p_trans_short().start()
            p_trans_tail().start()
            p_extra().start()

    def dy_in(q):
        dy_to_y(q).wait_recv()
        dy_to_sib(OTH, q).start()

    def other_pass(q):
        dy_in(q)
        dy_to_sib(OTH, q).wait_recv()

        def tile(kt):
            p_tile(poth, OTH, q, kt)
            if q < 2:
                @pl.when(jnp.logical_and(is_a, 4 * q + kt < 7))
                def _():
                    p_term(q, kt).start()

                @pl.when(jnp.logical_and(is_a, 4 * q + kt == 7))
                def _():
                    p_term_short().start()

                @pl.when(is_b)
                def _():
                    trans_tile(q, kt)
            else:
                @pl.when(is_b)
                def _():
                    p_other(q, kt).start()

        loop(4, tile)

    def w_loads(d, cc, src):
        ref = w_ref.at[qs(d)] if src == ARG else wbuf.at[cc, OWN, qs(d)]
        return (
            local(ref, wv.at[cc, OWN], wl_sem.at[cc, OWN]),
            local(wbuf.at[cc, OTH, qs(d)], wv.at[cc, OTH], wl_sem.at[cc, OTH]),
        )

    def start_loads(d, cc, src):
        for cp in w_loads(d, cc, src):
            cp.start()

    def wait_loads(d, cc, src):
        for cp in w_loads(d, cc, src):
            cp.wait()

    def dx_stripe(d, cc, lo=0, hi=4):
        cols = cut((c + cc * (1 - 2 * c)) * H + d * T, T, T)

        def rows(m):
            part = pl.ds(m * D, D)
            dx_ref[part, cols] = (
                _dot_t(dyv[ME, OWN, part, :], wv[cc, OWN]) + _dot_t(dyv[ME, OTH, part, :], wv[cc, OTH])
            ).astype(BF16)

        loop(hi, rows, lo)

    def pair_wait(d, src):
        w_to_sib(OWN, d, src).wait_recv()
        w_to_sib(OTH, d, BUF).wait_recv()

    other_pass(0)
    other_pass(1)

    @pl.when(is_a)
    def _():
        def add(q, kt):
            tile = dw_tile(q, kt)
            tile[...] = tile[...] + pown[q, kt]

        def final_early(t):
            q, kt = t // 4, t % 4

            @pl.when(t == 0)
            def _():
                for i in range(len(FIRST)):
                    p_first(i).wait_recv()

            @pl.when(t > 0)
            def _():
                p_half(q, kt, 0).wait_recv()
                p_half(q, kt, 1).wait_recv()
            add(q, kt)

        def final_late(t):
            q, kt = 2 + t // 4, t % 4
            p_own(q, kt).wait_recv()
            add(q, kt)

        def a_sum(q, kt):
            p_other(q, kt).wait_recv()
            poth[q, kt] = poth[q, kt] + land[q - 2, kt]

            @pl.when(4 * q + kt < 15)
            def _():
                sum_to_y(q, kt).start()

            @pl.when(4 * q + kt == 15)
            def _():
                sum_short().start()
                tail_y_store(poth).start()

        def early(i):
            w_to_y(i).wait_recv()
            w_fwd(i).start()
            w_to_sib(OTH, i, BUF).start()
            final_early(i)

        loop(4, early)
        dy_in(2)
        dy_to_sib(OTH, 2).wait_recv()

        def q2_tile(kt):
            p_tile(poth, OTH, 2, kt)
            final_early(4 + kt)

        loop(4, q2_tile)
        p_extra().wait_recv()
        poth[1, 3, D - E:] = poth[1, 3, D - E:] + extra[...]
        extra_to_y().start()
        start_loads(0, ME, ARG)
        dy_in(3)

        def step(i):
            @pl.when(i < 16)
            def _():
                w_to_y_piece(i).wait_recv()
                w_fwd_piece(i).start()

                @pl.when(i % 4 == 3)
                def _():
                    w_to_sib(OTH, 4 + i // 4, BUF).start()

            @pl.when(i >= 16)
            def _():
                k = i - 16
                q, kt, r = k // 16, (k // 4) % 4, k % 4
                p_trans(q, kt, r).wait_recv()
                p_fwd(q, kt, r).start()

            @pl.when(i == 0)
            def _():
                dy_to_sib(OTH, 3).wait_recv()

            @pl.when(i < 4)
            def _():
                p_tile(poth, OTH, 3, i)

            @pl.when(jnp.logical_and(i >= 4, i < 36))
            def _():
                e = (i - 4) // 2
                d, cc = e // 2, e % 2
                odd = i % 2

                @pl.when(jnp.logical_and(odd == 0, cc == ME))
                def _():
                    pair_wait(d, ARG)
                    start_loads(d, SIB, BUF)
                    wait_loads(d, ME, ARG)

                @pl.when(jnp.logical_and(odd == 0, cc == SIB))
                def _():
                    @pl.when(d < 7)
                    def _():
                        start_loads(d + 1, ME, ARG)
                    wait_loads(d, SIB, BUF)

                dx_stripe(d, cc, 2 * odd, 2 * odd + 2)

            @pl.when(jnp.logical_and(i < 8, i % 2 == 1))
            def _():
                a_sum(2, i // 2)

            @pl.when(jnp.logical_and(jnp.logical_and(i >= 10, i < 26), i % 4 == 2))
            def _():
                a_sum(3, (i - 10) // 4)

            @pl.when(jnp.logical_and(i >= 26, i % 4 == 2))
            def _():
                final_late((i - 26) // 4)

        loop(44, step)
        p_trans_short().wait_recv()
        p_fwd_short().start()
        low = dw_part(3, 4 * D - R, R)
        low[...] = pown[3, 3, D - R:]
        final_late(5)
        final_late(6)
        p_trans_tail().wait_recv()
        p_own_last().wait_recv()
        top = dw_part(3, 3 * D, D - R)
        top[...] = top[...] + pown[3, 3, :D - R]
        drain(wbuf.at[ME], s_w)
        tail_y_store(poth).wait()
        drain(dyv.at[ME, OWN, pl.ds(0, H - (E + R) // 2)], s_px)
        drain(land, s_py)
        drain(dyv.at[ME, OWN, pl.ds(0, H - E // 2)], s_sum)

    @pl.when(is_b)
    def _():
        other_pass(2)
        other_pass(3)
        for t in range(7):
            p_own(2 + t // 4, t % 4).start()
        p_own_last().start()
        tail_store().start()
        tail_y_store(pown).start()

        def own_w(i):
            w_own_to_x(i).wait_recv()
            w_to_sib(OWN, i, BUF).start()

        loop(8, own_w)

        def stripes(d):
            @pl.when(d < 4)
            def _():
                w_to_y(d).wait_recv()

            @pl.when(d >= 4)
            def _():
                for p in range(4):
                    w_to_y_piece(4 * (d - 4) + p).wait_recv()
            w_to_sib(OTH, d, BUF).start()
            start_loads(d, ME, BUF)
            pair_wait(d, BUF)
            start_loads(d, SIB, BUF)
            for cc in (ME, SIB):
                wait_loads(d, cc, BUF)
                dx_stripe(d, cc)

        loop(8, stripes)

        def fin(i):
            q, kt, r = i // 16, (i // 4) % 4, i % 4

            @pl.when(r == 0)
            def _():
                p_term(q, kt).wait_recv()
            p_fwd(q, kt, r).wait_recv()
            tile = dw_part(q, kt * D + r * Q, Q)
            tile[...] = tile[...] + land[q, kt, pl.ds(r * Q, Q)]

        loop(28, fin)
        p_term_short().wait_recv()
        p_fwd_short().wait_recv()
        tile = dw_part(1, 3 * D, F)
        tile[...] = tile[...] + land[1, 3, :F]
        extra_to_y().wait_recv()
        for t in range(7):
            sum_to_y(2 + t // 4, t % 4).wait_recv()
        sum_short().wait_recv()
        tail_y_store(pown).wait()
        tail_store().wait()
        drain(wbuf.at[ME, OWN], s_w)
        drain(dw_ref.at[pl.ds(0, H - R // 4)], s_px)
        drain(land, s_po)
        drain(extra, s_ex)
        drain(dyv.at[ME, OWN, pl.ds(0, H - E // 2)], s_py)

    drain(dyv.at[ME], s_dys)
    drain(dyv.at[ME, OWN], s_dyy)
    drain(wbuf.at[ME], s_xs)
    drain(swap.at[0], s_sw)
    drain(wbuf.at[ME], s_ws)


def store_kernel(dx_ref, dw_ref, dx_out, dw_out, sem):
    copies = []
    for i in range(4):
        part = pl.ds(i * D, D)
        copies.append(pltpu.make_async_copy(dx_ref.at[part], dx_out.at[part], sem.at[0, i]))
        copies.append(pltpu.make_async_copy(dw_ref.at[part], dw_out.at[part], sem.at[1, i]))
    for cp in copies:
        cp.start()
    for cp in copies:
        cp.wait()


def add_kernel(done_ref, dw_ref, tail_ref, tail_y_ref, dw_out, buf, buf_y, sem, sem_y):
    is_a = lax.axis_index("row") // 2 == lax.axis_index("col")
    rows = cut(jnp.where(is_a, H - R, 3 * D + F), R, 32)
    cols = cut(jnp.where(is_a, 3 * T, T), T)
    buf[...] = dw_ref[rows, cols] + tail_ref[...]
    first = pltpu.make_async_copy(buf, dw_out.at[rows, cols], sem)
    first.start()
    rows_y, cols_y = pl.ds(H - E, E), cut(jnp.where(is_a, 0, 3 * T), T)
    buf_y[...] = jnp.where(is_a, dw_ref[rows_y, cols_y], tail_y_ref[...])
    second = pltpu.make_async_copy(buf_y, dw_out.at[rows_y, cols_y], sem_y)
    second.start()
    first.wait()
    second.wait()


def local_backward(act_blk, w_blk, grad_blk):
    any_spec = pl.BlockSpec(memory_space=pl.ANY)
    vmem_spec = pl.BlockSpec(memory_space=pltpu.VMEM)
    dma = pltpu.SemaphoreType.DMA
    outs = pl.pallas_call(
        kernel,
        out_shape=(
            pltpu.VMEM((H, 2 * H), BF16),
            pltpu.VMEM((H, N), F32),
            jax.ShapeDtypeStruct((2, 2, H, N), BF16),
            jax.ShapeDtypeStruct((2, 4, D, T), F32),
            jax.ShapeDtypeStruct((R, T), F32),
            jax.ShapeDtypeStruct((E, T), F32),
        ),
        in_specs=[any_spec] * 3,
        out_specs=(vmem_spec,) * 2 + (any_spec,) * 4,
        scratch_shapes=[
            pltpu.VMEM((2, 2, H, N), BF16),
            pltpu.VMEM((4, 4, D, T), F32),
            pltpu.VMEM((4, 4, D, T), F32),
            pltpu.VMEM((2, 2, T, N), BF16),
            pltpu.VMEM((2, 4, D, T), F32),
            pltpu.VMEM((E, T), F32),
            pltpu.VMEM((2, T, T), F32),
            dma, dma((4,)), dma((2, 4)), dma((4,)), dma((4,)), dma((5,)), dma((2, 8)), dma((16,)), dma((2, 8)),
            dma((4,)), dma((2, 8)), dma((2, 4)), dma((2, 4)), dma((4, 4)), dma((2, 16)),
            dma, dma, dma, dma, dma, dma, dma, dma, dma, dma((2, 2)), dma,
            dma, dma, dma, dma, dma, dma, dma, dma, dma,
        ],
        compiler_params=pltpu.CompilerParams(
            collective_id=0, has_side_effects=True, vmem_limit_bytes=41_800_000
        ),
        cost_estimate=pl.CostEstimate(flops=8 * H * H * H, bytes_accessed=100 << 20, transcendentals=0),
    )(act_blk, w_blk, grad_blk)
    tail = lax.ppermute(outs[4], "row", [(i, (i + 2) % 4) for i in range(4)])
    tail_y = lax.ppermute(outs[5], "col", [(0, 1), (1, 0)])
    dx, dw = pl.pallas_call(
        store_kernel,
        out_shape=(jax.ShapeDtypeStruct((H, 2 * H), BF16), jax.ShapeDtypeStruct((H, N), F32)),
        in_specs=[vmem_spec] * 2,
        out_specs=(any_spec,) * 2,
        scratch_shapes=[dma((2, 4))],
        compiler_params=pltpu.CompilerParams(vmem_limit_bytes=1 << 20),
        cost_estimate=pl.CostEstimate(flops=0, bytes_accessed=48 << 20, transcendentals=0),
    )(outs[0], outs[1])
    dw = pl.pallas_call(
        add_kernel,
        out_shape=jax.ShapeDtypeStruct((H, N), F32),
        in_specs=[any_spec] + [vmem_spec] * 3,
        out_specs=any_spec,
        scratch_shapes=[pltpu.VMEM((R, T), F32), pltpu.VMEM((E, T), F32), dma, dma],
        input_output_aliases={0: 0},
        compiler_params=pltpu.CompilerParams(vmem_limit_bytes=2 << 20),
        cost_estimate=pl.CostEstimate(flops=0, bytes_accessed=1 << 20, transcendentals=0),
    )(dw, outs[1], tail, tail_y)
    return dx, dw


def solution(mesh):
    io_spec = P(("dp", "row"), "col")
    w_spec = P("row", "col")
    return jax.shard_map(
        local_backward, mesh=mesh, in_specs=(io_spec, w_spec, io_spec), out_specs=(io_spec, io_spec), check_vma=False
    )
```

```python
import jax
import jax.numpy as jnp
from jax import lax
from jax.experimental import pallas as pl
from jax.experimental.pallas import tpu as pltpu
from jax.sharding import PartitionSpec as P

MESH = pl.DeviceIdType.MESH
F32 = jnp.float32
BF16 = jnp.bfloat16
H, N, D, T, Q, S = 2048, 1024, 512, 256, 128, 64
R = 384
E = 112
EY = 72
F = D - E - R
ME, SIB = 0, 1
OWN, OTH = 0, 1
ARG, BUF = "arg", "buf"
FIRST = ((0, T), (T, T))


def _tdot(a, b):
    return lax.dot_general(a, b, (((0,), (0,)), ((), ())), preferred_element_type=F32)


def _dot_t(a, b):
    return lax.dot_general(a, b, (((1,), (1,)), ((), ())), preferred_element_type=F32)


def loop(n, f, start=0):
    def body(i, carry):
        f(i)
        return carry

    lax.fori_loop(start, n, body, start)


def cut(k0, n, unit=Q):
    return pl.ds(pl.multiple_of(k0, unit), n)


def kernel(
    x_ref, w_ref, dy_ref,
    dx_ref, dw_ref, wbuf, bufy, tail, tail_y,
    dyv, pown, poth, wv, land, extra, swap,
    dy_sem, x_sem, dys_r, dyy_r, xs_r, xf_r, w_r, wp_r, ws_r, pa_r, ph_r, po_r, ps_r, py_r, pf_r,
    s_dys, s_dyy, s_xs, s_w, s_ws, s_px, s_po, s_py, s_sum, wl_sem, tail_sem, tail_y_sem, s_ex, ex_r, py_ex, dyq_sem, xt_sem, xq_sem, s_sw, sw_r, s_last,
):
    row = lax.axis_index("row")
    y = lax.axis_index("col")
    x = row // 2
    c = row % 2
    is_a = x == y
    is_b = x != y
    sib = {"row": row + 1 - 2 * c}
    xn = {"row": (row + 2) % 4}
    yn = {"col": 1 - y}

    def remote(src, dst, ssem, rsem, dev):
        return pltpu.make_async_remote_copy(
            src_ref=src, dst_ref=dst, send_sem=ssem, recv_sem=rsem, device_id=dev, device_id_type=MESH
        )

    def local(src, dst, sem):
        return pltpu.make_async_copy(src, dst, sem)

    def qs(q):
        return pl.ds(q * T, T)

    def xo(k0, n):
        return dx_ref.at[:, cut(k0, n)]

    def xs(k0, n):
        return dx_ref.at[:, cut(H + k0, n)]

    def dw_part(q, r0, n):
        return dw_ref.at[pl.ds(r0, n), cut(q * T, T)]

    def dw_tile(q, kt):
        return dw_part(q, kt * D, D)

    dyq_load = local(dy_ref.at[:, pl.ds(0, T)], dyv.at[ME, OWN, :, pl.ds(0, T)], dyq_sem)
    dy_load = local(dy_ref.at[:, pl.ds(T, N - T)], dyv.at[ME, OWN, :, pl.ds(T, N - T)], dy_sem)
    xt_load = local(x_ref.at[:, pl.ds((1 - c) * H, T)], xo(3 * D, T), xt_sem)
    xq_load = local(x_ref.at[:, pl.ds(c * H, T)], xo(0, T), xq_sem)
    x0_load = local(x_ref.at[:, pl.ds(c * H + T, D - T)], xo(T, D - T), x_sem.at[0])
    swap_part = remote(swap.at[0], swap.at[1], s_sw, sw_r, sib)

    def x_load(kt):
        return local(x_ref.at[:, pl.ds(c * H + kt * D, D)], xo(kt * D, D), x_sem.at[kt])

    def x_cols_to_sib(k0, n, sem):
        return remote(x_ref.at[:, pl.ds((1 - c) * H + k0, n)], xs(k0, n), s_xs, sem, sib)

    def x_to_sib(kt):
        return x_cols_to_sib(kt * D, D, xs_r.at[kt])

    def x_first(i):
        k0, n = FIRST[i]
        return x_cols_to_sib(k0, n, xf_r.at[i])

    def dy_to_sib(j, q):
        src = dy_ref.at[:, qs(q)] if j == OWN else dyv.at[ME, OTH, :, qs(q)]
        return remote(src, dyv.at[SIB, j, :, qs(q)], s_dys, dys_r.at[j, q], sib)

    def dy_to_y(q):
        return remote(dy_ref.at[:, qs(q)], dyv.at[ME, OTH, :, qs(q)], s_dyy, dyy_r.at[q], yn)

    def w_own_to_x(i):
        return remote(w_ref.at[qs(i)], wbuf.at[ME, OWN, qs(i)], s_w, w_r.at[OWN, i], xn)

    def w_to_y(i):
        return remote(w_ref.at[qs(i)], wbuf.at[ME, OTH, qs(i)], s_w, w_r.at[OTH, i], yn)

    def w_fwd(i):
        return remote(wbuf.at[ME, OTH, qs(i)], wbuf.at[ME, OTH, qs(i)], s_w, w_r.at[OTH, i], xn)

    def w_piece(p):
        return pl.ds(N + p * S, S)

    def w_to_y_piece(p):
        return remote(w_ref.at[w_piece(p)], wbuf.at[ME, OTH, w_piece(p)], s_w, wp_r.at[p], yn)

    def w_fwd_piece(p):
        return remote(wbuf.at[ME, OTH, w_piece(p)], wbuf.at[ME, OTH, w_piece(p)], s_w, wp_r.at[p], xn)

    def w_to_sib(j, i, src):
        ref = w_ref.at[qs(i)] if src == ARG else wbuf.at[ME, j, qs(i)]
        return remote(ref, wbuf.at[SIB, j, qs(i)], s_ws, ws_r.at[j, i], sib)

    def p_first(i):
        r0, n = FIRST[i]
        return remote(pown.at[0, 0, pl.ds(r0, n)], dw_part(0, r0, n), s_px, pa_r.at[i], xn)

    def p_half(q, kt, h):
        return remote(
            pown.at[q, kt, pl.ds(h * T, T)], dw_part(q, kt * D + h * T, T), s_px, ph_r.at[q, 2 * kt + h], xn
        )

    def p_own(q, kt):
        return remote(pown.at[q, kt], dw_tile(q, kt), s_px, po_r.at[q - 2, kt], xn)

    def p_own_last():
        return remote(
            pown.at[3, 3, pl.ds(0, D - R)], dw_part(3, 3 * D, D - R), s_sum, po_r.at[1, 3], xn
        )

    def tail_store():
        return local(pown.at[3, 3, pl.ds(D - R, R)], tail, tail_sem)

    def p_other(q, kt):
        return remote(poth.at[q, kt], land.at[q - 2, kt], s_po, ps_r.at[q - 2, kt], xn)

    def p_trans(q, kt, r):
        part = pl.ds(r * Q, Q)
        return remote(poth.at[q, kt, part], bufy.at[q, kt, part], s_py, pf_r.at[q, 4 * kt + r], yn)

    def p_fwd(q, kt, r):
        part = pl.ds(r * Q, Q)
        return remote(bufy.at[q, kt, part], land.at[q, kt, part], s_px, pf_r.at[q, 4 * kt + r], xn)

    def p_trans_short():
        part = pl.ds(0, F)
        return remote(poth.at[1, 3, part], bufy.at[1, 3, part], s_last, pf_r.at[1, 12], yn)

    def p_fwd_short():
        part = pl.ds(0, F)
        return remote(bufy.at[1, 3, part], land.at[1, 3, part], s_last, pf_r.at[1, 12], xn)

    def p_trans_tail():
        return remote(poth.at[1, 3, pl.ds(F, R)], tail, s_last, pf_r.at[1, 13], yn)

    def p_extra():
        return remote(poth.at[1, 3, pl.ds(D - E, E)], extra, s_ex, ex_r, xn)

    def extra_to_y():
        return remote(poth.at[1, 3, pl.ds(D - E, E)], dw_part(1, 4 * D - E, E), s_py, py_ex, yn)

    def p_term(q, kt):
        return remote(poth.at[q, kt], dw_tile(q, kt), s_py, py_r.at[q, kt], yn)

    def p_term_short():
        part = pl.ds(0, D - E)
        return remote(poth.at[1, 3, part], dw_part(1, 3 * D, D - E), s_py, py_r.at[1, 3], yn)

    def sum_short():
        part = pl.ds(0, D - EY)
        return remote(poth.at[3, 3, part], dw_part(3, 3 * D, D - EY), s_last, py_r.at[3, 3], yn)

    def tail_y_store(src):
        return local(src.at[3, 3, pl.ds(D - EY, EY)], tail_y, tail_y_sem)

    def sum_to_y(q, kt):
        return remote(poth.at[q, kt], dw_tile(q, kt), s_sum, py_r.at[q, kt], yn)

    def drain(ref, sem):
        remote(ref, ref, sem, dyy_r.at[0], yn).wait_send()

    for cp in (dyq_load, xt_load, xq_load):
        cp.start()

    barrier = pltpu.get_barrier_semaphore()
    for dev in (sib, xn, yn):
        pl.semaphore_signal(barrier, inc=1, device_id=dev, device_id_type=MESH)
    pl.semaphore_wait(barrier, 3)

    dy_to_y(0).start()
    dy_to_y(1).start()

    @pl.when(is_a)
    def _():
        for i in range(8):
            w_own_to_x(i).start()
        for q in (2, 3):
            dy_to_y(q).start()

    @pl.when(is_b)
    def _():
        for i in range(4):
            w_to_y(i).start()
        for q in (2, 3):
            dy_to_y(q).start()
        for p in range(16):
            w_to_y_piece(p).start()

    dyq_load.wait()
    xt_load.wait()
    xq_load.wait()
    swap[0] = _tdot(dx_ref[:, 3 * D:3 * D + T], dyv[ME, OWN, :, :T])
    swap_part.start()
    dy_to_sib(OWN, 0).start()
    x_first(1).start()
    pown[0, 0, :T] = _tdot(dx_ref[:, :T], dyv[ME, OWN, :, :T])
    for cp in (x0_load, dy_load, x_load(1), x_load(2), x_load(3)):
        cp.start()
    x_first(0).start()
    for kt in (1, 2, 3):
        x_to_sib(kt).start()
    for q in (1, 2, 3):
        dy_to_sib(OWN, q).start()

    @pl.when(is_a)
    def _():
        for i in range(8):
            w_to_sib(OWN, i, ARG).start()

    swap_part.wait_recv()
    pown[0, 0, :T] = pown[0, 0, :T] + swap[1]

    @pl.when(is_b)
    def _():
        p_first(0).start()

    def p_part(j, c0, k0, n):
        dy = pl.ds(c0, T)
        acc = None
        for t in range(2):
            part = pl.ds(t * N, N)
            for who, base in ((ME, k0), (SIB, H + k0)):
                term = _tdot(dx_ref[part, cut(base, n)], dyv[who, j, part, dy])
                acc = term if acc is None else acc + term
        return acc

    def p_tile(dst, j, q, kt):
        loop(2, lambda h: put(dst.at[q, kt, pl.ds(h * T, T)], p_part(j, q * T, kt * D + h * T, T)))

    def put(ref, value):
        ref[...] = value

    x0_load.wait()
    dy_to_sib(OWN, 0).wait_recv()
    x_first(1).wait_recv()
    pown[0, 0, T:] = p_part(OWN, 0, T, T)

    @pl.when(is_b)
    def _():
        p_first(1).start()

    x_first(0).wait_recv()
    dy_load.wait()

    def own_tile(q, kt):
        if q == 0:
            x_load(kt).wait()
            x_to_sib(kt).wait_recv()
        p_tile(pown, OWN, q, kt)
        if q < 2:
            @pl.when(is_b)
            def _():
                p_half(q, kt, 0).start()
                p_half(q, kt, 1).start()

    for q in range(4):
        if q > 0:
            dy_to_sib(OWN, q).wait_recv()
        loop(4, lambda kt, q=q: own_tile(q, kt), int(q == 0))

    def trans_tile(q, kt):
        if q == 0:
            for r in range(4):
                p_trans(q, kt, r).start()
            return

        @pl.when(kt < 3)
        def _():
            for r in range(4):
                p_trans(q, kt, r).start()

        @pl.when(kt == 3)
        def _():
            p_trans_short().start()
            p_trans_tail().start()
            p_extra().start()

    def dy_in(q):
        dy_to_y(q).wait_recv()
        dy_to_sib(OTH, q).start()

    def other_pass(q):
        dy_in(q)
        dy_to_sib(OTH, q).wait_recv()

        def tile(kt):
            p_tile(poth, OTH, q, kt)
            if q < 2:
                @pl.when(jnp.logical_and(is_a, 4 * q + kt < 7))
                def _():
                    p_term(q, kt).start()

                @pl.when(jnp.logical_and(is_a, 4 * q + kt == 7))
                def _():
                    p_term_short().start()

                @pl.when(is_b)
                def _():
                    trans_tile(q, kt)
            else:
                @pl.when(is_b)
                def _():
                    p_other(q, kt).start()

        loop(4, tile)

    def w_loads(d, cc, src):
        ref = w_ref.at[qs(d)] if src == ARG else wbuf.at[cc, OWN, qs(d)]
        return (
            local(ref, wv.at[cc, OWN], wl_sem.at[cc, OWN]),
            local(wbuf.at[cc, OTH, qs(d)], wv.at[cc, OTH], wl_sem.at[cc, OTH]),
        )

    def start_loads(d, cc, src):
        for cp in w_loads(d, cc, src):
            cp.start()

    def wait_loads(d, cc, src):
        for cp in w_loads(d, cc, src):
            cp.wait()

    def dx_stripe(d, cc, lo=0, hi=4):
        cols = cut((c + cc * (1 - 2 * c)) * H + d * T, T, T)

        def rows(m):
            part = pl.ds(m * D, D)
            dx_ref[part, cols] = (
                _dot_t(dyv[ME, OWN, part, :], wv[cc, OWN]) + _dot_t(dyv[ME, OTH, part, :], wv[cc, OTH])
            ).astype(BF16)

        loop(hi, rows, lo)

    def pair_wait(d, src):
        w_to_sib(OWN, d, src).wait_recv()
        w_to_sib(OTH, d, BUF).wait_recv()

    other_pass(0)
    other_pass(1)

    @pl.when(is_a)
    def _():
        def add(q, kt):
            tile = dw_tile(q, kt)
            tile[...] = tile[...] + pown[q, kt]

        def final_early(t):
            q, kt = t // 4, t % 4

            @pl.when(t == 0)
            def _():
                for i in range(len(FIRST)):
                    p_first(i).wait_recv()

            @pl.when(t > 0)
            def _():
                p_half(q, kt, 0).wait_recv()
                p_half(q, kt, 1).wait_recv()
            add(q, kt)

        def final_late(t):
            q, kt = 2 + t // 4, t % 4
            p_own(q, kt).wait_recv()
            add(q, kt)

        def a_sum(q, kt):
            p_other(q, kt).wait_recv()
            poth[q, kt] = poth[q, kt] + land[q - 2, kt]

            @pl.when(4 * q + kt < 15)
            def _():
                sum_to_y(q, kt).start()

            @pl.when(4 * q + kt == 15)
            def _():
                sum_short().start()
                tail_y_store(poth).start()

        def early(i):
            w_to_y(i).wait_recv()
            w_fwd(i).start()
            w_to_sib(OTH, i, BUF).start()
            final_early(i)

        loop(4, early)
        dy_in(2)
        dy_to_sib(OTH, 2).wait_recv()

        def q2_tile(kt):
            p_tile(poth, OTH, 2, kt)
            final_early(4 + kt)

        loop(4, q2_tile)
        p_extra().wait_recv()
        poth[1, 3, D - E:] = poth[1, 3, D - E:] + extra[...]
        extra_to_y().start()
        start_loads(0, ME, ARG)
        dy_in(3)

        def step(i):
            @pl.when(i < 16)
            def _():
                w_to_y_piece(i).wait_recv()
                w_fwd_piece(i).start()

                @pl.when(i % 4 == 3)
                def _():
                    w_to_sib(OTH, 4 + i // 4, BUF).start()

            @pl.when(i >= 16)
            def _():
                k = i - 16
                q, kt, r = k // 16, (k // 4) % 4, k % 4
                p_trans(q, kt, r).wait_recv()
                p_fwd(q, kt, r).start()

            @pl.when(i == 0)
            def _():
                dy_to_sib(OTH, 3).wait_recv()

            @pl.when(i < 4)
            def _():
                p_tile(poth, OTH, 3, i)

            @pl.when(jnp.logical_and(i >= 4, i < 36))
            def _():
                e = (i - 4) // 2
                d, cc = e // 2, e % 2
                odd = i % 2

                @pl.when(jnp.logical_and(odd == 0, cc == ME))
                def _():
                    pair_wait(d, ARG)
                    start_loads(d, SIB, BUF)
                    wait_loads(d, ME, ARG)

                @pl.when(jnp.logical_and(odd == 0, cc == SIB))
                def _():
                    @pl.when(d < 7)
                    def _():
                        start_loads(d + 1, ME, ARG)
                    wait_loads(d, SIB, BUF)

                dx_stripe(d, cc, 2 * odd, 2 * odd + 2)

            @pl.when(jnp.logical_and(i < 8, i % 2 == 1))
            def _():
                a_sum(2, i // 2)

            @pl.when(jnp.logical_and(jnp.logical_and(i >= 10, i < 26), i % 4 == 2))
            def _():
                a_sum(3, (i - 10) // 4)

            @pl.when(jnp.logical_and(i >= 26, i % 4 == 2))
            def _():
                final_late((i - 26) // 4)

        loop(44, step)
        p_trans_short().wait_recv()
        p_fwd_short().start()
        low = dw_part(3, 4 * D - R, R)
        low[...] = pown[3, 3, D - R:]
        final_late(5)
        final_late(6)
        p_trans_tail().wait_recv()
        p_own_last().wait_recv()
        top = dw_part(3, 3 * D, D - R)
        top[...] = top[...] + pown[3, 3, :D - R]
        drain(wbuf.at[ME], s_w)
        tail_y_store(poth).wait()
        drain(dyv.at[ME, OWN, pl.ds(0, H - T)], s_px)
        drain(land, s_py)
        drain(dyv.at[ME, OWN, pl.ds(0, H - T)], s_sum)
        drain(land.at[0, 0, pl.ds(0, D - EY + F)], s_last)

    @pl.when(is_b)
    def _():
        other_pass(2)
        other_pass(3)
        for t in range(7):
            p_own(2 + t // 4, t % 4).start()
        p_own_last().start()
        tail_store().start()
        tail_y_store(pown).start()

        def own_w(i):
            w_own_to_x(i).wait_recv()
            w_to_sib(OWN, i, BUF).start()

        loop(8, own_w)

        def stripes(d):
            @pl.when(d < 4)
            def _():
                w_to_y(d).wait_recv()

            @pl.when(d >= 4)
            def _():
                for p in range(4):
                    w_to_y_piece(4 * (d - 4) + p).wait_recv()
            w_to_sib(OTH, d, BUF).start()
            start_loads(d, ME, BUF)
            pair_wait(d, BUF)
            start_loads(d, SIB, BUF)
            for cc in (ME, SIB):
                wait_loads(d, cc, BUF)
                dx_stripe(d, cc)

        loop(8, stripes)

        def fin(i):
            q, kt, r = i // 16, (i // 4) % 4, i % 4

            @pl.when(r == 0)
            def _():
                p_term(q, kt).wait_recv()
            p_fwd(q, kt, r).wait_recv()
            tile = dw_part(q, kt * D + r * Q, Q)
            tile[...] = tile[...] + land[q, kt, pl.ds(r * Q, Q)]

        loop(28, fin)
        p_term_short().wait_recv()
        p_fwd_short().wait_recv()
        tile = dw_part(1, 3 * D, F)
        tile[...] = tile[...] + land[1, 3, :F]
        extra_to_y().wait_recv()
        for t in range(7):
            sum_to_y(2 + t // 4, t % 4).wait_recv()
        sum_short().wait_recv()
        tail_y_store(pown).wait()
        tail_store().wait()
        drain(wbuf.at[ME, OWN], s_w)
        drain(dw_ref.at[pl.ds(0, H - Q)], s_px)
        drain(land.at[0, 0, pl.ds(0, D - R)], s_sum)
        drain(land.at[0, 0, pl.ds(0, D - E)], s_last)
        drain(land, s_po)
        drain(extra, s_ex)
        drain(dyv.at[ME, OWN, pl.ds(0, H - T)], s_py)

    drain(dyv.at[ME], s_dys)
    drain(dyv.at[ME, OWN], s_dyy)
    drain(wbuf.at[ME], s_xs)
    drain(swap.at[0], s_sw)
    drain(wbuf.at[ME], s_ws)


def store_kernel(dx_ref, dw_ref, dx_out, dw_out, sem):
    copies = []
    for i in range(4):
        part = pl.ds(i * D, D)
        copies.append(pltpu.make_async_copy(dx_ref.at[part], dx_out.at[part], sem.at[0, i]))
        copies.append(pltpu.make_async_copy(dw_ref.at[part], dw_out.at[part], sem.at[1, i]))
    for cp in copies:
        cp.start()
    for cp in copies:
        cp.wait()


def add_kernel(done_ref, dw_ref, tail_ref, tail_y_ref, dw_out, buf, buf_y, sem, sem_y):
    is_a = lax.axis_index("row") // 2 == lax.axis_index("col")
    rows = cut(jnp.where(is_a, H - R, 3 * D + F), R, 16)
    cols = cut(jnp.where(is_a, 3 * T, T), T)
    buf[...] = dw_ref[rows, cols] + tail_ref[...]
    first = pltpu.make_async_copy(buf, dw_out.at[rows, cols], sem)
    first.start()
    rows_y, cols_y = pl.ds(H - EY, EY), cut(jnp.where(is_a, 0, 3 * T), T)
    buf_y[...] = jnp.where(is_a, dw_ref[rows_y, cols_y], tail_y_ref[...])
    second = pltpu.make_async_copy(buf_y, dw_out.at[rows_y, cols_y], sem_y)
    second.start()
    first.wait()
    second.wait()


def local_backward(act_blk, w_blk, grad_blk):
    any_spec = pl.BlockSpec(memory_space=pl.ANY)
    vmem_spec = pl.BlockSpec(memory_space=pltpu.VMEM)
    dma = pltpu.SemaphoreType.DMA
    outs = pl.pallas_call(
        kernel,
        out_shape=(
            pltpu.VMEM((H, 2 * H), BF16),
            pltpu.VMEM((H, N), F32),
            jax.ShapeDtypeStruct((2, 2, H, N), BF16),
            jax.ShapeDtypeStruct((2, 4, D, T), F32),
            jax.ShapeDtypeStruct((R, T), F32),
            jax.ShapeDtypeStruct((EY, T), F32),
        ),
        in_specs=[any_spec] * 3,
        out_specs=(vmem_spec,) * 2 + (any_spec,) * 4,
        scratch_shapes=[
            pltpu.VMEM((2, 2, H, N), BF16),
            pltpu.VMEM((4, 4, D, T), F32),
            pltpu.VMEM((4, 4, D, T), F32),
            pltpu.VMEM((2, 2, T, N), BF16),
            pltpu.VMEM((2, 4, D, T), F32),
            pltpu.VMEM((E, T), F32),
            pltpu.VMEM((2, T, T), F32),
            dma, dma((4,)), dma((2, 4)), dma((4,)), dma((4,)), dma((5,)), dma((2, 8)), dma((16,)), dma((2, 8)),
            dma((4,)), dma((2, 8)), dma((2, 4)), dma((2, 4)), dma((4, 4)), dma((2, 16)),
            dma, dma, dma, dma, dma, dma, dma, dma, dma, dma((2, 2)), dma,
            dma, dma, dma, dma, dma, dma, dma, dma, dma, dma,
        ],
        compiler_params=pltpu.CompilerParams(
            collective_id=0, has_side_effects=True, vmem_limit_bytes=41_800_000
        ),
        cost_estimate=pl.CostEstimate(flops=8 * H * H * H, bytes_accessed=100 << 20, transcendentals=0),
    )(act_blk, w_blk, grad_blk)
    tail = lax.ppermute(outs[4], "row", [(i, (i + 2) % 4) for i in range(4)])
    tail_y = lax.ppermute(outs[5], "col", [(0, 1), (1, 0)])
    dx, dw = pl.pallas_call(
        store_kernel,
        out_shape=(jax.ShapeDtypeStruct((H, 2 * H), BF16), jax.ShapeDtypeStruct((H, N), F32)),
        in_specs=[vmem_spec] * 2,
        out_specs=(any_spec,) * 2,
        scratch_shapes=[dma((2, 4))],
        compiler_params=pltpu.CompilerParams(vmem_limit_bytes=1 << 20),
        cost_estimate=pl.CostEstimate(flops=0, bytes_accessed=48 << 20, transcendentals=0),
    )(outs[0], outs[1])
    dw = pl.pallas_call(
        add_kernel,
        out_shape=jax.ShapeDtypeStruct((H, N), F32),
        in_specs=[any_spec] + [vmem_spec] * 3,
        out_specs=any_spec,
        scratch_shapes=[pltpu.VMEM((R, T), F32), pltpu.VMEM((EY, T), F32), dma, dma],
        input_output_aliases={0: 0},
        compiler_params=pltpu.CompilerParams(vmem_limit_bytes=2 << 20),
        cost_estimate=pl.CostEstimate(flops=0, bytes_accessed=1 << 20, transcendentals=0),
    )(dw, outs[1], tail, tail_y)
    return dx, dw


def solution(mesh):
    io_spec = P(("dp", "row"), "col")
    w_spec = P("row", "col")
    return jax.shard_map(
        local_backward, mesh=mesh, in_specs=(io_spec, w_spec, io_spec), out_specs=(io_spec, io_spec), check_vma=False
    )
```

```python
import jax
import jax.numpy as jnp
from jax import lax
from jax.experimental import pallas as pl
from jax.experimental.pallas import tpu as pltpu
from jax.sharding import PartitionSpec as P

MESH = pl.DeviceIdType.MESH
F32 = jnp.float32
BF16 = jnp.bfloat16
H, N, D, T, Q, S = 2048, 1024, 512, 256, 128, 64
R = 368
E = 112
EY = 72
F = D - E - R
ME, SIB = 0, 1
OWN, OTH = 0, 1
ARG, BUF = "arg", "buf"
FIRST = ((0, Q), (Q, Q), (T, T))


def _tdot(a, b):
    return lax.dot_general(a, b, (((0,), (0,)), ((), ())), preferred_element_type=F32)


def _dot_t(a, b):
    return lax.dot_general(a, b, (((1,), (1,)), ((), ())), preferred_element_type=F32)


def loop(n, f, start=0):
    def body(i, carry):
        f(i)
        return carry

    lax.fori_loop(start, n, body, start)


def cut(k0, n, unit=Q):
    return pl.ds(pl.multiple_of(k0, unit), n)


def kernel(
    x_ref, w_ref, dy_ref,
    dx_ref, dw_ref, wbuf, bufy, tail, tail_y,
    dyv, pown, poth, wv, land, extra, swap,
    dy_sem, x_sem, dys_r, dyy_r, xs_r, xf_r, w_r, wp_r, ws_r, pa_r, ph_r, po_r, ps_r, py_r, pf_r,
    s_dys, s_dyy, s_xs, s_w, s_ws, s_px, s_po, s_py, s_sum, wl_sem, tail_sem, tail_y_sem, s_ex, ex_r, py_ex, dyq_sem, xt_sem, xq_sem, s_sw, sw_r, s_last,
):
    row = lax.axis_index("row")
    y = lax.axis_index("col")
    x = row // 2
    c = row % 2
    is_a = x == y
    is_b = x != y
    sib = {"row": row + 1 - 2 * c}
    xn = {"row": (row + 2) % 4}
    yn = {"col": 1 - y}

    def remote(src, dst, ssem, rsem, dev):
        return pltpu.make_async_remote_copy(
            src_ref=src, dst_ref=dst, send_sem=ssem, recv_sem=rsem, device_id=dev, device_id_type=MESH
        )

    def local(src, dst, sem):
        return pltpu.make_async_copy(src, dst, sem)

    def qs(q):
        return pl.ds(q * T, T)

    def xo(k0, n):
        return dx_ref.at[:, cut(k0, n)]

    def xs(k0, n):
        return dx_ref.at[:, cut(H + k0, n)]

    def dw_part(q, r0, n):
        return dw_ref.at[pl.ds(r0, n), cut(q * T, T)]

    def dw_tile(q, kt):
        return dw_part(q, kt * D, D)

    dyq_load = local(dy_ref.at[:, pl.ds(0, T)], dyv.at[ME, OWN, :, pl.ds(0, T)], dyq_sem)
    dy_load = local(dy_ref.at[:, pl.ds(T, N - T)], dyv.at[ME, OWN, :, pl.ds(T, N - T)], dy_sem)
    def xt_load(h):
        return local(x_ref.at[:, pl.ds((1 - c) * H + h * Q, Q)], xo(3 * D + h * Q, Q), xt_sem.at[h])

    def xq_load(h):
        return local(x_ref.at[:, pl.ds(c * H + h * Q, Q)], xo(h * Q, Q), xq_sem.at[h])

    def swap_part(h):
        part = pl.ds(h * Q, Q)
        return remote(swap.at[0, part], swap.at[1, part], s_sw, sw_r.at[h], sib)

    x0_load = local(x_ref.at[:, pl.ds(c * H + T, D - T)], xo(T, D - T), x_sem.at[0])
    def x_load(kt):
        return local(x_ref.at[:, pl.ds(c * H + kt * D, D)], xo(kt * D, D), x_sem.at[kt])

    def x_cols_to_sib(k0, n, sem):
        return remote(x_ref.at[:, pl.ds((1 - c) * H + k0, n)], xs(k0, n), s_xs, sem, sib)

    def x_to_sib(kt):
        return x_cols_to_sib(kt * D, D, xs_r.at[kt])

    def x_first(i):
        return x_cols_to_sib(i * T, T, xf_r.at[i])

    def dy_to_sib(j, q):
        src = dy_ref.at[:, qs(q)] if j == OWN else dyv.at[ME, OTH, :, qs(q)]
        return remote(src, dyv.at[SIB, j, :, qs(q)], s_dys, dys_r.at[j, q], sib)

    def dy_to_y(q):
        return remote(dy_ref.at[:, qs(q)], dyv.at[ME, OTH, :, qs(q)], s_dyy, dyy_r.at[q], yn)

    def w_own_to_x(i):
        return remote(w_ref.at[qs(i)], wbuf.at[ME, OWN, qs(i)], s_w, w_r.at[OWN, i], xn)

    def w_to_y(i):
        return remote(w_ref.at[qs(i)], wbuf.at[ME, OTH, qs(i)], s_w, w_r.at[OTH, i], yn)

    def w_fwd(i):
        return remote(wbuf.at[ME, OTH, qs(i)], wbuf.at[ME, OTH, qs(i)], s_w, w_r.at[OTH, i], xn)

    def w_piece(p):
        return pl.ds(N + p * S, S)

    def w_to_y_piece(p):
        return remote(w_ref.at[w_piece(p)], wbuf.at[ME, OTH, w_piece(p)], s_w, wp_r.at[p], yn)

    def w_fwd_piece(p):
        return remote(wbuf.at[ME, OTH, w_piece(p)], wbuf.at[ME, OTH, w_piece(p)], s_w, wp_r.at[p], xn)

    def w_to_sib(j, i, src):
        ref = w_ref.at[qs(i)] if src == ARG else wbuf.at[ME, j, qs(i)]
        return remote(ref, wbuf.at[SIB, j, qs(i)], s_ws, ws_r.at[j, i], sib)

    def p_first(i):
        r0, n = FIRST[i]
        return remote(pown.at[0, 0, pl.ds(r0, n)], dw_part(0, r0, n), s_px, pa_r.at[i], xn)

    def p_half(q, kt, h):
        return remote(
            pown.at[q, kt, pl.ds(h * T, T)], dw_part(q, kt * D + h * T, T), s_px, ph_r.at[q, 2 * kt + h], xn
        )

    def p_own(q, kt):
        return remote(pown.at[q, kt], dw_tile(q, kt), s_px, po_r.at[q - 2, kt], xn)

    def p_own_last():
        return remote(
            pown.at[3, 3, pl.ds(0, D - R)], dw_part(3, 3 * D, D - R), s_sum, po_r.at[1, 3], xn
        )

    def tail_store():
        return local(pown.at[3, 3, pl.ds(D - R, R)], tail, tail_sem)

    def p_other(q, kt):
        return remote(poth.at[q, kt], land.at[q - 2, kt], s_po, ps_r.at[q - 2, kt], xn)

    def p_trans(q, kt, r):
        part = pl.ds(r * Q, Q)
        return remote(poth.at[q, kt, part], bufy.at[q, kt, part], s_py, pf_r.at[q, 4 * kt + r], yn)

    def p_fwd(q, kt, r):
        part = pl.ds(r * Q, Q)
        return remote(bufy.at[q, kt, part], land.at[q, kt, part], s_px, pf_r.at[q, 4 * kt + r], xn)

    def p_trans_short():
        part = pl.ds(0, F)
        return remote(poth.at[1, 3, part], bufy.at[1, 3, part], s_last, pf_r.at[1, 12], yn)

    def p_fwd_short():
        part = pl.ds(0, F)
        return remote(bufy.at[1, 3, part], land.at[1, 3, part], s_last, pf_r.at[1, 12], xn)

    def p_trans_tail():
        return remote(poth.at[1, 3, pl.ds(F, R)], tail, s_last, pf_r.at[1, 13], yn)

    def p_extra():
        return remote(poth.at[1, 3, pl.ds(D - E, E)], extra, s_ex, ex_r, xn)

    def extra_to_y():
        return remote(poth.at[1, 3, pl.ds(D - E, E)], dw_part(1, 4 * D - E, E), s_py, py_ex, yn)

    def p_term(q, kt):
        return remote(poth.at[q, kt], dw_tile(q, kt), s_py, py_r.at[q, kt], yn)

    def p_term_short():
        part = pl.ds(0, D - E)
        return remote(poth.at[1, 3, part], dw_part(1, 3 * D, D - E), s_py, py_r.at[1, 3], yn)

    def sum_short():
        part = pl.ds(0, D - EY)
        return remote(poth.at[3, 3, part], dw_part(3, 3 * D, D - EY), s_last, py_r.at[3, 3], yn)

    def tail_y_store(src):
        return local(src.at[3, 3, pl.ds(D - EY, EY)], tail_y, tail_y_sem)

    def sum_to_y(q, kt):
        return remote(poth.at[q, kt], dw_tile(q, kt), s_sum, py_r.at[q, kt], yn)

    def drain(ref, sem):
        remote(ref, ref, sem, dyy_r.at[0], yn).wait_send()

    for cp in (dyq_load, xt_load(0), xq_load(0)):
        cp.start()

    barrier = pltpu.get_barrier_semaphore()
    for dev in (sib, xn, yn):
        pl.semaphore_signal(barrier, inc=1, device_id=dev, device_id_type=MESH)
    pl.semaphore_wait(barrier, 3)

    dy_to_y(0).start()
    dy_to_y(1).start()

    @pl.when(is_a)
    def _():
        for i in range(8):
            w_own_to_x(i).start()
        for q in (2, 3):
            dy_to_y(q).start()

    @pl.when(is_b)
    def _():
        for i in range(4):
            w_to_y(i).start()
        for q in (2, 3):
            dy_to_y(q).start()
        for p in range(16):
            w_to_y_piece(p).start()

    def swap_send(h):
        xt_load(h).wait()
        xq_load(h).wait()
        if h == 0:
            xt_load(1).start()
            xq_load(1).start()
        swap[0, pl.ds(h * Q, Q)] = _tdot(dx_ref[:, 3 * D + h * Q:3 * D + h * Q + Q], dyv[ME, OWN, :, :T])
        swap_part(h).start()

    def own_first(h):
        pown[0, 0, pl.ds(h * Q, Q)] = _tdot(dx_ref[:, h * Q:h * Q + Q], dyv[ME, OWN, :, :T])

    def swap_add(h):
        part = pl.ds(h * Q, Q)
        swap_part(h).wait_recv()
        pown[0, 0, part] = pown[0, 0, part] + swap[1, part]

        @pl.when(is_b)
        def _():
            p_first(h).start()

    dyq_load.wait()
    swap_send(0)
    own_first(0)
    swap_send(1)
    dy_to_sib(OWN, 0).start()
    x_first(1).start()
    swap_add(0)
    own_first(1)
    swap_add(1)
    for cp in (x0_load, dy_load, x_load(1), x_load(2), x_load(3)):
        cp.start()
    x_first(0).start()
    for kt in (1, 2, 3):
        x_to_sib(kt).start()
    for q in (1, 2, 3):
        dy_to_sib(OWN, q).start()

    @pl.when(is_a)
    def _():
        for i in range(8):
            w_to_sib(OWN, i, ARG).start()

    def p_part(j, c0, k0, n):
        dy = pl.ds(c0, T)
        acc = None
        for t in range(2):
            part = pl.ds(t * N, N)
            for who, base in ((ME, k0), (SIB, H + k0)):
                term = _tdot(dx_ref[part, cut(base, n)], dyv[who, j, part, dy])
                acc = term if acc is None else acc + term
        return acc

    def p_tile(dst, j, q, kt):
        loop(2, lambda h: put(dst.at[q, kt, pl.ds(h * T, T)], p_part(j, q * T, kt * D + h * T, T)))

    def put(ref, value):
        ref[...] = value

    x0_load.wait()
    dy_to_sib(OWN, 0).wait_recv()
    x_first(1).wait_recv()
    pown[0, 0, T:] = p_part(OWN, 0, T, T)

    @pl.when(is_b)
    def _():
        p_first(2).start()

    x_first(0).wait_recv()
    dy_load.wait()

    def own_tile(q, kt):
        if q == 0:
            x_load(kt).wait()
            x_to_sib(kt).wait_recv()
        p_tile(pown, OWN, q, kt)
        if q < 2:
            @pl.when(is_b)
            def _():
                p_half(q, kt, 0).start()
                p_half(q, kt, 1).start()

    for q in range(4):
        if q > 0:
            dy_to_sib(OWN, q).wait_recv()
        loop(4, lambda kt, q=q: own_tile(q, kt), int(q == 0))

    def trans_tile(q, kt):
        if q == 0:
            for r in range(4):
                p_trans(q, kt, r).start()
            return

        @pl.when(kt < 3)
        def _():
            for r in range(4):
                p_trans(q, kt, r).start()

        @pl.when(kt == 3)
        def _():
            p_trans_short().start()
            p_trans_tail().start()
            p_extra().start()

    def dy_in(q):
        dy_to_y(q).wait_recv()
        dy_to_sib(OTH, q).start()

    def other_pass(q):
        dy_in(q)
        dy_to_sib(OTH, q).wait_recv()

        def tile(kt):
            p_tile(poth, OTH, q, kt)
            if q < 2:
                @pl.when(jnp.logical_and(is_a, 4 * q + kt < 7))
                def _():
                    p_term(q, kt).start()

                @pl.when(jnp.logical_and(is_a, 4 * q + kt == 7))
                def _():
                    p_term_short().start()

                @pl.when(is_b)
                def _():
                    trans_tile(q, kt)
            else:
                @pl.when(is_b)
                def _():
                    p_other(q, kt).start()

        loop(4, tile)

    def w_loads(d, cc, src):
        ref = w_ref.at[qs(d)] if src == ARG else wbuf.at[cc, OWN, qs(d)]
        return (
            local(ref, wv.at[cc, OWN], wl_sem.at[cc, OWN]),
            local(wbuf.at[cc, OTH, qs(d)], wv.at[cc, OTH], wl_sem.at[cc, OTH]),
        )

    def start_loads(d, cc, src):
        for cp in w_loads(d, cc, src):
            cp.start()

    def wait_loads(d, cc, src):
        for cp in w_loads(d, cc, src):
            cp.wait()

    def dx_stripe(d, cc, lo=0, hi=4):
        cols = cut((c + cc * (1 - 2 * c)) * H + d * T, T, T)

        def rows(m):
            part = pl.ds(m * D, D)
            dx_ref[part, cols] = (
                _dot_t(dyv[ME, OWN, part, :], wv[cc, OWN]) + _dot_t(dyv[ME, OTH, part, :], wv[cc, OTH])
            ).astype(BF16)

        loop(hi, rows, lo)

    def pair_wait(d, src):
        w_to_sib(OWN, d, src).wait_recv()
        w_to_sib(OTH, d, BUF).wait_recv()

    other_pass(0)
    other_pass(1)

    @pl.when(is_a)
    def _():
        def add(q, kt):
            tile = dw_tile(q, kt)
            tile[...] = tile[...] + pown[q, kt]

        def final_early(t):
            q, kt = t // 4, t % 4

            @pl.when(t == 0)
            def _():
                for i in range(len(FIRST)):
                    p_first(i).wait_recv()

            @pl.when(t > 0)
            def _():
                p_half(q, kt, 0).wait_recv()
                p_half(q, kt, 1).wait_recv()
            add(q, kt)

        def final_late(t):
            q, kt = 2 + t // 4, t % 4
            p_own(q, kt).wait_recv()
            add(q, kt)

        def a_sum(q, kt):
            p_other(q, kt).wait_recv()
            poth[q, kt] = poth[q, kt] + land[q - 2, kt]

            @pl.when(4 * q + kt < 15)
            def _():
                sum_to_y(q, kt).start()

            @pl.when(4 * q + kt == 15)
            def _():
                sum_short().start()
                tail_y_store(poth).start()

        def early(i):
            w_to_y(i).wait_recv()
            w_fwd(i).start()
            w_to_sib(OTH, i, BUF).start()
            final_early(i)

        loop(4, early)
        dy_in(2)
        dy_to_sib(OTH, 2).wait_recv()

        def q2_tile(kt):
            p_tile(poth, OTH, 2, kt)
            final_early(4 + kt)

        loop(4, q2_tile)
        p_extra().wait_recv()
        poth[1, 3, D - E:] = poth[1, 3, D - E:] + extra[...]
        extra_to_y().start()
        start_loads(0, ME, ARG)
        dy_in(3)

        def step(i):
            @pl.when(i < 16)
            def _():
                w_to_y_piece(i).wait_recv()
                w_fwd_piece(i).start()

                @pl.when(i % 4 == 3)
                def _():
                    w_to_sib(OTH, 4 + i // 4, BUF).start()

            @pl.when(i >= 16)
            def _():
                k = i - 16
                q, kt, r = k // 16, (k // 4) % 4, k % 4
                p_trans(q, kt, r).wait_recv()
                p_fwd(q, kt, r).start()

            @pl.when(i == 0)
            def _():
                dy_to_sib(OTH, 3).wait_recv()

            @pl.when(i < 4)
            def _():
                p_tile(poth, OTH, 3, i)

            @pl.when(jnp.logical_and(i >= 4, i < 36))
            def _():
                e = (i - 4) // 2
                d, cc = e // 2, e % 2
                odd = i % 2

                @pl.when(jnp.logical_and(odd == 0, cc == ME))
                def _():
                    pair_wait(d, ARG)
                    start_loads(d, SIB, BUF)
                    wait_loads(d, ME, ARG)

                @pl.when(jnp.logical_and(odd == 0, cc == SIB))
                def _():
                    @pl.when(d < 7)
                    def _():
                        start_loads(d + 1, ME, ARG)
                    wait_loads(d, SIB, BUF)

                dx_stripe(d, cc, 2 * odd, 2 * odd + 2)

            @pl.when(jnp.logical_and(i < 8, i % 2 == 1))
            def _():
                a_sum(2, i // 2)

            @pl.when(jnp.logical_and(jnp.logical_and(i >= 10, i < 26), i % 4 == 2))
            def _():
                a_sum(3, (i - 10) // 4)

            @pl.when(jnp.logical_and(i >= 26, i % 4 == 2))
            def _():
                final_late((i - 26) // 4)

        loop(44, step)
        p_trans_short().wait_recv()
        p_fwd_short().start()
        low = dw_part(3, 4 * D - R, R)
        low[...] = pown[3, 3, D - R:]
        final_late(5)
        final_late(6)
        p_trans_tail().wait_recv()
        p_own_last().wait_recv()
        top = dw_part(3, 3 * D, D - R)
        top[...] = top[...] + pown[3, 3, :D - R]
        drain(wbuf.at[ME], s_w)
        tail_y_store(poth).wait()
        drain(dyv.at[ME, OWN, pl.ds(0, H - T)], s_px)
        drain(land, s_py)
        drain(dyv.at[ME, OWN, pl.ds(0, H - T)], s_sum)
        drain(land.at[0, 0, pl.ds(0, D - EY + F)], s_last)

    @pl.when(is_b)
    def _():
        other_pass(2)
        other_pass(3)
        for t in range(7):
            p_own(2 + t // 4, t % 4).start()
        p_own_last().start()
        tail_store().start()
        tail_y_store(pown).start()

        def own_w(i):
            w_own_to_x(i).wait_recv()
            w_to_sib(OWN, i, BUF).start()

        loop(8, own_w)

        def stripes(d):
            @pl.when(d < 4)
            def _():
                w_to_y(d).wait_recv()

            @pl.when(d >= 4)
            def _():
                for p in range(4):
                    w_to_y_piece(4 * (d - 4) + p).wait_recv()
            w_to_sib(OTH, d, BUF).start()
            start_loads(d, ME, BUF)
            pair_wait(d, BUF)
            start_loads(d, SIB, BUF)
            for cc in (ME, SIB):
                wait_loads(d, cc, BUF)
                dx_stripe(d, cc)

        loop(8, stripes)

        def fin(i):
            q, kt, r = i // 16, (i // 4) % 4, i % 4

            @pl.when(r == 0)
            def _():
                p_term(q, kt).wait_recv()
            p_fwd(q, kt, r).wait_recv()
            tile = dw_part(q, kt * D + r * Q, Q)
            tile[...] = tile[...] + land[q, kt, pl.ds(r * Q, Q)]

        loop(28, fin)
        p_term_short().wait_recv()
        p_fwd_short().wait_recv()
        tile = dw_part(1, 3 * D, F)
        tile[...] = tile[...] + land[1, 3, :F]
        extra_to_y().wait_recv()
        for t in range(7):
            sum_to_y(2 + t // 4, t % 4).wait_recv()
        sum_short().wait_recv()
        tail_y_store(pown).wait()
        tail_store().wait()
        drain(wbuf.at[ME, OWN], s_w)
        drain(dw_ref.at[pl.ds(0, H - Q)], s_px)
        drain(land.at[0, 0, pl.ds(0, D - R)], s_sum)
        drain(land.at[0, 0, pl.ds(0, D - E)], s_last)
        drain(land, s_po)
        drain(extra, s_ex)
        drain(dyv.at[ME, OWN, pl.ds(0, H - T)], s_py)

    drain(dyv.at[ME], s_dys)
    drain(dyv.at[ME, OWN], s_dyy)
    drain(wbuf.at[ME], s_xs)
    drain(swap.at[0], s_sw)
    drain(wbuf.at[ME], s_ws)


def store_kernel(dx_ref, dw_ref, dx_out, dw_out, sem):
    copies = []
    for i in range(4):
        part = pl.ds(i * D, D)
        copies.append(pltpu.make_async_copy(dx_ref.at[part], dx_out.at[part], sem.at[0, i]))
        copies.append(pltpu.make_async_copy(dw_ref.at[part], dw_out.at[part], sem.at[1, i]))
    for cp in copies:
        cp.start()
    for cp in copies:
        cp.wait()


def add_kernel(done_ref, dw_ref, tail_ref, tail_y_ref, dw_out, buf, buf_y, sem, sem_y):
    is_a = lax.axis_index("row") // 2 == lax.axis_index("col")
    rows = cut(jnp.where(is_a, H - R, 3 * D + F), R, 16)
    cols = cut(jnp.where(is_a, 3 * T, T), T)
    buf[...] = dw_ref[rows, cols] + tail_ref[...]
    first = pltpu.make_async_copy(buf, dw_out.at[rows, cols], sem)
    first.start()
    rows_y, cols_y = pl.ds(H - EY, EY), cut(jnp.where(is_a, 0, 3 * T), T)
    buf_y[...] = jnp.where(is_a, dw_ref[rows_y, cols_y], tail_y_ref[...])
    second = pltpu.make_async_copy(buf_y, dw_out.at[rows_y, cols_y], sem_y)
    second.start()
    first.wait()
    second.wait()


def local_backward(act_blk, w_blk, grad_blk):
    any_spec = pl.BlockSpec(memory_space=pl.ANY)
    vmem_spec = pl.BlockSpec(memory_space=pltpu.VMEM)
    dma = pltpu.SemaphoreType.DMA
    outs = pl.pallas_call(
        kernel,
        out_shape=(
            pltpu.VMEM((H, 2 * H), BF16),
            pltpu.VMEM((H, N), F32),
            jax.ShapeDtypeStruct((2, 2, H, N), BF16),
            jax.ShapeDtypeStruct((2, 4, D, T), F32),
            jax.ShapeDtypeStruct((R, T), F32),
            jax.ShapeDtypeStruct((EY, T), F32),
        ),
        in_specs=[any_spec] * 3,
        out_specs=(vmem_spec,) * 2 + (any_spec,) * 4,
        scratch_shapes=[
            pltpu.VMEM((2, 2, H, N), BF16),
            pltpu.VMEM((4, 4, D, T), F32),
            pltpu.VMEM((4, 4, D, T), F32),
            pltpu.VMEM((2, 2, T, N), BF16),
            pltpu.VMEM((2, 4, D, T), F32),
            pltpu.VMEM((E, T), F32),
            pltpu.VMEM((2, T, T), F32),
            dma, dma((4,)), dma((2, 4)), dma((4,)), dma((4,)), dma((5,)), dma((2, 8)), dma((16,)), dma((2, 8)),
            dma((4,)), dma((2, 8)), dma((2, 4)), dma((2, 4)), dma((4, 4)), dma((2, 16)),
            dma, dma, dma, dma, dma, dma, dma, dma, dma, dma((2, 2)), dma,
            dma, dma, dma, dma, dma, dma((2,)), dma((2,)), dma, dma((2,)), dma,
        ],
        compiler_params=pltpu.CompilerParams(
            collective_id=0, has_side_effects=True, vmem_limit_bytes=41_800_000
        ),
        cost_estimate=pl.CostEstimate(flops=8 * H * H * H, bytes_accessed=100 << 20, transcendentals=0),
    )(act_blk, w_blk, grad_blk)
    tail = lax.ppermute(outs[4], "row", [(i, (i + 2) % 4) for i in range(4)])
    tail_y = lax.ppermute(outs[5], "col", [(0, 1), (1, 0)])
    dx, dw = pl.pallas_call(
        store_kernel,
        out_shape=(jax.ShapeDtypeStruct((H, 2 * H), BF16), jax.ShapeDtypeStruct((H, N), F32)),
        in_specs=[vmem_spec] * 2,
        out_specs=(any_spec,) * 2,
        scratch_shapes=[dma((2, 4))],
        compiler_params=pltpu.CompilerParams(vmem_limit_bytes=1 << 20),
        cost_estimate=pl.CostEstimate(flops=0, bytes_accessed=48 << 20, transcendentals=0),
    )(outs[0], outs[1])
    dw = pl.pallas_call(
        add_kernel,
        out_shape=jax.ShapeDtypeStruct((H, N), F32),
        in_specs=[any_spec] + [vmem_spec] * 3,
        out_specs=any_spec,
        scratch_shapes=[pltpu.VMEM((R, T), F32), pltpu.VMEM((EY, T), F32), dma, dma],
        input_output_aliases={0: 0},
        compiler_params=pltpu.CompilerParams(vmem_limit_bytes=2 << 20),
        cost_estimate=pl.CostEstimate(flops=0, bytes_accessed=1 << 20, transcendentals=0),
    )(dw, outs[1], tail, tail_y)
    return dx, dw


def solution(mesh):
    io_spec = P(("dp", "row"), "col")
    w_spec = P("row", "col")
    return jax.shard_map(
        local_backward, mesh=mesh, in_specs=(io_spec, w_spec, io_spec), out_specs=(io_spec, io_spec), check_vma=False
    )
```

```python
import jax
import jax.numpy as jnp
from jax import lax
from jax.experimental import pallas as pl
from jax.experimental.pallas import tpu as pltpu
from jax.sharding import PartitionSpec as P

MESH = pl.DeviceIdType.MESH
F32 = jnp.float32
BF16 = jnp.bfloat16
H, N, D, T, Q, S = 2048, 1024, 512, 256, 128, 64
R = 376
E = 112
EY = 96
F = D - E - R
ME, SIB = 0, 1
OWN, OTH = 0, 1
ARG, BUF = "arg", "buf"
FIRST = ((0, Q), (Q, Q), (T, T))


def _tdot(a, b):
    return lax.dot_general(a, b, (((0,), (0,)), ((), ())), preferred_element_type=F32)


def _dot_t(a, b):
    return lax.dot_general(a, b, (((1,), (1,)), ((), ())), preferred_element_type=F32)


def loop(n, f, start=0):
    def body(i, carry):
        f(i)
        return carry

    lax.fori_loop(start, n, body, start)


def cut(k0, n, unit=Q):
    return pl.ds(pl.multiple_of(k0, unit), n)


def kernel(
    x_ref, w_ref, dy_ref,
    dx_ref, dw_ref, wbuf, bufy, tail, tail_y,
    dyv, pown, poth, wv, land, extra, swap,
    dy_sem, x_sem, dys_r, dyy_r, xs_r, xf_r, w_r, wp_r, ws_r, pa_r, ph_r, po_r, ps_r, py_r, pf_r,
    s_dys, s_dyy, s_xs, s_w, s_ws, s_px, s_po, s_py, s_sum, wl_sem, tail_sem, tail_y_sem, s_ex, ex_r, py_ex, dyq_sem, xt_sem, xq_sem, s_sw, sw_r, s_last,
):
    row = lax.axis_index("row")
    y = lax.axis_index("col")
    x = row // 2
    c = row % 2
    is_a = x == y
    is_b = x != y
    sib = {"row": row + 1 - 2 * c}
    xn = {"row": (row + 2) % 4}
    yn = {"col": 1 - y}

    def remote(src, dst, ssem, rsem, dev):
        return pltpu.make_async_remote_copy(
            src_ref=src, dst_ref=dst, send_sem=ssem, recv_sem=rsem, device_id=dev, device_id_type=MESH
        )

    def local(src, dst, sem):
        return pltpu.make_async_copy(src, dst, sem)

    def qs(q):
        return pl.ds(q * T, T)

    def xo(k0, n):
        return dx_ref.at[:, cut(k0, n)]

    def xs(k0, n):
        return dx_ref.at[:, cut(H + k0, n)]

    def dw_part(q, r0, n):
        return dw_ref.at[pl.ds(r0, n), cut(q * T, T)]

    def dw_tile(q, kt):
        return dw_part(q, kt * D, D)

    dyq_load = local(dy_ref.at[:, pl.ds(0, T)], dyv.at[ME, OWN, :, pl.ds(0, T)], dyq_sem)
    dy_load = local(dy_ref.at[:, pl.ds(T, N - T)], dyv.at[ME, OWN, :, pl.ds(T, N - T)], dy_sem)
    def xt_load(h):
        return local(x_ref.at[:, pl.ds((1 - c) * H + h * Q, Q)], xo(3 * D + h * Q, Q), xt_sem.at[h])

    def xq_load(h):
        return local(x_ref.at[:, pl.ds(c * H + h * Q, Q)], xo(h * Q, Q), xq_sem.at[h])

    def swap_part(h):
        part = pl.ds(h * Q, Q)
        return remote(swap.at[0, part], swap.at[1, part], s_sw, sw_r.at[h], sib)

    x0_load = local(x_ref.at[:, pl.ds(c * H + T, D - T)], xo(T, D - T), x_sem.at[0])
    def x_load(kt):
        return local(x_ref.at[:, pl.ds(c * H + kt * D, D)], xo(kt * D, D), x_sem.at[kt])

    def x_cols_to_sib(k0, n, sem):
        return remote(x_ref.at[:, pl.ds((1 - c) * H + k0, n)], xs(k0, n), s_xs, sem, sib)

    def x_to_sib(kt):
        return x_cols_to_sib(kt * D, D, xs_r.at[kt])

    def x_first(i):
        return x_cols_to_sib(i * T, T, xf_r.at[i])

    def dy_to_sib(j, q):
        src = dy_ref.at[:, qs(q)] if j == OWN else dyv.at[ME, OTH, :, qs(q)]
        return remote(src, dyv.at[SIB, j, :, qs(q)], s_dys, dys_r.at[j, q], sib)

    def dy_to_y(q):
        return remote(dy_ref.at[:, qs(q)], dyv.at[ME, OTH, :, qs(q)], s_dyy, dyy_r.at[q], yn)

    def w_own_to_x(i):
        return remote(w_ref.at[qs(i)], wbuf.at[ME, OWN, qs(i)], s_w, w_r.at[OWN, i], xn)

    def w_to_y(i):
        return remote(w_ref.at[qs(i)], wbuf.at[ME, OTH, qs(i)], s_w, w_r.at[OTH, i], yn)

    def w_fwd(i):
        return remote(wbuf.at[ME, OTH, qs(i)], wbuf.at[ME, OTH, qs(i)], s_w, w_r.at[OTH, i], xn)

    def w_piece(p):
        return pl.ds(N + p * S, S)

    def w_to_y_piece(p):
        return remote(w_ref.at[w_piece(p)], wbuf.at[ME, OTH, w_piece(p)], s_w, wp_r.at[p], yn)

    def w_fwd_piece(p):
        return remote(wbuf.at[ME, OTH, w_piece(p)], wbuf.at[ME, OTH, w_piece(p)], s_w, wp_r.at[p], xn)

    def w_to_sib(j, i, src):
        ref = w_ref.at[qs(i)] if src == ARG else wbuf.at[ME, j, qs(i)]
        return remote(ref, wbuf.at[SIB, j, qs(i)], s_ws, ws_r.at[j, i], sib)

    def p_first(i):
        r0, n = FIRST[i]
        return remote(pown.at[0, 0, pl.ds(r0, n)], dw_part(0, r0, n), s_px, pa_r.at[i], xn)

    def p_half(q, kt, h):
        return remote(
            pown.at[q, kt, pl.ds(h * T, T)], dw_part(q, kt * D + h * T, T), s_px, ph_r.at[q, 2 * kt + h], xn
        )

    def p_own(q, kt):
        return remote(pown.at[q, kt], dw_tile(q, kt), s_px, po_r.at[q - 2, kt], xn)

    def p_own_last():
        return remote(
            pown.at[3, 3, pl.ds(0, D - R)], dw_part(3, 3 * D, D - R), s_sum, po_r.at[1, 3], xn
        )

    def tail_store():
        return local(pown.at[3, 3, pl.ds(D - R, R)], tail, tail_sem)

    def p_other(q, kt):
        return remote(poth.at[q, kt], land.at[q - 2, kt], s_po, ps_r.at[q - 2, kt], xn)

    def p_trans(q, kt, r):
        part = pl.ds(r * Q, Q)
        return remote(poth.at[q, kt, part], bufy.at[q, kt, part], s_py, pf_r.at[q, 4 * kt + r], yn)

    def p_fwd(q, kt, r):
        part = pl.ds(r * Q, Q)
        return remote(bufy.at[q, kt, part], land.at[q, kt, part], s_px, pf_r.at[q, 4 * kt + r], xn)

    def p_trans_short():
        part = pl.ds(0, F)
        return remote(poth.at[1, 3, part], bufy.at[1, 3, part], s_last, pf_r.at[1, 12], yn)

    def p_fwd_short():
        part = pl.ds(0, F)
        return remote(bufy.at[1, 3, part], land.at[1, 3, part], s_last, pf_r.at[1, 12], xn)

    def p_trans_tail():
        return remote(poth.at[1, 3, pl.ds(F, R)], tail, s_last, pf_r.at[1, 13], yn)

    def p_extra():
        return remote(poth.at[1, 3, pl.ds(D - E, E)], extra, s_ex, ex_r, xn)

    def extra_to_y():
        return remote(poth.at[1, 3, pl.ds(D - E, E)], dw_part(1, 4 * D - E, E), s_py, py_ex, yn)

    def p_term(q, kt):
        return remote(poth.at[q, kt], dw_tile(q, kt), s_py, py_r.at[q, kt], yn)

    def p_term_short():
        part = pl.ds(0, D - E)
        return remote(poth.at[1, 3, part], dw_part(1, 3 * D, D - E), s_py, py_r.at[1, 3], yn)

    def sum_short():
        part = pl.ds(0, D - EY)
        return remote(poth.at[3, 3, part], dw_part(3, 3 * D, D - EY), s_last, py_r.at[3, 3], yn)

    def tail_y_store(src):
        return local(src.at[3, 3, pl.ds(D - EY, EY)], tail_y, tail_y_sem)

    def sum_to_y(q, kt):
        return remote(poth.at[q, kt], dw_tile(q, kt), s_sum, py_r.at[q, kt], yn)

    def drain(ref, sem):
        remote(ref, ref, sem, dyy_r.at[0], yn).wait_send()

    for cp in (dyq_load, xt_load(0), xq_load(0)):
        cp.start()

    barrier = pltpu.get_barrier_semaphore()
    for dev in (sib, xn, yn):
        pl.semaphore_signal(barrier, inc=1, device_id=dev, device_id_type=MESH)
    pl.semaphore_wait(barrier, 3)

    dy_to_y(0).start()
    dy_to_y(1).start()

    @pl.when(is_a)
    def _():
        for i in range(8):
            w_own_to_x(i).start()
        for q in (2, 3):
            dy_to_y(q).start()

    @pl.when(is_b)
    def _():
        for i in range(4):
            w_to_y(i).start()
        for q in (2, 3):
            dy_to_y(q).start()
        for p in range(16):
            w_to_y_piece(p).start()

    def swap_send(h):
        xt_load(h).wait()
        xq_load(h).wait()
        if h == 0:
            xt_load(1).start()
            xq_load(1).start()
        swap[0, pl.ds(h * Q, Q)] = _tdot(dx_ref[:, 3 * D + h * Q:3 * D + h * Q + Q], dyv[ME, OWN, :, :T])
        swap_part(h).start()

    def own_first(h):
        pown[0, 0, pl.ds(h * Q, Q)] = _tdot(dx_ref[:, h * Q:h * Q + Q], dyv[ME, OWN, :, :T])

    def swap_add(h):
        part = pl.ds(h * Q, Q)
        swap_part(h).wait_recv()
        pown[0, 0, part] = pown[0, 0, part] + swap[1, part]

        @pl.when(is_b)
        def _():
            p_first(h).start()

    dyq_load.wait()
    swap_send(0)
    own_first(0)
    swap_send(1)
    dy_to_sib(OWN, 0).start()
    x_first(1).start()
    swap_add(0)
    own_first(1)
    swap_add(1)
    for cp in (x0_load, dy_load, x_load(1), x_load(2), x_load(3)):
        cp.start()
    x_first(0).start()
    for kt in (1, 2, 3):
        x_to_sib(kt).start()
    for q in (1, 2, 3):
        dy_to_sib(OWN, q).start()

    @pl.when(is_a)
    def _():
        for i in range(8):
            w_to_sib(OWN, i, ARG).start()

    def p_part(j, c0, k0, n):
        dy = pl.ds(c0, T)
        acc = None
        for t in range(2):
            part = pl.ds(t * N, N)
            for who, base in ((ME, k0), (SIB, H + k0)):
                term = _tdot(dx_ref[part, cut(base, n)], dyv[who, j, part, dy])
                acc = term if acc is None else acc + term
        return acc

    def p_tile(dst, j, q, kt):
        loop(2, lambda h: put(dst.at[q, kt, pl.ds(h * T, T)], p_part(j, q * T, kt * D + h * T, T)))

    def put(ref, value):
        ref[...] = value

    x0_load.wait()
    dy_to_sib(OWN, 0).wait_recv()
    x_first(1).wait_recv()
    pown[0, 0, T:] = p_part(OWN, 0, T, T)

    @pl.when(is_b)
    def _():
        p_first(2).start()

    x_first(0).wait_recv()
    dy_load.wait()

    def own_tile(q, kt):
        if q == 0:
            x_load(kt).wait()
            x_to_sib(kt).wait_recv()
        p_tile(pown, OWN, q, kt)
        if q < 2:
            @pl.when(is_b)
            def _():
                p_half(q, kt, 0).start()
                p_half(q, kt, 1).start()

    for q in range(4):
        if q > 0:
            dy_to_sib(OWN, q).wait_recv()
        loop(4, lambda kt, q=q: own_tile(q, kt), int(q == 0))

    def trans_tile(q, kt):
        if q == 0:
            for r in range(4):
                p_trans(q, kt, r).start()
            return

        @pl.when(kt < 3)
        def _():
            for r in range(4):
                p_trans(q, kt, r).start()

        @pl.when(kt == 3)
        def _():
            p_trans_short().start()
            p_trans_tail().start()
            p_extra().start()

    def dy_in(q):
        dy_to_y(q).wait_recv()
        dy_to_sib(OTH, q).start()

    def other_pass(q):
        dy_in(q)
        dy_to_sib(OTH, q).wait_recv()

        def tile(kt):
            p_tile(poth, OTH, q, kt)
            if q < 2:
                @pl.when(jnp.logical_and(is_a, 4 * q + kt < 7))
                def _():
                    p_term(q, kt).start()

                @pl.when(jnp.logical_and(is_a, 4 * q + kt == 7))
                def _():
                    p_term_short().start()

                @pl.when(is_b)
                def _():
                    trans_tile(q, kt)
            else:
                @pl.when(is_b)
                def _():
                    p_other(q, kt).start()

        loop(4, tile)

    def w_loads(d, cc, src):
        ref = w_ref.at[qs(d)] if src == ARG else wbuf.at[cc, OWN, qs(d)]
        return (
            local(ref, wv.at[cc, OWN], wl_sem.at[cc, OWN]),
            local(wbuf.at[cc, OTH, qs(d)], wv.at[cc, OTH], wl_sem.at[cc, OTH]),
        )

    def start_loads(d, cc, src):
        for cp in w_loads(d, cc, src):
            cp.start()

    def wait_loads(d, cc, src):
        for cp in w_loads(d, cc, src):
            cp.wait()

    def dx_stripe(d, cc, lo=0, hi=4):
        cols = cut((c + cc * (1 - 2 * c)) * H + d * T, T, T)

        def rows(m):
            part = pl.ds(m * D, D)
            dx_ref[part, cols] = (
                _dot_t(dyv[ME, OWN, part, :], wv[cc, OWN]) + _dot_t(dyv[ME, OTH, part, :], wv[cc, OTH])
            ).astype(BF16)

        loop(hi, rows, lo)

    def pair_wait(d, src):
        w_to_sib(OWN, d, src).wait_recv()
        w_to_sib(OTH, d, BUF).wait_recv()

    other_pass(0)
    other_pass(1)

    @pl.when(is_a)
    def _():
        def add(q, kt):
            tile = dw_tile(q, kt)
            tile[...] = tile[...] + pown[q, kt]

        def final_early(t):
            q, kt = t // 4, t % 4

            @pl.when(t == 0)
            def _():
                for i in range(len(FIRST)):
                    p_first(i).wait_recv()

            @pl.when(t > 0)
            def _():
                p_half(q, kt, 0).wait_recv()
                p_half(q, kt, 1).wait_recv()
            add(q, kt)

        def final_late(t):
            q, kt = 2 + t // 4, t % 4
            p_own(q, kt).wait_recv()
            add(q, kt)

        def a_sum(q, kt):
            p_other(q, kt).wait_recv()
            poth[q, kt] = poth[q, kt] + land[q - 2, kt]

            @pl.when(4 * q + kt < 15)
            def _():
                sum_to_y(q, kt).start()

            @pl.when(4 * q + kt == 15)
            def _():
                sum_short().start()
                tail_y_store(poth).start()

        def early(i):
            w_to_y(i).wait_recv()
            w_fwd(i).start()
            w_to_sib(OTH, i, BUF).start()
            final_early(i)

        loop(4, early)
        dy_in(2)
        dy_to_sib(OTH, 2).wait_recv()

        def q2_tile(kt):
            p_tile(poth, OTH, 2, kt)
            final_early(4 + kt)

        loop(4, q2_tile)
        p_extra().wait_recv()
        poth[1, 3, D - E:] = poth[1, 3, D - E:] + extra[...]
        extra_to_y().start()
        start_loads(0, ME, ARG)
        dy_in(3)

        def step(i):
            @pl.when(i < 16)
            def _():
                w_to_y_piece(i).wait_recv()
                w_fwd_piece(i).start()

                @pl.when(i % 4 == 3)
                def _():
                    w_to_sib(OTH, 4 + i // 4, BUF).start()

            @pl.when(i >= 16)
            def _():
                k = i - 16
                q, kt, r = k // 16, (k // 4) % 4, k % 4
                p_trans(q, kt, r).wait_recv()
                p_fwd(q, kt, r).start()

            @pl.when(i == 0)
            def _():
                dy_to_sib(OTH, 3).wait_recv()

            @pl.when(i < 4)
            def _():
                p_tile(poth, OTH, 3, i)

            @pl.when(jnp.logical_and(i >= 4, i < 36))
            def _():
                e = (i - 4) // 2
                d, cc = e // 2, e % 2
                odd = i % 2

                @pl.when(jnp.logical_and(odd == 0, cc == ME))
                def _():
                    pair_wait(d, ARG)
                    start_loads(d, SIB, BUF)
                    wait_loads(d, ME, ARG)

                @pl.when(jnp.logical_and(odd == 0, cc == SIB))
                def _():
                    @pl.when(d < 7)
                    def _():
                        start_loads(d + 1, ME, ARG)
                    wait_loads(d, SIB, BUF)

                dx_stripe(d, cc, 2 * odd, 2 * odd + 2)

            @pl.when(jnp.logical_and(i < 8, i % 2 == 1))
            def _():
                a_sum(2, i // 2)

            @pl.when(jnp.logical_and(jnp.logical_and(i >= 10, i < 26), i % 4 == 2))
            def _():
                a_sum(3, (i - 10) // 4)

            @pl.when(jnp.logical_and(i >= 26, i % 4 == 2))
            def _():
                final_late((i - 26) // 4)

        loop(44, step)
        p_trans_short().wait_recv()
        p_fwd_short().start()
        low = dw_part(3, 4 * D - R, R)
        low[...] = pown[3, 3, D - R:]
        final_late(5)
        final_late(6)
        p_trans_tail().wait_recv()
        p_own_last().wait_recv()
        top = dw_part(3, 3 * D, D - R)
        top[...] = top[...] + pown[3, 3, :D - R]
        drain(wbuf.at[ME], s_w)
        tail_y_store(poth).wait()
        drain(dyv.at[ME, OWN, pl.ds(0, H - T)], s_px)
        drain(land, s_py)
        drain(dyv.at[ME, OWN, pl.ds(0, H - T)], s_sum)
        drain(land.at[0, 0, pl.ds(0, D - EY + F)], s_last)

    @pl.when(is_b)
    def _():
        other_pass(2)
        other_pass(3)
        for t in range(7):
            p_own(2 + t // 4, t % 4).start()
        p_own_last().start()
        tail_store().start()
        tail_y_store(pown).start()

        def own_w(i):
            w_own_to_x(i).wait_recv()
            w_to_sib(OWN, i, BUF).start()

        loop(8, own_w)

        def stripes(d):
            @pl.when(d < 4)
            def _():
                w_to_y(d).wait_recv()

            @pl.when(d >= 4)
            def _():
                for p in range(4):
                    w_to_y_piece(4 * (d - 4) + p).wait_recv()
            w_to_sib(OTH, d, BUF).start()
            start_loads(d, ME, BUF)
            pair_wait(d, BUF)
            start_loads(d, SIB, BUF)
            for cc in (ME, SIB):
                wait_loads(d, cc, BUF)
                dx_stripe(d, cc)

        loop(8, stripes)

        def fin(i):
            q, kt, r = i // 16, (i // 4) % 4, i % 4

            @pl.when(r == 0)
            def _():
                p_term(q, kt).wait_recv()
            p_fwd(q, kt, r).wait_recv()
            tile = dw_part(q, kt * D + r * Q, Q)
            tile[...] = tile[...] + land[q, kt, pl.ds(r * Q, Q)]

        loop(28, fin)
        p_term_short().wait_recv()
        p_fwd_short().wait_recv()
        tile = dw_part(1, 3 * D, F)
        tile[...] = tile[...] + land[1, 3, :F]
        extra_to_y().wait_recv()
        for t in range(7):
            sum_to_y(2 + t // 4, t % 4).wait_recv()
        sum_short().wait_recv()
        tail_y_store(pown).wait()
        tail_store().wait()
        drain(wbuf.at[ME, OWN], s_w)
        drain(dw_ref.at[pl.ds(0, H - Q)], s_px)
        drain(land.at[0, 0, pl.ds(0, D - R)], s_sum)
        drain(land.at[0, 0, pl.ds(0, D - E)], s_last)
        drain(land, s_po)
        drain(extra, s_ex)
        drain(dyv.at[ME, OWN, pl.ds(0, H - T)], s_py)

    drain(dyv.at[ME], s_dys)
    drain(dyv.at[ME, OWN], s_dyy)
    drain(wbuf.at[ME], s_xs)
    drain(swap.at[0], s_sw)
    drain(wbuf.at[ME], s_ws)


def store_kernel(dx_ref, dw_ref, dx_out, dw_out, sem):
    copies = []
    for i in range(16):
        part = pl.ds(i * Q, Q)
        copies.append(pltpu.make_async_copy(dx_ref.at[part], dx_out.at[part], sem.at[0, i]))
        if i % 2:
            part = pl.ds((i - 1) * Q, T)
            copies.append(pltpu.make_async_copy(dw_ref.at[part], dw_out.at[part], sem.at[1, i]))
    for cp in copies:
        cp.start()
    for cp in copies:
        cp.wait()


def add_kernel(done_ref, dw_ref, tail_ref, tail_y_ref, dw_out, buf, buf_y, sem, sem_y):
    is_a = lax.axis_index("row") // 2 == lax.axis_index("col")
    rows = cut(jnp.where(is_a, H - R, 3 * D + F), R, 8)
    cols = cut(jnp.where(is_a, 3 * T, T), T)
    buf[...] = dw_ref[rows, cols] + tail_ref[...]
    first = pltpu.make_async_copy(buf, dw_out.at[rows, cols], sem)
    first.start()
    rows_y, cols_y = pl.ds(H - EY, EY), cut(jnp.where(is_a, 0, 3 * T), T)
    buf_y[...] = jnp.where(is_a, dw_ref[rows_y, cols_y], tail_y_ref[...])
    second = pltpu.make_async_copy(buf_y, dw_out.at[rows_y, cols_y], sem_y)
    second.start()
    first.wait()
    second.wait()


def local_backward(act_blk, w_blk, grad_blk):
    any_spec = pl.BlockSpec(memory_space=pl.ANY)
    vmem_spec = pl.BlockSpec(memory_space=pltpu.VMEM)
    dma = pltpu.SemaphoreType.DMA
    outs = pl.pallas_call(
        kernel,
        out_shape=(
            pltpu.VMEM((H, 2 * H), BF16),
            pltpu.VMEM((H, N), F32),
            jax.ShapeDtypeStruct((2, 2, H, N), BF16),
            jax.ShapeDtypeStruct((2, 4, D, T), F32),
            jax.ShapeDtypeStruct((R, T), F32),
            jax.ShapeDtypeStruct((EY, T), F32),
        ),
        in_specs=[any_spec] * 3,
        out_specs=(vmem_spec,) * 2 + (any_spec,) * 4,
        scratch_shapes=[
            pltpu.VMEM((2, 2, H, N), BF16),
            pltpu.VMEM((4, 4, D, T), F32),
            pltpu.VMEM((4, 4, D, T), F32),
            pltpu.VMEM((2, 2, T, N), BF16),
            pltpu.VMEM((2, 4, D, T), F32),
            pltpu.VMEM((E, T), F32),
            pltpu.VMEM((2, T, T), F32),
            dma, dma((4,)), dma((2, 4)), dma((4,)), dma((4,)), dma((5,)), dma((2, 8)), dma((16,)), dma((2, 8)),
            dma((4,)), dma((2, 8)), dma((2, 4)), dma((2, 4)), dma((4, 4)), dma((2, 16)),
            dma, dma, dma, dma, dma, dma, dma, dma, dma, dma((2, 2)), dma,
            dma, dma, dma, dma, dma, dma((2,)), dma((2,)), dma, dma((2,)), dma,
        ],
        compiler_params=pltpu.CompilerParams(
            collective_id=0, has_side_effects=True, vmem_limit_bytes=41_800_000
        ),
        cost_estimate=pl.CostEstimate(flops=8 * H * H * H, bytes_accessed=100 << 20, transcendentals=0),
    )(act_blk, w_blk, grad_blk)
    tail = lax.ppermute(outs[4], "row", [(i, (i + 2) % 4) for i in range(4)])
    tail_y = lax.ppermute(outs[5], "col", [(0, 1), (1, 0)])
    dx, dw = pl.pallas_call(
        store_kernel,
        out_shape=(jax.ShapeDtypeStruct((H, 2 * H), BF16), jax.ShapeDtypeStruct((H, N), F32)),
        in_specs=[vmem_spec] * 2,
        out_specs=(any_spec,) * 2,
        scratch_shapes=[dma((2, 16))],
        compiler_params=pltpu.CompilerParams(vmem_limit_bytes=1 << 20),
        cost_estimate=pl.CostEstimate(flops=0, bytes_accessed=48 << 20, transcendentals=0),
    )(outs[0], outs[1])
    dw = pl.pallas_call(
        add_kernel,
        out_shape=jax.ShapeDtypeStruct((H, N), F32),
        in_specs=[any_spec] + [vmem_spec] * 3,
        out_specs=any_spec,
        scratch_shapes=[pltpu.VMEM((R, T), F32), pltpu.VMEM((EY, T), F32), dma, dma],
        input_output_aliases={0: 0},
        compiler_params=pltpu.CompilerParams(vmem_limit_bytes=2 << 20),
        cost_estimate=pl.CostEstimate(flops=0, bytes_accessed=1 << 20, transcendentals=0),
    )(dw, outs[1], tail, tail_y)
    return dx, dw


def solution(mesh):
    io_spec = P(("dp", "row"), "col")
    w_spec = P("row", "col")
    return jax.shard_map(
        local_backward, mesh=mesh, in_specs=(io_spec, w_spec, io_spec), out_specs=(io_spec, io_spec), check_vma=False
    )
```

```python
import jax
import jax.numpy as jnp
from jax import lax
from jax.experimental import pallas as pl
from jax.experimental.pallas import tpu as pltpu
from jax.sharding import PartitionSpec as P

MESH = pl.DeviceIdType.MESH
F32 = jnp.float32
BF16 = jnp.bfloat16
H, N, D, T, Q, S = 2048, 1024, 512, 256, 128, 64
R = 376
E = 112
EY = 96
F = D - E - R
ME, SIB = 0, 1
OWN, OTH = 0, 1
ARG, BUF = "arg", "buf"
FIRST = ((0, Q), (Q, Q), (T, T))


def _tdot(a, b):
    return lax.dot_general(a, b, (((0,), (0,)), ((), ())), preferred_element_type=F32)


def _dot_t(a, b):
    return lax.dot_general(a, b, (((1,), (1,)), ((), ())), preferred_element_type=F32)


def loop(n, f, start=0):
    def body(i, carry):
        f(i)
        return carry

    lax.fori_loop(start, n, body, start)


def cut(k0, n, unit=Q):
    return pl.ds(pl.multiple_of(k0, unit), n)


def kernel(
    x_ref, w_ref, dy_ref,
    dx_ref, dw_ref, wbuf, bufy, tail, tail_y,
    dyv, pown, poth, wv, land, extra, swap,
    dy_sem, x_sem, dys_r, dyy_r, xs_r, xf_r, w_r, wp_r, ws_r, pa_r, ph_r, po_r, ps_r, py_r, pf_r,
    s_dys, s_dyy, s_xs, s_w, s_ws, s_px, s_po, s_py, s_sum, wl_sem, tail_sem, tail_y_sem, s_ex, ex_r, py_ex, dyq_sem, xt_sem, xq_sem, s_sw, sw_r, s_last,
):
    row = lax.axis_index("row")
    y = lax.axis_index("col")
    x = row // 2
    c = row % 2
    is_a = x == y
    is_b = x != y
    sib = {"row": row + 1 - 2 * c}
    xn = {"row": (row + 2) % 4}
    yn = {"col": 1 - y}

    def remote(src, dst, ssem, rsem, dev):
        return pltpu.make_async_remote_copy(
            src_ref=src, dst_ref=dst, send_sem=ssem, recv_sem=rsem, device_id=dev, device_id_type=MESH
        )

    def local(src, dst, sem):
        return pltpu.make_async_copy(src, dst, sem)

    def qs(q):
        return pl.ds(q * T, T)

    def xo(k0, n):
        return dx_ref.at[:, cut(k0, n)]

    def xs(k0, n):
        return dx_ref.at[:, cut(H + k0, n)]

    def dw_part(q, r0, n):
        return dw_ref.at[pl.ds(r0, n), cut(q * T, T)]

    def dw_tile(q, kt):
        return dw_part(q, kt * D, D)

    dyq_load = local(dy_ref.at[:, pl.ds(0, T)], dyv.at[ME, OWN, :, pl.ds(0, T)], dyq_sem)
    dy_load = local(dy_ref.at[:, pl.ds(T, N - T)], dyv.at[ME, OWN, :, pl.ds(T, N - T)], dy_sem)
    def xt_load(h):
        return local(x_ref.at[:, pl.ds((1 - c) * H + h * Q, Q)], xo(3 * D + h * Q, Q), xt_sem.at[h])

    def xq_load(h):
        return local(x_ref.at[:, pl.ds(c * H + h * Q, Q)], xo(h * Q, Q), xq_sem.at[h])

    def swap_part(h):
        part = pl.ds(h * Q, Q)
        return remote(swap.at[0, part], swap.at[1, part], s_sw, sw_r.at[h], sib)

    x0_load = local(x_ref.at[:, pl.ds(c * H + T, D - T)], xo(T, D - T), x_sem.at[0])
    def x_load(kt):
        return local(x_ref.at[:, pl.ds(c * H + kt * D, D)], xo(kt * D, D), x_sem.at[kt])

    def x_cols_to_sib(k0, n, sem):
        return remote(x_ref.at[:, pl.ds((1 - c) * H + k0, n)], xs(k0, n), s_xs, sem, sib)

    def x_to_sib(kt):
        return x_cols_to_sib(kt * D, D, xs_r.at[kt])

    def x_first(i):
        return x_cols_to_sib(i * T, T, xf_r.at[i])

    def dy_to_sib(j, q):
        src = dy_ref.at[:, qs(q)] if j == OWN else dyv.at[ME, OTH, :, qs(q)]
        return remote(src, dyv.at[SIB, j, :, qs(q)], s_dys, dys_r.at[j, q], sib)

    def dy_to_y(q):
        return remote(dy_ref.at[:, qs(q)], dyv.at[ME, OTH, :, qs(q)], s_dyy, dyy_r.at[q], yn)

    def w_own_to_x(i):
        return remote(w_ref.at[qs(i)], wbuf.at[ME, OWN, qs(i)], s_w, w_r.at[OWN, i], xn)

    def w_to_y(i):
        return remote(w_ref.at[qs(i)], wbuf.at[ME, OTH, qs(i)], s_w, w_r.at[OTH, i], yn)

    def w_fwd(i):
        return remote(wbuf.at[ME, OTH, qs(i)], wbuf.at[ME, OTH, qs(i)], s_w, w_r.at[OTH, i], xn)

    def w_piece(p):
        return pl.ds(N + p * S, S)

    def w_to_y_piece(p):
        return remote(w_ref.at[w_piece(p)], wbuf.at[ME, OTH, w_piece(p)], s_w, wp_r.at[p], yn)

    def w_fwd_piece(p):
        return remote(wbuf.at[ME, OTH, w_piece(p)], wbuf.at[ME, OTH, w_piece(p)], s_w, wp_r.at[p], xn)

    def w_to_sib(j, i, src):
        ref = w_ref.at[qs(i)] if src == ARG else wbuf.at[ME, j, qs(i)]
        return remote(ref, wbuf.at[SIB, j, qs(i)], s_ws, ws_r.at[j, i], sib)

    def p_first(i):
        r0, n = FIRST[i]
        return remote(pown.at[0, 0, pl.ds(r0, n)], dw_part(0, r0, n), s_px, pa_r.at[i], xn)

    def p_half(q, kt, h):
        return remote(
            pown.at[q, kt, pl.ds(h * T, T)], dw_part(q, kt * D + h * T, T), s_px, ph_r.at[q, 2 * kt + h], xn
        )

    def p_own(q, kt):
        return remote(pown.at[q, kt], dw_tile(q, kt), s_px, po_r.at[q - 2, kt], xn)

    def p_own_last():
        return remote(
            pown.at[3, 3, pl.ds(0, D - R)], dw_part(3, 3 * D, D - R), s_sum, po_r.at[1, 3], xn
        )

    def tail_store():
        return local(pown.at[3, 3, pl.ds(D - R, R)], tail, tail_sem)

    def p_other(q, kt):
        return remote(poth.at[q, kt], land.at[q - 2, kt], s_po, ps_r.at[q - 2, kt], xn)

    def p_trans(q, kt, r):
        part = pl.ds(r * Q, Q)
        return remote(poth.at[q, kt, part], bufy.at[q, kt, part], s_py, pf_r.at[q, 4 * kt + r], yn)

    def p_fwd(q, kt, r):
        part = pl.ds(r * Q, Q)
        return remote(bufy.at[q, kt, part], land.at[q, kt, part], s_px, pf_r.at[q, 4 * kt + r], xn)

    def p_trans_short():
        part = pl.ds(0, F)
        return remote(poth.at[1, 3, part], bufy.at[1, 3, part], s_last, pf_r.at[1, 12], yn)

    def p_fwd_short():
        part = pl.ds(0, F)
        return remote(bufy.at[1, 3, part], land.at[1, 3, part], s_last, pf_r.at[1, 12], xn)

    def p_trans_tail():
        return remote(poth.at[1, 3, pl.ds(F, R)], tail, s_last, pf_r.at[1, 13], yn)

    def p_extra():
        return remote(poth.at[1, 3, pl.ds(D - E, E)], extra, s_ex, ex_r, xn)

    def extra_to_y():
        return remote(poth.at[1, 3, pl.ds(D - E, E)], dw_part(1, 4 * D - E, E), s_py, py_ex, yn)

    def p_term(q, kt):
        return remote(poth.at[q, kt], dw_tile(q, kt), s_py, py_r.at[q, kt], yn)

    def p_term_short():
        part = pl.ds(0, D - E)
        return remote(poth.at[1, 3, part], dw_part(1, 3 * D, D - E), s_py, py_r.at[1, 3], yn)

    def sum_short():
        part = pl.ds(0, D - EY)
        return remote(poth.at[3, 3, part], dw_part(3, 3 * D, D - EY), s_last, py_r.at[3, 3], yn)

    def tail_y_store(src):
        return local(src.at[3, 3, pl.ds(D - EY, EY)], tail_y, tail_y_sem)

    def sum_to_y(q, kt):
        return remote(poth.at[q, kt], dw_tile(q, kt), s_sum, py_r.at[q, kt], yn)

    def drain(ref, sem):
        remote(ref, ref, sem, dyy_r.at[0], yn).wait_send()

    for cp in (dyq_load, xt_load(0), xq_load(0)):
        cp.start()

    barrier = pltpu.get_barrier_semaphore()
    for dev in (sib, xn, yn):
        pl.semaphore_signal(barrier, inc=1, device_id=dev, device_id_type=MESH)
    pl.semaphore_wait(barrier, 3)

    dy_to_y(0).start()
    dy_to_y(1).start()

    @pl.when(is_a)
    def _():
        for i in range(8):
            w_own_to_x(i).start()
        for q in (2, 3):
            dy_to_y(q).start()

    @pl.when(is_b)
    def _():
        for i in range(4):
            w_to_y(i).start()
        for q in (2, 3):
            dy_to_y(q).start()
        for p in range(16):
            w_to_y_piece(p).start()

    def swap_send(h):
        xt_load(h).wait()
        xq_load(h).wait()
        if h == 0:
            xt_load(1).start()
            xq_load(1).start()
        swap[0, pl.ds(h * Q, Q)] = _tdot(dx_ref[:, 3 * D + h * Q:3 * D + h * Q + Q], dyv[ME, OWN, :, :T])
        swap_part(h).start()

    def own_first(h):
        pown[0, 0, pl.ds(h * Q, Q)] = _tdot(dx_ref[:, h * Q:h * Q + Q], dyv[ME, OWN, :, :T])

    def swap_add(h):
        part = pl.ds(h * Q, Q)
        swap_part(h).wait_recv()
        pown[0, 0, part] = pown[0, 0, part] + swap[1, part]

        @pl.when(is_b)
        def _():
            p_first(h).start()

    dyq_load.wait()
    swap_send(0)
    own_first(0)
    swap_send(1)
    dy_to_sib(OWN, 0).start()
    x_first(1).start()
    swap_add(0)
    own_first(1)
    swap_add(1)
    for cp in (x0_load, dy_load, x_load(1), x_load(2), x_load(3)):
        cp.start()
    x_first(0).start()
    for kt in (1, 2, 3):
        x_to_sib(kt).start()
    for q in (1, 2, 3):
        dy_to_sib(OWN, q).start()

    @pl.when(is_a)
    def _():
        for i in range(8):
            w_to_sib(OWN, i, ARG).start()

    def p_part(j, c0, k0, n):
        dy = pl.ds(c0, T)
        acc = None
        for t in range(2):
            part = pl.ds(t * N, N)
            for who, base in ((ME, k0), (SIB, H + k0)):
                term = _tdot(dx_ref[part, cut(base, n)], dyv[who, j, part, dy])
                acc = term if acc is None else acc + term
        return acc

    def p_tile(dst, j, q, kt):
        loop(2, lambda h: put(dst.at[q, kt, pl.ds(h * T, T)], p_part(j, q * T, kt * D + h * T, T)))

    def put(ref, value):
        ref[...] = value

    x0_load.wait()
    dy_to_sib(OWN, 0).wait_recv()
    x_first(1).wait_recv()
    pown[0, 0, T:] = p_part(OWN, 0, T, T)

    @pl.when(is_b)
    def _():
        p_first(2).start()

    x_first(0).wait_recv()
    dy_load.wait()

    def own_tile(q, kt):
        if q == 0:
            x_load(kt).wait()
            x_to_sib(kt).wait_recv()
        p_tile(pown, OWN, q, kt)
        if q < 2:
            @pl.when(is_b)
            def _():
                p_half(q, kt, 0).start()
                p_half(q, kt, 1).start()

    for q in range(4):
        if q > 0:
            dy_to_sib(OWN, q).wait_recv()
        loop(4, lambda kt, q=q: own_tile(q, kt), int(q == 0))

    def trans_tile(q, kt):
        if q == 0:
            for r in range(4):
                p_trans(q, kt, r).start()
            return

        @pl.when(kt < 3)
        def _():
            for r in range(4):
                p_trans(q, kt, r).start()

        @pl.when(kt == 3)
        def _():
            p_trans_short().start()
            p_trans_tail().start()
            p_extra().start()

    def dy_in(q):
        dy_to_y(q).wait_recv()
        dy_to_sib(OTH, q).start()

    def other_pass(q):
        dy_in(q)
        dy_to_sib(OTH, q).wait_recv()

        def tile(kt):
            p_tile(poth, OTH, q, kt)
            if q < 2:
                @pl.when(jnp.logical_and(is_a, 4 * q + kt < 7))
                def _():
                    p_term(q, kt).start()

                @pl.when(jnp.logical_and(is_a, 4 * q + kt == 7))
                def _():
                    p_term_short().start()

                @pl.when(is_b)
                def _():
                    trans_tile(q, kt)
            else:
                @pl.when(is_b)
                def _():
                    p_other(q, kt).start()

        loop(4, tile)

    def w_loads(d, cc, src):
        ref = w_ref.at[qs(d)] if src == ARG else wbuf.at[cc, OWN, qs(d)]
        return (
            local(ref, wv.at[cc, OWN], wl_sem.at[cc, OWN]),
            local(wbuf.at[cc, OTH, qs(d)], wv.at[cc, OTH], wl_sem.at[cc, OTH]),
        )

    def start_loads(d, cc, src):
        for cp in w_loads(d, cc, src):
            cp.start()

    def wait_loads(d, cc, src):
        for cp in w_loads(d, cc, src):
            cp.wait()

    def dx_stripe(d, cc, lo=0, hi=4):
        cols = cut((c + cc * (1 - 2 * c)) * H + d * T, T, T)

        def rows(m):
            part = pl.ds(m * D, D)
            dx_ref[part, cols] = (
                _dot_t(dyv[ME, OWN, part, :], wv[cc, OWN]) + _dot_t(dyv[ME, OTH, part, :], wv[cc, OTH])
            ).astype(BF16)

        loop(hi, rows, lo)

    def pair_wait(d, src):
        w_to_sib(OWN, d, src).wait_recv()
        w_to_sib(OTH, d, BUF).wait_recv()

    other_pass(0)
    other_pass(1)

    @pl.when(is_a)
    def _():
        def add(q, kt):
            tile = dw_tile(q, kt)
            tile[...] = tile[...] + pown[q, kt]

        def final_early(t):
            q, kt = t // 4, t % 4

            @pl.when(t == 0)
            def _():
                for i in range(len(FIRST)):
                    p_first(i).wait_recv()

            @pl.when(t > 0)
            def _():
                p_half(q, kt, 0).wait_recv()
                p_half(q, kt, 1).wait_recv()
            add(q, kt)

        def final_late(t):
            q, kt = 2 + t // 4, t % 4
            p_own(q, kt).wait_recv()
            add(q, kt)

        def a_sum(q, kt):
            p_other(q, kt).wait_recv()
            poth[q, kt] = poth[q, kt] + land[q - 2, kt]

            @pl.when(4 * q + kt < 15)
            def _():
                sum_to_y(q, kt).start()

            @pl.when(4 * q + kt == 15)
            def _():
                sum_short().start()
                tail_y_store(poth).start()

        def early(i):
            w_to_y(i).wait_recv()
            w_fwd(i).start()
            w_to_sib(OTH, i, BUF).start()
            final_early(i)

        loop(4, early)
        dy_in(2)
        dy_to_sib(OTH, 2).wait_recv()

        def q2_tile(kt):
            p_tile(poth, OTH, 2, kt)
            final_early(4 + kt)

        loop(4, q2_tile)
        p_extra().wait_recv()
        poth[1, 3, D - E:] = poth[1, 3, D - E:] + extra[...]
        extra_to_y().start()
        start_loads(0, ME, ARG)
        dy_in(3)

        def step(i):
            @pl.when(i < 16)
            def _():
                w_to_y_piece(i).wait_recv()
                w_fwd_piece(i).start()

                @pl.when(i % 4 == 3)
                def _():
                    w_to_sib(OTH, 4 + i // 4, BUF).start()

            @pl.when(i >= 16)
            def _():
                k = i - 16
                q, kt, r = k // 16, (k // 4) % 4, k % 4
                p_trans(q, kt, r).wait_recv()
                p_fwd(q, kt, r).start()

            @pl.when(i == 0)
            def _():
                dy_to_sib(OTH, 3).wait_recv()

            @pl.when(i < 4)
            def _():
                p_tile(poth, OTH, 3, i)

            @pl.when(jnp.logical_and(i >= 4, i < 36))
            def _():
                e = (i - 4) // 2
                d, cc = e // 2, e % 2
                odd = i % 2

                @pl.when(jnp.logical_and(odd == 0, cc == ME))
                def _():
                    pair_wait(d, ARG)
                    start_loads(d, SIB, BUF)
                    wait_loads(d, ME, ARG)

                @pl.when(jnp.logical_and(odd == 0, cc == SIB))
                def _():
                    @pl.when(d < 7)
                    def _():
                        start_loads(d + 1, ME, ARG)
                    wait_loads(d, SIB, BUF)

                dx_stripe(d, cc, 2 * odd, 2 * odd + 2)

            @pl.when(jnp.logical_and(i < 8, i % 2 == 1))
            def _():
                a_sum(2, i // 2)

            @pl.when(jnp.logical_and(jnp.logical_and(i >= 10, i < 26), i % 4 == 2))
            def _():
                a_sum(3, (i - 10) // 4)

            @pl.when(jnp.logical_and(i >= 26, i % 4 == 2))
            def _():
                final_late((i - 26) // 4)

        loop(44, step)
        p_trans_short().wait_recv()
        p_fwd_short().start()
        low = dw_part(3, 4 * D - R, R)
        low[...] = pown[3, 3, D - R:]
        final_late(5)
        final_late(6)
        p_trans_tail().wait_recv()
        p_own_last().wait_recv()
        top = dw_part(3, 3 * D, D - R)
        top[...] = top[...] + pown[3, 3, :D - R]
        drain(wbuf.at[ME], s_w)
        tail_y_store(poth).wait()
        drain(dyv.at[ME, OWN, pl.ds(0, H - T)], s_px)
        drain(land, s_py)
        drain(dyv.at[ME, OWN, pl.ds(0, H - T)], s_sum)
        drain(land.at[0, 0, pl.ds(0, D - EY + F)], s_last)

    @pl.when(is_b)
    def _():
        other_pass(2)
        other_pass(3)
        for t in range(7):
            p_own(2 + t // 4, t % 4).start()
        p_own_last().start()
        tail_store().start()
        tail_y_store(pown).start()

        def own_w(i):
            w_own_to_x(i).wait_recv()
            w_to_sib(OWN, i, BUF).start()

        loop(8, own_w)

        def stripes(d):
            @pl.when(d < 4)
            def _():
                w_to_y(d).wait_recv()

            @pl.when(d >= 4)
            def _():
                for p in range(4):
                    w_to_y_piece(4 * (d - 4) + p).wait_recv()
            w_to_sib(OTH, d, BUF).start()
            start_loads(d, ME, BUF)
            pair_wait(d, BUF)
            start_loads(d, SIB, BUF)
            for cc in (ME, SIB):
                wait_loads(d, cc, BUF)
                dx_stripe(d, cc)

        loop(8, stripes)

        def fin(i):
            q, kt, r = i // 16, (i // 4) % 4, i % 4

            @pl.when(r == 0)
            def _():
                p_term(q, kt).wait_recv()
            p_fwd(q, kt, r).wait_recv()
            tile = dw_part(q, kt * D + r * Q, Q)
            tile[...] = tile[...] + land[q, kt, pl.ds(r * Q, Q)]

        loop(28, fin)
        p_term_short().wait_recv()
        p_fwd_short().wait_recv()
        tile = dw_part(1, 3 * D, F)
        tile[...] = tile[...] + land[1, 3, :F]
        extra_to_y().wait_recv()
        for t in range(7):
            sum_to_y(2 + t // 4, t % 4).wait_recv()
        sum_short().wait_recv()
        tail_y_store(pown).wait()
        tail_store().wait()
        drain(wbuf.at[ME, OWN], s_w)
        drain(dw_ref.at[pl.ds(0, H - Q)], s_px)
        drain(land.at[0, 0, pl.ds(0, D - R)], s_sum)
        drain(land.at[0, 0, pl.ds(0, D - E)], s_last)
        drain(land, s_po)
        drain(extra, s_ex)
        drain(dyv.at[ME, OWN, pl.ds(0, H - T)], s_py)

    drain(dyv.at[ME], s_dys)
    drain(dyv.at[ME, OWN], s_dyy)
    drain(wbuf.at[ME], s_xs)
    drain(swap.at[0], s_sw)
    drain(wbuf.at[ME], s_ws)


def store_kernel(dx_ref, dw_ref, dx_out, dw_out, sem):
    copies = []
    for i in range(2):
        part = pl.ds(i * N, N)
        copies.append(pltpu.make_async_copy(dx_ref.at[part], dx_out.at[part], sem.at[0, i]))
        copies.append(pltpu.make_async_copy(dw_ref.at[part], dw_out.at[part], sem.at[1, i]))
    for cp in copies:
        cp.start()
    for cp in copies:
        cp.wait()


def add_kernel(done_ref, dw_ref, tail_ref, tail_y_ref, dw_out, buf, buf_y, sem, sem_y):
    is_a = lax.axis_index("row") // 2 == lax.axis_index("col")
    rows = cut(jnp.where(is_a, H - R, 3 * D + F), R, 8)
    cols = cut(jnp.where(is_a, 3 * T, T), T)
    buf[...] = dw_ref[rows, cols] + tail_ref[...]
    first = pltpu.make_async_copy(buf, dw_out.at[rows, cols], sem)
    first.start()
    rows_y, cols_y = pl.ds(H - EY, EY), cut(jnp.where(is_a, 0, 3 * T), T)
    buf_y[...] = jnp.where(is_a, dw_ref[rows_y, cols_y], tail_y_ref[...])
    second = pltpu.make_async_copy(buf_y, dw_out.at[rows_y, cols_y], sem_y)
    second.start()
    first.wait()
    second.wait()


def local_backward(act_blk, w_blk, grad_blk):
    any_spec = pl.BlockSpec(memory_space=pl.ANY)
    vmem_spec = pl.BlockSpec(memory_space=pltpu.VMEM)
    dma = pltpu.SemaphoreType.DMA
    outs = pl.pallas_call(
        kernel,
        out_shape=(
            pltpu.VMEM((H, 2 * H), BF16),
            pltpu.VMEM((H, N), F32),
            jax.ShapeDtypeStruct((2, 2, H, N), BF16),
            jax.ShapeDtypeStruct((2, 4, D, T), F32),
            jax.ShapeDtypeStruct((R, T), F32),
            jax.ShapeDtypeStruct((EY, T), F32),
        ),
        in_specs=[any_spec] * 3,
        out_specs=(vmem_spec,) * 2 + (any_spec,) * 4,
        scratch_shapes=[
            pltpu.VMEM((2, 2, H, N), BF16),
            pltpu.VMEM((4, 4, D, T), F32),
            pltpu.VMEM((4, 4, D, T), F32),
            pltpu.VMEM((2, 2, T, N), BF16),
            pltpu.VMEM((2, 4, D, T), F32),
            pltpu.VMEM((E, T), F32),
            pltpu.VMEM((2, T, T), F32),
            dma, dma((4,)), dma((2, 4)), dma((4,)), dma((4,)), dma((5,)), dma((2, 8)), dma((16,)), dma((2, 8)),
            dma((4,)), dma((2, 8)), dma((2, 4)), dma((2, 4)), dma((4, 4)), dma((2, 16)),
            dma, dma, dma, dma, dma, dma, dma, dma, dma, dma((2, 2)), dma,
            dma, dma, dma, dma, dma, dma((2,)), dma((2,)), dma, dma((2,)), dma,
        ],
        compiler_params=pltpu.CompilerParams(
            collective_id=0, has_side_effects=True, vmem_limit_bytes=41_800_000
        ),
        cost_estimate=pl.CostEstimate(flops=8 * H * H * H, bytes_accessed=100 << 20, transcendentals=0),
    )(act_blk, w_blk, grad_blk)
    tail = lax.ppermute(outs[4], "row", [(i, (i + 2) % 4) for i in range(4)])
    tail_y = lax.ppermute(outs[5], "col", [(0, 1), (1, 0)])
    dx, dw = pl.pallas_call(
        store_kernel,
        out_shape=(jax.ShapeDtypeStruct((H, 2 * H), BF16), jax.ShapeDtypeStruct((H, N), F32)),
        in_specs=[vmem_spec] * 2,
        out_specs=(any_spec,) * 2,
        scratch_shapes=[dma((2, 2))],
        compiler_params=pltpu.CompilerParams(vmem_limit_bytes=1 << 20),
        cost_estimate=pl.CostEstimate(flops=0, bytes_accessed=48 << 20, transcendentals=0),
    )(outs[0], outs[1])
    dw = pl.pallas_call(
        add_kernel,
        out_shape=jax.ShapeDtypeStruct((H, N), F32),
        in_specs=[any_spec] + [vmem_spec] * 3,
        out_specs=any_spec,
        scratch_shapes=[pltpu.VMEM((R, T), F32), pltpu.VMEM((EY, T), F32), dma, dma],
        input_output_aliases={0: 0},
        compiler_params=pltpu.CompilerParams(vmem_limit_bytes=2 << 20),
        cost_estimate=pl.CostEstimate(flops=0, bytes_accessed=1 << 20, transcendentals=0),
    )(dw, outs[1], tail, tail_y)
    return dx, dw


def solution(mesh):
    io_spec = P(("dp", "row"), "col")
    w_spec = P("row", "col")
    return jax.shard_map(
        local_backward, mesh=mesh, in_specs=(io_spec, w_spec, io_spec), out_specs=(io_spec, io_spec), check_vma=False
    )
```

```python
import jax
import jax.numpy as jnp
from jax import lax
from jax.experimental import pallas as pl
from jax.experimental.pallas import tpu as pltpu
from jax.sharding import PartitionSpec as P

MESH = pl.DeviceIdType.MESH
F32 = jnp.float32
BF16 = jnp.bfloat16
H, N, D, T, Q, S = 2048, 1024, 512, 256, 128, 64
R = 376
E = 120
EY = 88
F = D - E - R
ME, SIB = 0, 1
OWN, OTH = 0, 1
ARG, BUF = "arg", "buf"
FIRST = ((0, Q), (Q, Q), (T, T))


def _tdot(a, b):
    return lax.dot_general(a, b, (((0,), (0,)), ((), ())), preferred_element_type=F32)


def _dot_t(a, b):
    return lax.dot_general(a, b, (((1,), (1,)), ((), ())), preferred_element_type=F32)


def loop(n, f, start=0):
    def body(i, carry):
        f(i)
        return carry

    lax.fori_loop(start, n, body, start)


def cut(k0, n, unit=Q):
    return pl.ds(pl.multiple_of(k0, unit), n)


def kernel(
    x_ref, w_ref, dy_ref,
    dx_ref, dw_ref, wbuf, bufy, tail, tail_y,
    dyv, pown, poth, wv, land, extra, swap,
    dy_sem, x_sem, dys_r, dyy_r, xs_r, xf_r, w_r, wp_r, ws_r, pa_r, ph_r, po_r, ps_r, py_r, pf_r,
    s_dys, s_dyy, s_xs, s_w, s_ws, s_px, s_po, s_py, s_sum, wl_sem, tail_sem, tail_y_sem, s_ex, ex_r, py_ex, dyq_sem, xt_sem, xq_sem, s_sw, sw_r, s_last,
):
    row = lax.axis_index("row")
    y = lax.axis_index("col")
    x = row // 2
    c = row % 2
    is_a = x == y
    is_b = x != y
    sib = {"row": row + 1 - 2 * c}
    xn = {"row": (row + 2) % 4}
    yn = {"col": 1 - y}

    def remote(src, dst, ssem, rsem, dev):
        return pltpu.make_async_remote_copy(
            src_ref=src, dst_ref=dst, send_sem=ssem, recv_sem=rsem, device_id=dev, device_id_type=MESH
        )

    def local(src, dst, sem):
        return pltpu.make_async_copy(src, dst, sem)

    def qs(q):
        return pl.ds(q * T, T)

    def xo(k0, n):
        return dx_ref.at[:, cut(k0, n)]

    def xs(k0, n):
        return dx_ref.at[:, cut(H + k0, n)]

    def dw_part(q, r0, n):
        return dw_ref.at[pl.ds(r0, n), cut(q * T, T)]

    def dw_tile(q, kt):
        return dw_part(q, kt * D, D)

    dyq_load = local(dy_ref.at[:, pl.ds(0, T)], dyv.at[ME, OWN, :, pl.ds(0, T)], dyq_sem)
    dy_load = local(dy_ref.at[:, pl.ds(T, N - T)], dyv.at[ME, OWN, :, pl.ds(T, N - T)], dy_sem)
    def xt_load(h):
        return local(x_ref.at[:, pl.ds((1 - c) * H + h * Q, Q)], xo(3 * D + h * Q, Q), xt_sem.at[h])

    def xq_load(h):
        return local(x_ref.at[:, pl.ds(c * H + h * Q, Q)], xo(h * Q, Q), xq_sem.at[h])

    def swap_part(h):
        part = pl.ds(h * Q, Q)
        return remote(swap.at[0, part], swap.at[1, part], s_sw, sw_r.at[h], sib)

    x0_load = local(x_ref.at[:, pl.ds(c * H + T, D - T)], xo(T, D - T), x_sem.at[0])
    def x_load(kt):
        return local(x_ref.at[:, pl.ds(c * H + kt * D, D)], xo(kt * D, D), x_sem.at[kt])

    def x_cols_to_sib(k0, n, sem):
        return remote(x_ref.at[:, pl.ds((1 - c) * H + k0, n)], xs(k0, n), s_xs, sem, sib)

    def x_to_sib(kt):
        return x_cols_to_sib(kt * D, D, xs_r.at[kt])

    def x_first(i):
        return x_cols_to_sib(i * T, T, xf_r.at[i])

    def dy_to_sib(j, q):
        src = dy_ref.at[:, qs(q)] if j == OWN else dyv.at[ME, OTH, :, qs(q)]
        return remote(src, dyv.at[SIB, j, :, qs(q)], s_dys, dys_r.at[j, q], sib)

    def dy_to_y(q):
        return remote(dy_ref.at[:, qs(q)], dyv.at[ME, OTH, :, qs(q)], s_dyy, dyy_r.at[q], yn)

    def w_own_to_x(i):
        return remote(w_ref.at[qs(i)], wbuf.at[ME, OWN, qs(i)], s_w, w_r.at[OWN, i], xn)

    def w_to_y(i):
        return remote(w_ref.at[qs(i)], wbuf.at[ME, OTH, qs(i)], s_w, w_r.at[OTH, i], yn)

    def w_fwd(i):
        return remote(wbuf.at[ME, OTH, qs(i)], wbuf.at[ME, OTH, qs(i)], s_w, w_r.at[OTH, i], xn)

    def w_piece(p):
        return pl.ds(N + p * S, S)

    def w_to_y_piece(p):
        return remote(w_ref.at[w_piece(p)], wbuf.at[ME, OTH, w_piece(p)], s_w, wp_r.at[p], yn)

    def w_fwd_piece(p):
        return remote(wbuf.at[ME, OTH, w_piece(p)], wbuf.at[ME, OTH, w_piece(p)], s_w, wp_r.at[p], xn)

    def w_to_sib(j, i, src):
        ref = w_ref.at[qs(i)] if src == ARG else wbuf.at[ME, j, qs(i)]
        return remote(ref, wbuf.at[SIB, j, qs(i)], s_ws, ws_r.at[j, i], sib)

    def p_first(i):
        r0, n = FIRST[i]
        return remote(pown.at[0, 0, pl.ds(r0, n)], dw_part(0, r0, n), s_px, pa_r.at[i], xn)

    def p_half(q, kt, h):
        return remote(
            pown.at[q, kt, pl.ds(h * T, T)], dw_part(q, kt * D + h * T, T), s_px, ph_r.at[q, 2 * kt + h], xn
        )

    def p_own(q, kt):
        return remote(pown.at[q, kt], dw_tile(q, kt), s_px, po_r.at[q - 2, kt], xn)

    def p_own_last():
        return remote(
            pown.at[3, 3, pl.ds(0, D - R)], dw_part(3, 3 * D, D - R), s_sum, po_r.at[1, 3], xn
        )

    def tail_store():
        return local(pown.at[3, 3, pl.ds(D - R, R)], tail, tail_sem)

    def p_other(q, kt):
        return remote(poth.at[q, kt], land.at[q - 2, kt], s_po, ps_r.at[q - 2, kt], xn)

    def p_trans(q, kt, r):
        part = pl.ds(r * Q, Q)
        return remote(poth.at[q, kt, part], bufy.at[q, kt, part], s_py, pf_r.at[q, 4 * kt + r], yn)

    def p_fwd(q, kt, r):
        part = pl.ds(r * Q, Q)
        return remote(bufy.at[q, kt, part], land.at[q, kt, part], s_px, pf_r.at[q, 4 * kt + r], xn)

    def p_trans_short():
        part = pl.ds(0, F)
        return remote(poth.at[1, 3, part], bufy.at[1, 3, part], s_last, pf_r.at[1, 12], yn)

    def p_fwd_short():
        part = pl.ds(0, F)
        return remote(bufy.at[1, 3, part], land.at[1, 3, part], s_last, pf_r.at[1, 12], xn)

    def p_trans_tail():
        return remote(poth.at[1, 3, pl.ds(F, R)], tail, s_last, pf_r.at[1, 13], yn)

    def p_extra():
        return remote(poth.at[1, 3, pl.ds(D - E, E)], extra, s_ex, ex_r, xn)

    def extra_to_y():
        return remote(poth.at[1, 3, pl.ds(D - E, E)], dw_part(1, 4 * D - E, E), s_py, py_ex, yn)

    def p_term(q, kt):
        return remote(poth.at[q, kt], dw_tile(q, kt), s_py, py_r.at[q, kt], yn)

    def p_term_short():
        part = pl.ds(0, D - E)
        return remote(poth.at[1, 3, part], dw_part(1, 3 * D, D - E), s_py, py_r.at[1, 3], yn)

    def sum_short():
        part = pl.ds(0, D - EY)
        return remote(poth.at[3, 3, part], dw_part(3, 3 * D, D - EY), s_last, py_r.at[3, 3], yn)

    def tail_y_store(src):
        return local(src.at[3, 3, pl.ds(D - EY, EY)], tail_y, tail_y_sem)

    def sum_to_y(q, kt):
        return remote(poth.at[q, kt], dw_tile(q, kt), s_sum, py_r.at[q, kt], yn)

    def drain(ref, sem):
        remote(ref, ref, sem, dyy_r.at[0], yn).wait_send()

    for cp in (dyq_load, xt_load(0), xq_load(0)):
        cp.start()

    barrier = pltpu.get_barrier_semaphore()
    for dev in (sib, xn, yn):
        pl.semaphore_signal(barrier, inc=1, device_id=dev, device_id_type=MESH)
    pl.semaphore_wait(barrier, 3)

    dy_to_y(0).start()
    dy_to_y(1).start()

    @pl.when(is_a)
    def _():
        for i in range(8):
            w_own_to_x(i).start()
        for q in (2, 3):
            dy_to_y(q).start()

    @pl.when(is_b)
    def _():
        for i in range(4):
            w_to_y(i).start()
        for q in (2, 3):
            dy_to_y(q).start()
        for p in range(16):
            w_to_y_piece(p).start()

    def swap_send(h):
        xt_load(h).wait()
        xq_load(h).wait()
        if h == 0:
            xt_load(1).start()
            xq_load(1).start()
        swap[0, pl.ds(h * Q, Q)] = _tdot(dx_ref[:, 3 * D + h * Q:3 * D + h * Q + Q], dyv[ME, OWN, :, :T])
        swap_part(h).start()

    def own_first(h):
        pown[0, 0, pl.ds(h * Q, Q)] = _tdot(dx_ref[:, h * Q:h * Q + Q], dyv[ME, OWN, :, :T])

    def swap_add(h):
        part = pl.ds(h * Q, Q)
        swap_part(h).wait_recv()
        pown[0, 0, part] = pown[0, 0, part] + swap[1, part]

        @pl.when(is_b)
        def _():
            p_first(h).start()

    dyq_load.wait()
    swap_send(0)
    own_first(0)
    swap_send(1)
    dy_to_sib(OWN, 0).start()
    x_first(1).start()
    swap_add(0)
    own_first(1)
    swap_add(1)
    for cp in (x0_load, dy_load, x_load(1), x_load(2), x_load(3)):
        cp.start()
    x_first(0).start()
    for kt in (1, 2, 3):
        x_to_sib(kt).start()
    for q in (1, 2, 3):
        dy_to_sib(OWN, q).start()

    @pl.when(is_a)
    def _():
        for i in range(8):
            w_to_sib(OWN, i, ARG).start()

    def p_part(j, c0, k0, n):
        dy = pl.ds(c0, T)
        acc = None
        for t in range(2):
            part = pl.ds(t * N, N)
            for who, base in ((ME, k0), (SIB, H + k0)):
                term = _tdot(dx_ref[part, cut(base, n)], dyv[who, j, part, dy])
                acc = term if acc is None else acc + term
        return acc

    def p_tile(dst, j, q, kt):
        loop(2, lambda h: put(dst.at[q, kt, pl.ds(h * T, T)], p_part(j, q * T, kt * D + h * T, T)))

    def put(ref, value):
        ref[...] = value

    x0_load.wait()
    dy_to_sib(OWN, 0).wait_recv()
    x_first(1).wait_recv()
    pown[0, 0, T:] = p_part(OWN, 0, T, T)

    @pl.when(is_b)
    def _():
        p_first(2).start()

    x_first(0).wait_recv()
    dy_load.wait()

    def own_tile(q, kt):
        if q == 0:
            x_load(kt).wait()
            x_to_sib(kt).wait_recv()
        p_tile(pown, OWN, q, kt)
        if q < 2:
            @pl.when(is_b)
            def _():
                p_half(q, kt, 0).start()
                p_half(q, kt, 1).start()

    for q in range(4):
        if q > 0:
            dy_to_sib(OWN, q).wait_recv()
        loop(4, lambda kt, q=q: own_tile(q, kt), int(q == 0))

    def trans_tile(q, kt):
        if q == 0:
            for r in range(4):
                p_trans(q, kt, r).start()
            return

        @pl.when(kt < 3)
        def _():
            for r in range(4):
                p_trans(q, kt, r).start()

        @pl.when(kt == 3)
        def _():
            p_trans_short().start()
            p_trans_tail().start()
            p_extra().start()

    def dy_in(q):
        dy_to_y(q).wait_recv()
        dy_to_sib(OTH, q).start()

    def other_pass(q):
        dy_in(q)
        dy_to_sib(OTH, q).wait_recv()

        def tile(kt):
            p_tile(poth, OTH, q, kt)
            if q < 2:
                @pl.when(jnp.logical_and(is_a, 4 * q + kt < 7))
                def _():
                    p_term(q, kt).start()

                @pl.when(jnp.logical_and(is_a, 4 * q + kt == 7))
                def _():
                    p_term_short().start()

                @pl.when(is_b)
                def _():
                    trans_tile(q, kt)
            else:
                @pl.when(is_b)
                def _():
                    p_other(q, kt).start()

        loop(4, tile)

    def w_loads(d, cc, src):
        ref = w_ref.at[qs(d)] if src == ARG else wbuf.at[cc, OWN, qs(d)]
        return (
            local(ref, wv.at[cc, OWN], wl_sem.at[cc, OWN]),
            local(wbuf.at[cc, OTH, qs(d)], wv.at[cc, OTH], wl_sem.at[cc, OTH]),
        )

    def start_loads(d, cc, src):
        for cp in w_loads(d, cc, src):
            cp.start()

    def wait_loads(d, cc, src):
        for cp in w_loads(d, cc, src):
            cp.wait()

    def dx_stripe(d, cc, lo=0, hi=4):
        cols = cut((c + cc * (1 - 2 * c)) * H + d * T, T, T)

        def rows(m):
            part = pl.ds(m * D, D)
            dx_ref[part, cols] = (
                _dot_t(dyv[ME, OWN, part, :], wv[cc, OWN]) + _dot_t(dyv[ME, OTH, part, :], wv[cc, OTH])
            ).astype(BF16)

        loop(hi, rows, lo)

    def pair_wait(d, src):
        w_to_sib(OWN, d, src).wait_recv()
        w_to_sib(OTH, d, BUF).wait_recv()

    other_pass(0)
    other_pass(1)

    @pl.when(is_a)
    def _():
        def add(q, kt):
            tile = dw_tile(q, kt)
            tile[...] = tile[...] + pown[q, kt]

        def final_early(t):
            q, kt = t // 4, t % 4

            @pl.when(t == 0)
            def _():
                for i in range(len(FIRST)):
                    p_first(i).wait_recv()

            @pl.when(t > 0)
            def _():
                p_half(q, kt, 0).wait_recv()
                p_half(q, kt, 1).wait_recv()
            add(q, kt)

        def final_late(t):
            q, kt = 2 + t // 4, t % 4
            p_own(q, kt).wait_recv()
            add(q, kt)

        def a_sum(q, kt):
            p_other(q, kt).wait_recv()
            poth[q, kt] = poth[q, kt] + land[q - 2, kt]

            @pl.when(4 * q + kt < 15)
            def _():
                sum_to_y(q, kt).start()

            @pl.when(4 * q + kt == 15)
            def _():
                sum_short().start()
                tail_y_store(poth).start()

        def early(i):
            w_to_y(i).wait_recv()
            w_fwd(i).start()
            w_to_sib(OTH, i, BUF).start()
            final_early(i)

        loop(4, early)
        dy_in(2)
        dy_to_sib(OTH, 2).wait_recv()

        def q2_tile(kt):
            p_tile(poth, OTH, 2, kt)
            final_early(4 + kt)

        loop(4, q2_tile)
        p_extra().wait_recv()
        poth[1, 3, D - E:] = poth[1, 3, D - E:] + extra[...]
        extra_to_y().start()
        start_loads(0, ME, ARG)
        dy_in(3)

        def step(i):
            @pl.when(i < 16)
            def _():
                w_to_y_piece(i).wait_recv()
                w_fwd_piece(i).start()

                @pl.when(i % 4 == 3)
                def _():
                    w_to_sib(OTH, 4 + i // 4, BUF).start()

            @pl.when(i >= 16)
            def _():
                k = i - 16
                q, kt, r = k // 16, (k // 4) % 4, k % 4
                p_trans(q, kt, r).wait_recv()
                p_fwd(q, kt, r).start()

            @pl.when(i == 0)
            def _():
                dy_to_sib(OTH, 3).wait_recv()

            @pl.when(i < 4)
            def _():
                p_tile(poth, OTH, 3, i)

            @pl.when(jnp.logical_and(i >= 4, i < 36))
            def _():
                e = (i - 4) // 2
                d, cc = e // 2, e % 2
                odd = i % 2

                @pl.when(jnp.logical_and(odd == 0, cc == ME))
                def _():
                    pair_wait(d, ARG)
                    start_loads(d, SIB, BUF)
                    wait_loads(d, ME, ARG)

                @pl.when(jnp.logical_and(odd == 0, cc == SIB))
                def _():
                    @pl.when(d < 7)
                    def _():
                        start_loads(d + 1, ME, ARG)
                    wait_loads(d, SIB, BUF)

                dx_stripe(d, cc, 2 * odd, 2 * odd + 2)

            @pl.when(jnp.logical_and(i < 8, i % 2 == 1))
            def _():
                a_sum(2, i // 2)

            @pl.when(jnp.logical_and(jnp.logical_and(i >= 10, i < 26), i % 4 == 2))
            def _():
                a_sum(3, (i - 10) // 4)

            @pl.when(jnp.logical_and(i >= 26, i % 4 == 2))
            def _():
                final_late((i - 26) // 4)

        loop(44, step)
        p_trans_short().wait_recv()
        p_fwd_short().start()
        low = dw_part(3, 4 * D - R, R)
        low[...] = pown[3, 3, D - R:]
        final_late(5)
        final_late(6)
        p_trans_tail().wait_recv()
        p_own_last().wait_recv()
        top = dw_part(3, 3 * D, D - R)
        top[...] = top[...] + pown[3, 3, :D - R]
        drain(wbuf.at[ME], s_w)
        tail_y_store(poth).wait()
        drain(dyv.at[ME, OWN, pl.ds(0, H - T)], s_px)
        drain(land, s_py)
        drain(dyv.at[ME, OWN, pl.ds(0, H - T)], s_sum)
        drain(land.at[0, 0, pl.ds(0, D - EY + F)], s_last)

    @pl.when(is_b)
    def _():
        other_pass(2)
        other_pass(3)
        for t in range(7):
            p_own(2 + t // 4, t % 4).start()
        p_own_last().start()
        tail_store().start()
        tail_y_store(pown).start()

        def own_w(i):
            w_own_to_x(i).wait_recv()
            w_to_sib(OWN, i, BUF).start()

        loop(8, own_w)

        def stripes(d):
            @pl.when(d < 4)
            def _():
                w_to_y(d).wait_recv()

            @pl.when(d >= 4)
            def _():
                for p in range(4):
                    w_to_y_piece(4 * (d - 4) + p).wait_recv()
            w_to_sib(OTH, d, BUF).start()
            start_loads(d, ME, BUF)
            pair_wait(d, BUF)
            start_loads(d, SIB, BUF)
            for cc in (ME, SIB):
                wait_loads(d, cc, BUF)
                dx_stripe(d, cc)

        loop(8, stripes)

        def fin(i):
            q, kt, r = i // 16, (i // 4) % 4, i % 4

            @pl.when(r == 0)
            def _():
                p_term(q, kt).wait_recv()
            p_fwd(q, kt, r).wait_recv()
            tile = dw_part(q, kt * D + r * Q, Q)
            tile[...] = tile[...] + land[q, kt, pl.ds(r * Q, Q)]

        loop(28, fin)
        p_term_short().wait_recv()
        p_fwd_short().wait_recv()
        tile = dw_part(1, 3 * D, F)
        tile[...] = tile[...] + land[1, 3, :F]
        extra_to_y().wait_recv()
        for t in range(7):
            sum_to_y(2 + t // 4, t % 4).wait_recv()
        sum_short().wait_recv()
        tail_y_store(pown).wait()
        tail_store().wait()
        drain(wbuf.at[ME, OWN], s_w)
        drain(dw_ref.at[pl.ds(0, H - Q)], s_px)
        drain(land.at[0, 0, pl.ds(0, D - R)], s_sum)
        drain(land.at[0, 0, pl.ds(0, D - E)], s_last)
        drain(land, s_po)
        drain(extra, s_ex)
        drain(dyv.at[ME, OWN, pl.ds(0, H - T)], s_py)

    drain(dyv.at[ME], s_dys)
    drain(dyv.at[ME, OWN], s_dyy)
    drain(wbuf.at[ME], s_xs)
    drain(swap.at[0], s_sw)
    drain(wbuf.at[ME], s_ws)


def store_kernel(dx_ref, dw_ref, dx_out, dw_out, sem):
    copies = []
    for i in range(4):
        part = pl.ds(i * D, D)
        copies.append(pltpu.make_async_copy(dx_ref.at[part], dx_out.at[part], sem.at[0, i]))
        copies.append(pltpu.make_async_copy(dw_ref.at[part], dw_out.at[part], sem.at[1, i]))
    for cp in copies:
        cp.start()
    for cp in copies:
        cp.wait()


def add_kernel(done_ref, dw_ref, tail_ref, tail_y_ref, dw_out, buf, buf_y, sem, sem_y):
    is_a = lax.axis_index("row") // 2 == lax.axis_index("col")
    rows = cut(jnp.where(is_a, H - R, 3 * D + F), R, 8)
    cols = cut(jnp.where(is_a, 3 * T, T), T)
    buf[...] = dw_ref[rows, cols] + tail_ref[...]
    first = pltpu.make_async_copy(buf, dw_out.at[rows, cols], sem)
    first.start()
    rows_y, cols_y = pl.ds(H - EY, EY), cut(jnp.where(is_a, 0, 3 * T), T)
    buf_y[...] = jnp.where(is_a, dw_ref[rows_y, cols_y], tail_y_ref[...])
    second = pltpu.make_async_copy(buf_y, dw_out.at[rows_y, cols_y], sem_y)
    second.start()
    first.wait()
    second.wait()


def local_backward(act_blk, w_blk, grad_blk):
    any_spec = pl.BlockSpec(memory_space=pl.ANY)
    vmem_spec = pl.BlockSpec(memory_space=pltpu.VMEM)
    dma = pltpu.SemaphoreType.DMA
    outs = pl.pallas_call(
        kernel,
        out_shape=(
            pltpu.VMEM((H, 2 * H), BF16),
            pltpu.VMEM((H, N), F32),
            jax.ShapeDtypeStruct((2, 2, H, N), BF16),
            jax.ShapeDtypeStruct((2, 4, D, T), F32),
            jax.ShapeDtypeStruct((R, T), F32),
            jax.ShapeDtypeStruct((EY, T), F32),
        ),
        in_specs=[any_spec] * 3,
        out_specs=(vmem_spec,) * 2 + (any_spec,) * 4,
        scratch_shapes=[
            pltpu.VMEM((2, 2, H, N), BF16),
            pltpu.VMEM((4, 4, D, T), F32),
            pltpu.VMEM((4, 4, D, T), F32),
            pltpu.VMEM((2, 2, T, N), BF16),
            pltpu.VMEM((2, 4, D, T), F32),
            pltpu.VMEM((E, T), F32),
            pltpu.VMEM((2, T, T), F32),
            dma, dma((4,)), dma((2, 4)), dma((4,)), dma((4,)), dma((5,)), dma((2, 8)), dma((16,)), dma((2, 8)),
            dma((4,)), dma((2, 8)), dma((2, 4)), dma((2, 4)), dma((4, 4)), dma((2, 16)),
            dma, dma, dma, dma, dma, dma, dma, dma, dma, dma((2, 2)), dma,
            dma, dma, dma, dma, dma, dma((2,)), dma((2,)), dma, dma((2,)), dma,
        ],
        compiler_params=pltpu.CompilerParams(
            collective_id=0, has_side_effects=True, vmem_limit_bytes=41_800_000
        ),
        cost_estimate=pl.CostEstimate(flops=8 * H * H * H, bytes_accessed=100 << 20, transcendentals=0),
    )(act_blk, w_blk, grad_blk)
    tail = lax.ppermute(outs[4], "row", [(i, (i + 2) % 4) for i in range(4)])
    tail_y = lax.ppermute(outs[5], "col", [(0, 1), (1, 0)])
    dx, dw = pl.pallas_call(
        store_kernel,
        out_shape=(jax.ShapeDtypeStruct((H, 2 * H), BF16), jax.ShapeDtypeStruct((H, N), F32)),
        in_specs=[vmem_spec] * 2,
        out_specs=(any_spec,) * 2,
        scratch_shapes=[dma((2, 4))],
        compiler_params=pltpu.CompilerParams(vmem_limit_bytes=1 << 20),
        cost_estimate=pl.CostEstimate(flops=0, bytes_accessed=48 << 20, transcendentals=0),
    )(outs[0], outs[1])
    dw = pl.pallas_call(
        add_kernel,
        out_shape=jax.ShapeDtypeStruct((H, N), F32),
        in_specs=[any_spec] + [vmem_spec] * 3,
        out_specs=any_spec,
        scratch_shapes=[pltpu.VMEM((R, T), F32), pltpu.VMEM((EY, T), F32), dma, dma],
        input_output_aliases={0: 0},
        compiler_params=pltpu.CompilerParams(vmem_limit_bytes=2 << 20),
        cost_estimate=pl.CostEstimate(flops=0, bytes_accessed=1 << 20, transcendentals=0),
    )(dw, outs[1], tail, tail_y)
    return dx, dw


def solution(mesh):
    io_spec = P(("dp", "row"), "col")
    w_spec = P("row", "col")
    return jax.shard_map(
        local_backward, mesh=mesh, in_specs=(io_spec, w_spec, io_spec), out_specs=(io_spec, io_spec), check_vma=False
    )
```
